32 devices in a mesh: member: 2 (over y), blk: 16 (over z, x, core).
Axes of the slice: x: 2, y: 2, z: 4, core: 2. Of those that a mesh axis runs over, the one named last changes fastest.
Arguments:
- heat_anomaly: float32 [8, 1536, 512], P('member', 'blk'), parts along dimension 0, may hold values from -6 to 6
- saltiness_anomaly: float32 [8, 1536, 512], P('member', 'blk'), parts along dimension 0, may hold values from -6 to 6
- first_axis_flow: float32 [8, 1536, 512], P('member', 'blk'), parts along dimension 0, may hold values from -4 to 4
- second_axis_flow: float32 [8, 1536, 512], P('member', 'blk'), parts along dimension 0, may hold values from -4 to 4
- layer_spacing: float32 [4], replicated, may hold values from 0.5 to 4
- diagonal_shift: float32 [1536, 512], P('blk'), may hold values from 0.02 to 0.2
- water_tile_flags: int32 [16, 8], P('blk'), may hold values 0 or 1
Outputs:
- new_temperature: bfloat16 [8, 1536, 512], P('member', 'blk'), parts along dimension 0
- new_salinity: bfloat16 [8, 1536, 512], P('member', 'blk'), parts along dimension 0
- new_u: bfloat16 [8, 1536, 512], P('member', 'blk'), parts along dimension 0
- new_v: bfloat16 [8, 1536, 512], P('member', 'blk'), parts along dimension 0
- height: float32 [3072, 512], P(('member', 'blk')), parts along dimension 0
- residual: float32 [3072, 512], P(('member', 'blk')), parts along dimension 0
The draws below stay inside these ranges and needn't reach their ends.
There are 2 independent parts, one for each index of `member`. The reference program is written for one: setup_inputs(seed, part) draws one part's arguments, and reference() takes and returns one part's arrays. A program takes and returns all parts, laid end to end along the dimension named above; an argument that names none is the same for every part. Nothing has to cross between parts.
Inputs may be any that keep to these rules, and one draw needn't show every extreme that they name: `water_tile_flags`: 1 marks an ocean block, 0 a land block.
All inputs are finite; a program needn't handle non-finite values.
Results may differ from the reference program's by a relative error of at most 0.001.
Values sent between devices are 32-bit elements; how exact they have to be, the bound alone decides.
A program may use at most 128 MiB of HBM per device.

```python
import math
import jax
import jax.numpy as jnp
import numpy as np
from jax import lax

BX = 96
BY = 64
HOME = 8
LAYER_TOTAL = 4
SSTEP = 4
CG_BLOCKS = 3
GRID_WIDTH_X = 1536
GRID_WIDTH_Y = 512
N_BLK = 16


def set_ends(drawn, own_key, low, largest):
    dims = drawn.shape
    index_at = [jax.random.randint(jax.random.fold_in(own_key, axis), (), 0, dims[axis]) for axis in range(len(dims))]
    drawn = drawn.at[tuple(index_at)].set(low)
    longest = dims.index(max(dims))
    index_at[longest] = (index_at[longest] + 1) % dims[longest]
    return drawn.at[tuple(index_at)].set(largest)


def steps_of(rng, shape, cuts, least, high):
    factor_of, own = 1.0, jax.random.fold_in(rng, 6)
    for axis_at, parts in cuts:
        draws = jnp.exp(jax.random.uniform(jax.random.fold_in(own, axis_at), (parts,), jnp.float32, least / len(cuts), high / len(cuts)))
        factor_of = factor_of * jnp.repeat(draws, shape[axis_at] // parts).reshape([-1 if axis == axis_at else 1 for axis in range(len(shape))])
    return factor_of


def gaussian(own_key, shape, scale, bound, pieces=(), kind=jnp.bfloat16):
    array = jax.random.normal(own_key, shape, jnp.float32) * scale
    if len(pieces) > 0:
        array = steps_of(own_key, shape, pieces, -0.22, 0.18) * array
    return jnp.clip(array, min=-bound, max=bound).astype(kind)


def setup_inputs(seed: int = 0, part: int = 0) -> dict:
    seeds = jax.random.split(jax.random.key(seed), 8)
    part_keys = jax.random.split(jax.random.fold_in(seeds[7], part), 8)
    return {
        "heat_anomaly": gaussian(part_keys[0], (LAYER_TOTAL, GRID_WIDTH_X, GRID_WIDTH_Y), 1.0, 6.0, ((1, 16),), jnp.float32),
        "saltiness_anomaly": gaussian(part_keys[1], (LAYER_TOTAL, GRID_WIDTH_X, GRID_WIDTH_Y), 1.0, 6.0, ((1, 16),), jnp.float32),
        "first_axis_flow": gaussian(part_keys[2], (LAYER_TOTAL, GRID_WIDTH_X, GRID_WIDTH_Y), 1.0, 4.0, ((1, 16),), jnp.float32),
        "second_axis_flow": gaussian(part_keys[3], (LAYER_TOTAL, GRID_WIDTH_X, GRID_WIDTH_Y), 1.0, 4.0, ((1, 16),), jnp.float32),
        "layer_spacing": jnp.clip(jnp.exp(jax.random.uniform(seeds[4], (LAYER_TOTAL,), jnp.float32, math.log(0.5), math.log(4.0))), 0.5, 4.0),
        "diagonal_shift": jnp.clip(jnp.exp(math.log(0.2) - 2.3025851 * jax.random.uniform(seeds[5], (GRID_WIDTH_X, GRID_WIDTH_Y), jnp.float32) ** steps_of(seeds[5], (GRID_WIDTH_X, GRID_WIDTH_Y), ((0, 16),), -0.2, 0.2)), 0.02, 0.2),
        "water_tile_flags": set_ends((jax.random.randint(seeds[6], (N_BLK, HOME), 0, 4) < 3).astype(jnp.int32), jax.random.fold_in(seeds[6], 1), 0, 1),
    }


COURANT = 0.2
HIGHEST = lax.Precision.HIGHEST


def wrap_east(field, margin):
    extent = field.shape[0]
    return jnp.concatenate([field[extent - margin:], field, field[:margin]], axis=0)


def pad_north(field):
    return jnp.pad(field, [(0, 0)] * (field.ndim - 1) + [(1, 1)])


def upwind(speed, behind, ahead):
    return jnp.where(speed > 0.0, speed * behind, speed * ahead)


def advect(tracer, east_vel, north_vel, wet_pad):
    east_face = 0.5 * (east_vel[..., :-1, 1:-1] + east_vel[..., 1:, 1:-1]) * (wet_pad[:-1, 1:-1] * wet_pad[1:, 1:-1])
    east_flux = upwind(east_face, tracer[..., :-1, 1:-1], tracer[..., 1:, 1:-1])
    north_face = 0.5 * (north_vel[..., 1:-1, :-1] + north_vel[..., 1:-1, 1:]) * (wet_pad[1:-1, :-1] * wet_pad[1:-1, 1:])
    north_flux = upwind(north_face, tracer[..., 1:-1, :-1], tracer[..., 1:-1, 1:])
    spread = (east_flux[..., 1:, :] - east_flux[..., :-1, :]) + (north_flux[..., 1:] - north_flux[..., :-1])
    return wet_pad[1:-1, 1:-1] * (tracer[..., 1:-1, 1:-1] - COURANT * spread)


def operate(field_band, wet_band, damp_core):
    values = pad_north(field_band)
    wetness = pad_north(wet_band)
    masked = wetness * values
    edges = (masked[:-2, 1:-1] + masked[2:, 1:-1]) + (masked[1:-1, :-2] + masked[1:-1, 2:])
    corners = (masked[:-2, :-2] + masked[:-2, 2:]) + (masked[2:, :-2] + masked[2:, 2:])
    centre = values[1:-1, 1:-1]
    wet_core = wetness[1:-1, 1:-1]
    return 0.125 * (wet_core * ((6.0 + damp_core) * centre - (edges + 0.5 * corners)) + (1.0 - wet_core) * centre)


def chebyshev_next(image, current, previous):
    if previous is None:
        return 2.0 * image - current
    return 4.0 * image - 2.0 * current - previous


def shift_table(powers):
    extent = 2 * powers + 1
    table = np.zeros((extent, extent), np.float32)
    for offset, count in ((0, powers), (powers + 1, powers - 1)):
        for place in range(count):
            source = offset + place
            if place == 0:
                table[source + 1, source] = 0.5
                table[source, source] = 0.5
            else:
                table[source + 1, source] = 0.25
                table[source, source] = 0.5
                table[source - 1, source] = 0.25
    return table


def inner_steps(gram, powers):
    extent = 2 * powers + 1
    table = jnp.asarray(shift_table(powers), gram.dtype)
    unit = jnp.eye(extent, dtype=gram.dtype)
    along = unit[0]
    resid = unit[powers + 1]
    offset = jnp.zeros((extent,), gram.dtype)
    for sweep in range(powers):
        norm_now = jnp.dot(resid, jnp.dot(gram, resid, precision=HIGHEST), precision=HIGHEST)
        image = jnp.dot(table, along, precision=HIGHEST)
        alpha = norm_now / jnp.dot(along, jnp.dot(gram, image, precision=HIGHEST), precision=HIGHEST)
        offset = offset + alpha * along
        resid = resid - alpha * image
        norm_next = jnp.dot(resid, jnp.dot(gram, resid, precision=HIGHEST), precision=HIGHEST)
        along = resid + (norm_next / norm_now) * along
    return offset, resid, along


def reference(heat_anomaly, saltiness_anomaly, first_axis_flow, second_axis_flow, layer_spacing, diagonal_shift, water_tile_flags):
    ocean = jnp.repeat(jnp.repeat(water_tile_flags.astype(diagonal_shift.dtype), BX, axis=0), BY, axis=1)
    wet_band = wrap_east(ocean, 1)
    wet_pad = pad_north(wet_band)

    def column_layer_advance(layers):
        padded = [pad_north(wrap_east(layer, 1)) for layer in layers]
        return jnp.stack([advect(tracer, padded[2], padded[3], wet_pad) for tracer in padded])

    stepped_fields = lax.map(column_layer_advance, (heat_anomaly, saltiness_anomaly, first_axis_flow, second_axis_flow))
    weights = layer_spacing / jnp.sum(layer_spacing)
    transport_u = jnp.einsum("k,kxy->xy", weights, stepped_fields[:, 2], precision=HIGHEST)
    transport_v = jnp.einsum("k,kxy->xy", weights, stepped_fields[:, 3], precision=HIGHEST)
    east_band = wrap_east(transport_u, 1)
    north_pad = pad_north(transport_v)
    forcing = ocean * (0.5 * ((east_band[2:] - east_band[:-2]) + (north_pad[:, 2:] - north_pad[:, :-2])))

    def apply_whole(field):
        return operate(wrap_east(field, 1), wet_band, diagonal_shift)

    def chebyshev_list(start, count):
        result = [start]
        previous = None
        for power in range(count):
            following = chebyshev_next(apply_whole(result[-1]), result[-1], previous)
            previous = result[-1]
            result.append(following)
        return result

    height = jnp.zeros_like(forcing)
    resid = forcing
    along = forcing
    for outer in range(CG_BLOCKS):
        along_list = chebyshev_list(along, SSTEP)
        resid_list = chebyshev_list(resid, SSTEP - 1)
        basis = jnp.stack(along_list + resid_list)
        gram = jnp.einsum("aij,bij->ab", basis, basis, precision=HIGHEST)
        offset, resid_coef, along_coef = inner_steps(gram, SSTEP)
        height = height + jnp.einsum("a,aij->ij", offset, basis, precision=HIGHEST)
        resid = jnp.einsum("a,aij->ij", resid_coef, basis, precision=HIGHEST)
        along = jnp.einsum("a,aij->ij", along_coef, basis, precision=HIGHEST)
    return (stepped_fields[:, 0].astype(jnp.bfloat16), stepped_fields[:, 1].astype(jnp.bfloat16),
            stepped_fields[:, 2].astype(jnp.bfloat16), stepped_fields[:, 3].astype(jnp.bfloat16), height, resid)
```

```python
import functools

import jax
import jax.numpy as jnp
import numpy as np
from jax import lax
from jax.experimental import pallas as pl
from jax.experimental.pallas import tpu as pltpu
from jax.sharding import PartitionSpec as P

SSTEP = 4
CG_BLOCKS = 3
SWEEPS = SSTEP * CG_BLOCKS
FIELDS = SWEEPS + 1
MOMENTS = 2 * SWEEPS + 1
COURANT = 0.2
SHIFT = SWEEPS + 2
WEST = -(-(2 * SWEEPS + 2) // 8) * 8
EAST = -(-(SWEEPS + 2) // 8) * 8
F32 = jnp.float32
BF16 = jnp.bfloat16


def shift_table(extent):
    table = np.zeros((extent, extent), np.float32)
    for source in range(extent - 1):
        if source == 0:
            table[1, 0] = table[0, 0] = 0.5
        else:
            table[source + 1, source] = 0.25
            table[source, source] = 0.5
            table[source - 1, source] = 0.25
    return table


def tree(terms):
    while len(terms) > 1:
        terms = [
            terms[i] + terms[i + 1] if i + 1 < len(terms) else terms[i]
            for i in range(0, len(terms), 2)
        ]
    return terms[0]


def quadratic(gram, left, right):
    rows = []
    for i, li in enumerate(left):
        if li is not None:
            rows.append(li * tree([gram[i][j] * rj for j, rj in enumerate(right) if rj is not None]))
    return tree(rows)


def plus(a, b):
    if a is None:
        return b
    if b is None:
        return a
    return a + b


def scaled(scale, a):
    return None if a is None else scale * a


def inner_steps(gram, sweeps):
    extent = sweeps + 1
    table = shift_table(extent)
    one = jnp.ones_like(gram[0][0])
    along = [one] + [None] * sweeps
    resid = [one] + [None] * sweeps
    offset = [None] * extent
    norm_now = quadratic(gram, resid, resid)
    for sweep in range(sweeps):
        image = []
        for i in range(extent):
            total = None
            for j in range(extent):
                if table[i, j] != 0.0:
                    total = plus(total, scaled(float(table[i, j]), along[j]))
            image.append(total)
        alpha = norm_now / quadratic(gram, along, image)
        offset = [plus(o, scaled(alpha, a)) for o, a in zip(offset, along)]
        resid = [plus(r, scaled(-alpha, a)) for r, a in zip(resid, image)]
        if sweep + 1 < sweeps:
            norm_next = quadratic(gram, resid, resid)
            beta = norm_next / norm_now
            along = [plus(r, scaled(beta, a)) for r, a in zip(resid, along)]
            norm_now = norm_next
    return offset, resid


def kernel(
    n,
    heat, salt, uvel, vvel, spacing, damp, flags,
    bh, bs, bu, bv, basis, mom,
    ue, ve, he, se, ef, nf, de, tu, tv, acc, edges,
    uv_tx, hs_tx, uv_rx, hs_rx, aw_tx, ae_tx, a4, fw_tx, fe_tx, fw_rx, fe_rx, slots,
    space, marks,
    lsem, ssem, rsem, gs_sem, gr_sem,
):
    levels, rows, lanes = ue.shape
    me = lax.axis_index("blk")
    right, left = lax.rem(me + 1, n), lax.rem(me + n - 1, n)
    late = rows - WEST
    split = late - 8

    def part(ref, buf, lo, hi, sem):
        return pltpu.make_async_copy(
            ref.at[:, pl.ds(lo, hi - lo)], buf.at[:, pl.ds(lo, hi - lo)], lsem.at[sem]
        )

    loads = [
        pltpu.make_async_copy(flags, marks, lsem.at[0]),
        pltpu.make_async_copy(spacing, space, lsem.at[1]),
        part(uvel, ue, split, rows, 2),
        part(vvel, ve, split, rows, 3),
        pltpu.make_async_copy(damp, de, lsem.at[4]),
        part(uvel, ue, 0, split, 5),
        part(vvel, ve, 0, split, 6),
        pltpu.make_async_copy(heat, he, lsem.at[7]),
        pltpu.make_async_copy(salt, se, lsem.at[8]),
    ]
    for load in loads:
        load.start()

    barrier = pltpu.get_barrier_semaphore()
    for k in range(1, n):
        pl.semaphore_signal(
            barrier, inc=1, device_id={"blk": lax.rem(me + k, n)},
            device_id_type=pl.DeviceIdType.MESH,
        )

    lane = lax.broadcasted_iota(jnp.int32, (8, lanes), 1)
    sub = lax.broadcasted_iota(jnp.int32, (8, lanes), 0)
    top, bottom = sub == 0, sub == 7
    zero = jnp.zeros((8, lanes), F32)

    def north_of(x):
        return pltpu.roll(x, lanes - 1, 1)

    def south_of(x):
        return pltpu.roll(x, 1, 1)

    def sides(x):
        return jnp.where(lane == lanes - 1, 0.0, north_of(x)), jnp.where(lane == 0, 0.0, south_of(x))

    def up_one(x):
        return pltpu.roll(x, 7, 0)

    def down_one(x):
        return pltpu.roll(x, 1, 0)

    loads[0].wait()
    loads[1].wait()
    tiles = marks.shape[1]
    lane_tile = lane // (lanes // tiles)
    own = zero
    for k in range(tiles):
        own = jnp.where(lane_tile == k, marks[0, k].astype(F32), own)
    ahead = jnp.where(lane == lanes - 1, 0.0, own * north_of(own))
    whole_w = jnp.zeros((8, 128), F32)
    for j in range(levels):
        whole_w = whole_w + space[j]
    portions = [jnp.full((8, 128), space[j], F32) / whole_w for j in range(levels)]

    def wide(x):
        return jnp.concatenate([x] * (lanes // 128), axis=1)

    weight = [wide(x) for x in portions]
    level_weight = zero
    for j in range(levels):
        level_weight = jnp.where(sub % levels == j, weight[j], level_weight)

    def gather_row(refs, row):
        block, place = row // 8 * 8, row % 8
        packed = None
        for i, ref in enumerate(refs):
            for level in range(levels):
                x = ref[level, pl.ds(block, 8)]
                spot = i * levels + level
                if (spot - place) % 8:
                    x = pltpu.roll(x, (spot - place) % 8, 0)
                packed = x if packed is None else jnp.where(sub == spot, x, packed)
        return packed

    def pick(packed, block, spot, place):
        return jnp.where(sub == spot, pltpu.roll(block, (spot - place) % 8, 0) if (spot - place) % 8 else block, packed)

    def advect(q, fe, fw, fn):
        return own * (q - (0.5 * COURANT) * ((fe - fw) + (fn - south_of(fn))))

    def flows(first, last, fresh, fields, outs, slot, keep):
        u_like = fields[0]
        ends = [zero, zero]
        for level in range(levels):
            def east_of(r):
                if keep:
                    u0 = u_like[level, pl.ds(r, 8)]
                    if r + 8 < rows:
                        return u0 + jnp.where(bottom, up_one(u_like[level, pl.ds(r + 8, 8)]), up_one(u0))
                    return jnp.where(bottom, 0.0, u0 + up_one(u0))
                return ef[level, pl.ds(r, 8)]

            def flux(ref, r, east):
                q0 = ref[level, pl.ds(r, 8)]
                qp = up_one(q0)
                if r + 8 < rows:
                    qp = jnp.where(bottom, up_one(ref[level, pl.ds(r + 8, 8)]), qp)
                return q0, east * jnp.where(east > 0.0, q0, qp)

            if first == 0:
                before = [zero, zero]
            else:
                e = east_of(first - 8)
                before = [down_one(flux(ref, first - 8, e)[1]) for ref in fields]
            pending = None
            for r in range(first, last, 8):
                here = pl.ds(r, 8)
                east = east_of(r)
                if keep:
                    v0 = fields[1][level, here]
                    north = (v0 + north_of(v0)) * ahead
                    ef[level, here] = east
                    nf[level, here] = north
                else:
                    north = nf[level, here]
                news = []
                for i, ref in enumerate(fields):
                    q0, fe = flux(ref, r, east)
                    shifted = down_one(fe)
                    fw = jnp.where(top, before[i], shifted)
                    before[i] = shifted
                    fn = north * jnp.where(north > 0.0, q0, north_of(q0))
                    new = advect(q0, fe, fw, fn)
                    news.append(new)
                    if keep:
                        total = (tu, tv)[i]
                        term = weight[level] * new
                        total[here] = term if level == 0 else total[here] + term
                    spot = i * levels + level
                    if r == 0:
                        ends[0] = pick(ends[0], new, spot, 0)
                    if r + 8 == rows:
                        ends[1] = pick(ends[1], new, spot, 7)
                if pending is None:
                    pending = news
                else:
                    for i, out in enumerate(outs):
                        out[level, pl.ds(r - 8, 16)] = jnp.concatenate([pending[i], news[i]], axis=0).astype(BF16)
                    pending = None
        if first == 0:
            edges[slot] = ends[0]
        if last == rows:
            edges[slot + 1] = ends[1]

    def forcing(r, low, high):
        t0, x0 = tv[pl.ds(r, 8)], tu[pl.ds(r, 8)]
        north, south = sides(t0)
        after = jnp.where(bottom, up_one(tu[pl.ds(r + 8, 8)]) if r + 8 < high else 0.0, up_one(x0))
        prior = jnp.where(top, down_one(tu[pl.ds(r - 8, 8)]) if r > low else 0.0, down_one(x0))
        return (0.5 * own) * ((after - prior) + (north - south))

    for k in (2, 3):
        loads[k].wait()
    uv_tx[1] = gather_row((ue, ve), rows - 1)
    flows(late, rows, True, (ue, ve), (bu, bv), 0, True)
    for r in range(late, rows, 8):
        f = forcing(r, late, rows)
        if r > late:
            basis[0, pl.ds(WEST + r, 8)] = f
        else:
            f = jnp.where(top, jnp.broadcast_to(tu[pl.ds(rows - 1, 1)], (8, lanes)), f)
        fw_tx[pl.ds(r - late, 8)] = f
    loads[4].wait()
    for r in range(0, rows, 8):
        a = 0.5 * (own * (6.0 + de[pl.ds(r, 8)]) + (1.0 - own)) - 2.0
        a4[pl.ds(WEST + r, 8)] = a
        if r >= late:
            aw_tx[pl.ds(r - late, 8)] = jnp.where(top, own, a) if r == late else a
        if r < EAST:
            ae_tx[pl.ds(r, 8)] = jnp.where(bottom, own, a) if r + 8 == EAST else a

    pl.semaphore_wait(barrier, n - 1)

    def send(k, src, dst, to):
        copy = pltpu.make_async_remote_copy(
            src_ref=src, dst_ref=dst, send_sem=ssem.at[k], recv_sem=rsem.at[k],
            device_id={"blk": to}, device_id_type=pl.DeviceIdType.MESH,
        )
        copy.start()
        return copy

    sent = {}
    sent[0] = send(0, fw_tx, fw_rx, right)
    sent[1] = send(1, uv_tx.at[1], uv_rx.at[0], right)
    sent[2] = send(2, aw_tx, a4.at[pl.ds(0, WEST)], right)

    for k in (5, 6):
        loads[k].wait()
    uv_tx[0] = gather_row((ue, ve), 0)
    sent[3] = send(3, uv_tx.at[0], uv_rx.at[1], left)
    sent[4] = send(4, ae_tx, a4.at[pl.ds(WEST + rows, EAST)], left)
    flows(0, late, True, (ue, ve), (bu, bv), 0, True)
    for r in range(0, late + 8, 8):
        f = forcing(r, 0, rows)
        basis[0, pl.ds(WEST + r, 8)] = f
        if r < EAST:
            if r + 8 == EAST:
                f = jnp.where(bottom, jnp.broadcast_to(tu[pl.ds(0, 1)], (8, lanes)), f)
            fe_tx[pl.ds(r, 8)] = f
    sent[5] = send(5, fe_tx, fe_rx, left)
    for k in (7, 8):
        loads[k].wait()
    hs_tx[0] = gather_row((he, se), 0)
    hs_tx[1] = gather_row((he, se), rows - 1)
    sent[6] = send(6, hs_tx.at[1], hs_rx.at[0], right)
    sent[7] = send(7, hs_tx.at[0], hs_rx.at[1], left)

    window = (-SHIFT, rows - SHIFT)

    def in_window(r, x):
        if r < window[0]:
            return jnp.where(sub >= window[0] - r, x, 0.0)
        if r + 8 > window[1]:
            return jnp.where(sub < window[1] - r, x, 0.0)
        return x

    def fold(x):
        return tree([x[:, c : c + 128] for c in range(0, lanes, 128)])

    def sweep(p, first, last, low, high, wet, summed):
        known = {}

        def block(r):
            if r not in known:
                k0 = basis[p, pl.ds(WEST + r, 8)]
                m = wet(r) * k0
                known[r] = (k0, m, down_one(m), up_one(m))
            return known[r]

        squares, crosses, lasts = [], [], []
        for r in range(first, last, 8):
            k0, m, down, up = block(r)
            prior = block(r - 8)[2] if r > low else down
            after = block(r + 8)[3] if r + 8 < high else up
            vert = jnp.where(top, prior, down) + jnp.where(bottom, after, up)
            north, south = sides(m + 0.5 * vert)
            here = pl.ds(WEST + r, 8)
            half = a4[here] * k0 - (0.5 * wet(r)) * (vert + (north + south))
            new = 0.5 * half if p == 0 else half - basis[p - 1, here]
            basis[p + 1, here] = new
            if summed[0] <= r < summed[1]:
                kept = in_window(r, k0)
                squares.append(kept * kept)
                crosses.append(kept * in_window(r, new))
                if p + 1 == SWEEPS:
                    lasts.append(in_window(r, new) * in_window(r, new))
        return [tree([fold(t) for t in x]) for x in (squares, crosses, lasts) if x]

    def floor8(x):
        return x // 8 * 8

    def ceil8(x):
        return -(-x // 8) * 8

    inner_from, inner_to = ceil8(SWEEPS + 2), rows - SHIFT
    for p in range(SWEEPS):
        j = p + 1
        sums = sweep(
            p, floor8(2 + j), ceil8(rows - 2 - j), 0, rows, lambda r: own, (inner_from, inner_to)
        )
        for i, x in enumerate(sums):
            acc[2 * p + i] = x

    flows(0, rows, True, (he, se), (bh, bs), 2, False)

    def total_of(x):
        for step in (4, 2, 1):
            x = x + pltpu.roll(x, step, 0)
        return x

    def face(low, high, both):
        twice = [jnp.where(sub < levels, x, pltpu.roll(x, levels, 0)) for x in (low, high)]
        return 0.5 * (twice[0] + twice[1]) * both

    def seam(uv_low, uv_high, wet_low, wet_high, tu_low, tu_high, f_low, f_high):
        speed = face(uv_low, uv_high, wet_low * wet_high)
        flux = speed * jnp.where(speed > 0.0, uv_low, uv_high)
        term = level_weight * flux
        gu = total_of(jnp.where(sub < levels, term, 0.0))
        gv = total_of(jnp.where(sub < levels, 0.0, term))
        low_u, high_u = (-COURANT * wet_low) * gu, (COURANT * wet_high) * gu
        low_v, high_v = (-COURANT * wet_low) * gv, (COURANT * wet_high) * gv
        north, south = sides(jnp.where(sub < 4, high_v, low_v))
        across = north - south
        f_low = f_low + (0.5 * wet_low) * jnp.where(
            sub == 7, (tu_high + high_u) + across, jnp.where(sub == 6, low_u, 0.0)
        )
        f_high = f_high + (0.5 * wet_high) * jnp.where(
            sub == 0, across - (tu_low + low_u), jnp.where(sub == 1, -high_u, 0.0)
        )
        return speed, flux, f_low, f_high

    def row_of(ref, row):
        return jnp.broadcast_to(ref[pl.ds(row, 1)], (8, lanes))

    for k in (0, 1, 2):
        sent[k].wait_recv()
    west = row_of(a4, 0)
    speed_w, flux_w, f_low, f_high = seam(
        uv_rx[0], uv_tx[0], west, own, row_of(fw_rx, 0), row_of(tu, 0),
        fw_rx[pl.ds(WEST - 8, 8)], basis[0, pl.ds(WEST, 8)],
    )
    for r in range(0, WEST - 8, 8):
        basis[0, pl.ds(r, 8)] = fw_rx[pl.ds(r, 8)]
    basis[0, pl.ds(WEST - 8, 8)] = f_low
    basis[0, pl.ds(WEST, 8)] = f_high

    moments = [None] * MOMENTS
    base = [None, None]
    for p in range(SWEEPS):
        j = p + 1
        sums = sweep(
            p, floor8(j - 2 * SWEEPS - 2), ceil8(2 + j) if j < SWEEPS else inner_from, -WEST, rows,
            lambda r: west if r < 0 else own, (floor8(-SHIFT), 8),
        )
        for i, x in enumerate(sums):
            moments[2 * p + i] = x
        tail = []
        for r in range(8, inner_from, 8):
            k0, k1 = basis[p, pl.ds(WEST + r, 8)], basis[p + 1, pl.ds(WEST + r, 8)]
            tail.append((k0 * k0, k0 * k1) + ((k1 * k1,) if j == SWEEPS else ()))
        for i in range(len(sums)):
            moments[2 * p + i] = tree(
                [moments[2 * p + i], acc[2 * p + i]] + [fold(t[i]) for t in tail]
            )
    base = moments[:2]
    moments = base + [2.0 * x - base[i % 2] for i, x in enumerate(moments[2:])]
    spread = jnp.zeros((8, 128), F32)
    for i, x in enumerate(moments):
        spread = jnp.where(lane[:, :128] == i, jnp.sum(x, axis=1, keepdims=True), spread)
    slots[me] = jnp.sum(spread, axis=0, keepdims=True)
    copies = []
    for k in range(1, n):
        copy = pltpu.make_async_remote_copy(
            src_ref=slots.at[me], dst_ref=slots.at[me],
            send_sem=gs_sem.at[k], recv_sem=gr_sem.at[k],
            device_id={"blk": lax.rem(me + k, n)}, device_id_type=pl.DeviceIdType.MESH,
        )
        copy.start()
        copies.append(copy)

    for k in (3, 4, 5):
        sent[k].wait_recv()
    east = row_of(a4, WEST + rows + EAST - 1)
    speed_e, flux_e, f_low, f_high = seam(
        uv_tx[1], uv_rx[1], own, east, row_of(tu, rows - 1), row_of(fe_rx, EAST - 1),
        basis[0, pl.ds(WEST + rows - 8, 8)], fe_rx[pl.ds(0, 8)],
    )
    basis[0, pl.ds(WEST + rows - 8, 8)] = f_low
    basis[0, pl.ds(WEST + rows, 8)] = f_high
    for r in range(8, EAST, 8):
        basis[0, pl.ds(WEST + rows + r, 8)] = fe_rx[pl.ds(r, 8)]
    for p in range(SWEEPS):
        j = p + 1
        sweep(
            p, floor8(rows - 2 - j), ceil8(rows + SWEEPS - j), 0, rows + EAST,
            lambda r: own if r < rows else east, (0, 0),
        )

    for k in (6, 7):
        sent[k].wait_recv()

    def mend(outs, fixed, row):
        block, place = row // 8 * 8, row % 8
        for i, out in enumerate(outs):
            for level in range(levels):
                spot = i * levels + level
                old = out[level, pl.ds(block, 8)].astype(F32)
                x = pltpu.roll(fixed, (place - spot) % 8, 0) if (place - spot) % 8 else fixed
                out[level, pl.ds(block, 8)] = jnp.where(sub == place, x, old).astype(BF16)

    def carried(speed, low, high):
        return speed * jnp.where(speed > 0.0, low, high)

    mend((bu, bv), edges[0] + (COURANT * own) * flux_w, 0)
    mend((bu, bv), edges[1] - (COURANT * own) * flux_e, rows - 1)
    mend((bh, bs), edges[2] + (COURANT * own) * carried(speed_w, hs_rx[0], hs_tx[0]), 0)
    mend((bh, bs), edges[3] - (COURANT * own) * carried(speed_e, hs_tx[1], hs_rx[1]), rows - 1)

    for k in range(1, n):
        src = lax.rem(me + n - k, n)
        pltpu.make_async_remote_copy(
            src_ref=slots.at[src], dst_ref=slots.at[src],
            send_sem=gs_sem.at[k], recv_sem=gr_sem.at[k],
            device_id={"blk": src}, device_id_type=pl.DeviceIdType.MESH,
        ).wait_recv()
    mom[...] = jnp.broadcast_to(tree([slots[i] for i in range(n)]), (8, 128))
    for copy in copies:
        copy.wait_send()
    for copy in sent.values():
        copy.wait_send()


def finish(bh, bs, bu, bv, basis, mom, o_heat, o_salt, o_u, o_v, o_height, o_resid, hgt, res, sems):
    rows, lanes = hgt.shape
    stores = [
        pltpu.make_async_copy(src, dst, sems.at[i])
        for i, (src, dst) in enumerate(((bh, o_heat), (bs, o_salt), (bu, o_u), (bv, o_v)))
    ]
    for store in stores:
        store.start()
    row = mom[...]
    m = [jnp.broadcast_to(row[:, i : i + 1], (8, 128)) for i in range(MOMENTS)]
    gram = [[m[a + b] + m[abs(a - b)] for b in range(FIELDS)] for a in range(FIELDS)]
    offset, resid = inner_steps(gram, SWEEPS)

    def combine(vals, coef):
        return tree([c * v for v, c in zip(vals, coef) if c is not None])

    parts = 2
    step = rows // 8 // parts
    for part in range(parts):
        for s in range(part * step, (part + 1) * step):
            r = 8 * s
            for c in range(0, lanes, 128):
                vals = [basis[i, pl.ds(WEST + r, 8), c : c + 128] for i in range(FIELDS)]
                hgt[pl.ds(r, 8), c : c + 128] = combine(vals, offset)
                res[pl.ds(r, 8), c : c + 128] = combine(vals, resid)
        span = pl.ds(part * step * 8, step * 8)
        for i, (src, dst) in enumerate(((hgt, o_height), (res, o_resid))):
            store = pltpu.make_async_copy(src.at[span], dst.at[span], sems.at[4 + 2 * part + i])
            store.start()
            stores.append(store)
    for store in stores:
        store.wait()


def on_device(heat, salt, uvel, vvel, spacing, damp, flags):
    n = lax.axis_size("blk")
    levels, rows, lanes = uvel.shape
    total = WEST + rows + EAST
    hbm = pl.BlockSpec(memory_space=pltpu.HBM)
    vmem = pl.BlockSpec(memory_space=pltpu.VMEM)
    args = [
        pltpu.with_memory_space_constraint(x, pltpu.HBM)
        for x in (heat, salt, uvel, vvel, spacing, damp, flags)
    ]
    vm = pltpu.VMEM
    half = jax.ShapeDtypeStruct((levels, rows, lanes), BF16)
    flat = jax.ShapeDtypeStruct((rows, lanes), F32)
    full = vm((levels, rows, lanes), F32)
    dma = pltpu.SemaphoreType.DMA
    mids = (
        half, half, half, half,
        jax.ShapeDtypeStruct((FIELDS, total, lanes), F32),
        jax.ShapeDtypeStruct((8, 128), F32),
    )
    results = pl.pallas_call(
        functools.partial(kernel, n),
        out_shape=mids,
        in_specs=[hbm] * 7,
        out_specs=(vmem,) * 6,
        scratch_shapes=[
            full, full, full, full, full, full,
            vm((rows, lanes), F32),
            vm((rows, lanes), F32),
            vm((rows, lanes), F32),
            vm((MOMENTS, 8, 128), F32),
            vm((4, 8, lanes), F32),
            vm((2, 8, lanes), F32),
            vm((2, 8, lanes), F32),
            vm((2, 8, lanes), F32),
            vm((2, 8, lanes), F32),
            vm((WEST, lanes), F32),
            vm((EAST, lanes), F32),
            vm((total, lanes), F32),
            vm((WEST, lanes), F32),
            vm((EAST, lanes), F32),
            vm((WEST, lanes), F32),
            vm((EAST, lanes), F32),
            vm((n, 1, 128), F32),
            pltpu.SMEM(spacing.shape, F32),
            pltpu.SMEM(flags.shape, flags.dtype),
            dma((9,)),
            dma((8,)),
            dma((8,)),
            dma((n,)),
            dma((n,)),
        ],
        compiler_params=pltpu.CompilerParams(
            collective_id=0, has_side_effects=True, vmem_limit_bytes=40 * 1024 * 1024
        ),
    )(*args)
    results = [pltpu.with_memory_space_constraint(x, pltpu.VMEM) for x in results]
    shapes = (half, half, half, half, flat, flat)
    return pl.pallas_call(
        finish,
        out_shape=tuple(pltpu.HBM(x.shape, x.dtype) for x in shapes),
        in_specs=[vmem] * 6,
        out_specs=(hbm,) * 6,
        scratch_shapes=[vm((rows, lanes), F32), vm((rows, lanes), F32), dma((8,))],
        compiler_params=pltpu.CompilerParams(vmem_limit_bytes=8 * 1024 * 1024),
    )(*results)


def solution(mesh):
    return jax.shard_map(
        on_device,
        mesh=mesh,
        in_specs=(
            P("member", "blk", None),
            P("member", "blk", None),
            P("member", "blk", None),
            P("member", "blk", None),
            P(),
            P("blk", None),
            P("blk", None),
        ),
        out_specs=(
            P("member", "blk", None),
            P("member", "blk", None),
            P("member", "blk", None),
            P("member", "blk", None),
            P(("member", "blk"), None),
            P(("member", "blk"), None),
        ),
        check_vma=False,
    )
```

```python
import functools

import jax
import jax.numpy as jnp
import numpy as np
from jax import lax
from jax.experimental import pallas as pl
from jax.experimental.pallas import tpu as pltpu
from jax.sharding import PartitionSpec as P

SSTEP = 4
CG_BLOCKS = 3
SWEEPS = SSTEP * CG_BLOCKS
FIELDS = SWEEPS + 1
MOMENTS = 2 * SWEEPS + 1
COURANT = 0.2
SHIFT = SWEEPS + 2
WEST = -(-(2 * SWEEPS + 2) // 8) * 8
EAST = -(-(SWEEPS + 2) // 8) * 8
F32 = jnp.float32
BF16 = jnp.bfloat16


def shift_table(extent):
    table = np.zeros((extent, extent), np.float32)
    for source in range(extent - 1):
        if source == 0:
            table[1, 0] = table[0, 0] = 0.5
        else:
            table[source + 1, source] = 0.25
            table[source, source] = 0.5
            table[source - 1, source] = 0.25
    return table


def tree(terms):
    while len(terms) > 1:
        terms = [
            terms[i] + terms[i + 1] if i + 1 < len(terms) else terms[i]
            for i in range(0, len(terms), 2)
        ]
    return terms[0]


def quadratic(gram, left, right):
    rows = []
    for i, li in enumerate(left):
        if li is not None:
            rows.append(li * tree([gram[i][j] * rj for j, rj in enumerate(right) if rj is not None]))
    return tree(rows)


def plus(a, b):
    if a is None:
        return b
    if b is None:
        return a
    return a + b


def scaled(scale, a):
    return None if a is None else scale * a


def inner_steps(gram, sweeps):
    extent = sweeps + 1
    table = shift_table(extent)
    one = jnp.ones_like(gram[0][0])
    along = [one] + [None] * sweeps
    resid = [one] + [None] * sweeps
    offset = [None] * extent
    norm_now = quadratic(gram, resid, resid)
    for sweep in range(sweeps):
        image = []
        for i in range(extent):
            total = None
            for j in range(extent):
                if table[i, j] != 0.0:
                    total = plus(total, scaled(float(table[i, j]), along[j]))
            image.append(total)
        alpha = norm_now / quadratic(gram, along, image)
        offset = [plus(o, scaled(alpha, a)) for o, a in zip(offset, along)]
        resid = [plus(r, scaled(-alpha, a)) for r, a in zip(resid, image)]
        if sweep + 1 < sweeps:
            norm_next = quadratic(gram, resid, resid)
            beta = norm_next / norm_now
            along = [plus(r, scaled(beta, a)) for r, a in zip(resid, along)]
            norm_now = norm_next
    return offset, resid


def kernel(
    n,
    heat, salt, uvel, vvel, spacing, damp, flags,
    bh, bs, bu, bv, basis, mom,
    ue, ve, he, se, ef, nf, ff, de, tu, tv, acc, edges,
    uv_tx, hs_tx, uv_rx, hs_rx, aw_tx, ae_tx, a4, fw_tx, fe_tx, fw_rx, fe_rx, slots,
    space, marks,
    lsem, ssem, rsem, gs_sem, gr_sem,
):
    levels, rows, lanes = ue.shape
    me = lax.axis_index("blk")
    right, left = lax.rem(me + 1, n), lax.rem(me + n - 1, n)
    late = rows - WEST
    split = late - 8

    def part(ref, buf, lo, hi, sem):
        return pltpu.make_async_copy(
            ref.at[:, pl.ds(lo, hi - lo)], buf.at[:, pl.ds(lo, hi - lo)], lsem.at[sem]
        )

    loads = [
        pltpu.make_async_copy(flags, marks, lsem.at[0]),
        pltpu.make_async_copy(spacing, space, lsem.at[1]),
        part(uvel, ue, split, rows, 2),
        part(vvel, ve, split, rows, 3),
        pltpu.make_async_copy(damp, de, lsem.at[4]),
        part(uvel, ue, 0, split, 5),
        part(vvel, ve, 0, split, 6),
        pltpu.make_async_copy(heat, he, lsem.at[7]),
        pltpu.make_async_copy(salt, se, lsem.at[8]),
    ]
    for load in loads:
        load.start()

    barrier = pltpu.get_barrier_semaphore()
    for k in range(1, n):
        pl.semaphore_signal(
            barrier, inc=1, device_id={"blk": lax.rem(me + k, n)},
            device_id_type=pl.DeviceIdType.MESH,
        )

    lane = lax.broadcasted_iota(jnp.int32, (8, lanes), 1)
    sub = lax.broadcasted_iota(jnp.int32, (8, lanes), 0)
    top, bottom = sub == 0, sub == 7
    zero = jnp.zeros((8, lanes), F32)

    def north_of(x):
        return pltpu.roll(x, lanes - 1, 1)

    def south_of(x):
        return pltpu.roll(x, 1, 1)

    def sides(x):
        return jnp.where(lane == lanes - 1, 0.0, north_of(x)), jnp.where(lane == 0, 0.0, south_of(x))

    def up_one(x):
        return pltpu.roll(x, 7, 0)

    def down_one(x):
        return pltpu.roll(x, 1, 0)

    loads[0].wait()
    loads[1].wait()
    tiles = marks.shape[1]
    lane_tile = lane // (lanes // tiles)
    own = zero
    for k in range(tiles):
        own = jnp.where(lane_tile == k, marks[0, k].astype(F32), own)
    ahead = jnp.where(lane == lanes - 1, 0.0, own * north_of(own))
    whole_w = jnp.zeros((8, 128), F32)
    for j in range(levels):
        whole_w = whole_w + space[j]
    portions = [jnp.full((8, 128), space[j], F32) / whole_w for j in range(levels)]

    def wide(x):
        return jnp.concatenate([x] * (lanes // 128), axis=1)

    weight = [wide(x) for x in portions]
    level_weight = zero
    for j in range(levels):
        level_weight = jnp.where(sub % levels == j, weight[j], level_weight)

    def gather_row(refs, row):
        block, place = row // 8 * 8, row % 8
        packed = None
        for i, ref in enumerate(refs):
            for level in range(levels):
                x = ref[level, pl.ds(block, 8)]
                spot = i * levels + level
                if (spot - place) % 8:
                    x = pltpu.roll(x, (spot - place) % 8, 0)
                packed = x if packed is None else jnp.where(sub == spot, x, packed)
        return packed

    def pick(packed, block, spot, place):
        return jnp.where(sub == spot, pltpu.roll(block, (spot - place) % 8, 0) if (spot - place) % 8 else block, packed)

    def north_flux(first, last, fields, keep):
        for level in range(levels):
            for r in range(first, last, 8):
                here = pl.ds(r, 8)
                q0 = [ref[level, here] for ref in fields]
                qn = [north_of(q) for q in q0]
                if keep:
                    north = (q0[1] + qn[1]) * ahead
                    nf[level, here] = north
                else:
                    north = nf[level, here]
                for i in range(2):
                    ff[i, level, here] = north * jnp.where(north > 0.0, q0[i], qn[i])

    def flows(first, last, fields, outs, slot, keep):
        ends = [zero, zero]
        for level in range(levels):
            def ahead_of(ref, r, q0):
                if r + 8 < rows:
                    return jnp.where(bottom, up_one(ref[level, pl.ds(r + 8, 8)]), up_one(q0))
                return up_one(q0)

            def east_fluxes(r):
                q0 = [ref[level, pl.ds(r, 8)] for ref in fields]
                qp = [ahead_of(ref, r, q) for ref, q in zip(fields, q0)]
                if keep:
                    east = q0[0] + qp[0]
                    if r + 8 == rows:
                        east = jnp.where(bottom, 0.0, east)
                    ef[level, pl.ds(r, 8)] = east
                else:
                    east = ef[level, pl.ds(r, 8)]
                return q0, [east * jnp.where(east > 0.0, a, b) for a, b in zip(q0, qp)]

            before = [zero, zero] if first == 0 else [down_one(f) for f in east_fluxes(first - 8)[1]]
            pending = None
            for r in range(first, last, 8):
                here = pl.ds(r, 8)
                q0, fe = east_fluxes(r)
                news = []
                for i in range(2):
                    shifted = down_one(fe[i])
                    fw = jnp.where(top, before[i], shifted)
                    before[i] = shifted
                    fn = ff[i, level, here]
                    spread = (fe[i] - fw) + (fn - south_of(fn))
                    new = own * (q0[i] - (0.5 * COURANT) * spread)
                    news.append(new)
                    if keep:
                        total = (tu, tv)[i]
                        term = weight[level] * new
                        total[here] = term if level == 0 else total[here] + term
                    spot = i * levels + level
                    if r == 0:
                        ends[0] = pick(ends[0], new, spot, 0)
                    if r + 8 == rows:
                        ends[1] = pick(ends[1], new, spot, 7)
                if pending is None:
                    pending = news
                else:
                    for i, out in enumerate(outs):
                        out[level, pl.ds(r - 8, 16)] = jnp.concatenate([pending[i], news[i]], axis=0).astype(BF16)
                    pending = None
        if first == 0:
            edges[slot] = ends[0]
        if last == rows:
            edges[slot + 1] = ends[1]

    def forcing(r, low, high):
        t0, x0 = tv[pl.ds(r, 8)], tu[pl.ds(r, 8)]
        north, south = sides(t0)
        after = jnp.where(bottom, up_one(tu[pl.ds(r + 8, 8)]) if r + 8 < high else 0.0, up_one(x0))
        prior = jnp.where(top, down_one(tu[pl.ds(r - 8, 8)]) if r > low else 0.0, down_one(x0))
        return (0.5 * own) * ((after - prior) + (north - south))

    for k in (2, 3):
        loads[k].wait()
    uv_tx[1] = gather_row((ue, ve), rows - 1)
    north_flux(late, rows, (ue, ve), True)
    flows(late, rows, (ue, ve), (bu, bv), 0, True)
    for r in range(late, rows, 8):
        f = forcing(r, late, rows)
        if r > late:
            basis[0, pl.ds(WEST + r, 8)] = f
        else:
            f = jnp.where(top, jnp.broadcast_to(tu[pl.ds(rows - 1, 1)], (8, lanes)), f)
        fw_tx[pl.ds(r - late, 8)] = f
    loads[4].wait()
    for r in range(0, rows, 8):
        a = 0.5 * (own * (6.0 + de[pl.ds(r, 8)]) + (1.0 - own)) - 2.0
        a4[pl.ds(WEST + r, 8)] = a
        if r >= late:
            aw_tx[pl.ds(r - late, 8)] = jnp.where(top, own, a) if r == late else a
        if r < EAST:
            ae_tx[pl.ds(r, 8)] = jnp.where(bottom, own, a) if r + 8 == EAST else a

    pl.semaphore_wait(barrier, n - 1)

    def send(k, src, dst, to):
        copy = pltpu.make_async_remote_copy(
            src_ref=src, dst_ref=dst, send_sem=ssem.at[k], recv_sem=rsem.at[k],
            device_id={"blk": to}, device_id_type=pl.DeviceIdType.MESH,
        )
        copy.start()
        return copy

    sent = {}
    sent[0] = send(0, fw_tx, fw_rx, right)
    sent[1] = send(1, uv_tx.at[1], uv_rx.at[0], right)
    sent[2] = send(2, aw_tx, a4.at[pl.ds(0, WEST)], right)

    for k in (5, 6):
        loads[k].wait()
    uv_tx[0] = gather_row((ue, ve), 0)
    sent[3] = send(3, uv_tx.at[0], uv_rx.at[1], left)
    sent[4] = send(4, ae_tx, a4.at[pl.ds(WEST + rows, EAST)], left)
    north_flux(0, late, (ue, ve), True)
    flows(0, late, (ue, ve), (bu, bv), 0, True)
    for r in range(0, late + 8, 8):
        f = forcing(r, 0, rows)
        basis[0, pl.ds(WEST + r, 8)] = f
        if r < EAST:
            if r + 8 == EAST:
                f = jnp.where(bottom, jnp.broadcast_to(tu[pl.ds(0, 1)], (8, lanes)), f)
            fe_tx[pl.ds(r, 8)] = f
    sent[5] = send(5, fe_tx, fe_rx, left)
    for k in (7, 8):
        loads[k].wait()
    hs_tx[0] = gather_row((he, se), 0)
    hs_tx[1] = gather_row((he, se), rows - 1)
    sent[6] = send(6, hs_tx.at[1], hs_rx.at[0], right)
    sent[7] = send(7, hs_tx.at[0], hs_rx.at[1], left)

    window = (-SHIFT, rows - SHIFT)

    def in_window(r, x):
        if r < window[0]:
            return jnp.where(sub >= window[0] - r, x, 0.0)
        if r + 8 > window[1]:
            return jnp.where(sub < window[1] - r, x, 0.0)
        return x

    def fold(x):
        return tree([x[:, c : c + 128] for c in range(0, lanes, 128)])

    def sweep(p, first, last, low, high, wet, summed):
        known = {}

        def block(r):
            if r not in known:
                k0 = basis[p, pl.ds(WEST + r, 8)]
                m = wet(r) * k0
                known[r] = (k0, m, down_one(m), up_one(m))
            return known[r]

        squares, crosses, lasts = [], [], []
        for r in range(first, last, 8):
            k0, m, down, up = block(r)
            prior = block(r - 8)[2] if r > low else down
            after = block(r + 8)[3] if r + 8 < high else up
            vert = jnp.where(top, prior, down) + jnp.where(bottom, after, up)
            north, south = sides(m + 0.5 * vert)
            here = pl.ds(WEST + r, 8)
            half = a4[here] * k0 - (0.5 * wet(r)) * (vert + (north + south))
            new = 0.5 * half if p == 0 else half - basis[p - 1, here]
            basis[p + 1, here] = new
            if summed[0] <= r < summed[1]:
                kept = in_window(r, k0)
                squares.append(kept * kept)
                crosses.append(kept * in_window(r, new))
                if p + 1 == SWEEPS:
                    lasts.append(in_window(r, new) * in_window(r, new))
        return [tree([fold(t) for t in x]) for x in (squares, crosses, lasts) if x]

    def floor8(x):
        return x // 8 * 8

    def ceil8(x):
        return -(-x // 8) * 8

    inner_from, inner_to = ceil8(SWEEPS + 2), rows - SHIFT
    for p in range(SWEEPS):
        j = p + 1
        sums = sweep(
            p, floor8(2 + j), ceil8(rows - 2 - j), 0, rows, lambda r: own, (inner_from, inner_to)
        )
        for i, x in enumerate(sums):
            acc[2 * p + i] = x

    north_flux(0, rows, (he, se), False)
    flows(0, rows, (he, se), (bh, bs), 2, False)

    def total_of(x):
        for step in (4, 2, 1):
            x = x + pltpu.roll(x, step, 0)
        return x

    def face(low, high, both):
        twice = [jnp.where(sub < levels, x, pltpu.roll(x, levels, 0)) for x in (low, high)]
        return 0.5 * (twice[0] + twice[1]) * both

    def seam(uv_low, uv_high, wet_low, wet_high, tu_low, tu_high, f_low, f_high):
        speed = face(uv_low, uv_high, wet_low * wet_high)
        flux = speed * jnp.where(speed > 0.0, uv_low, uv_high)
        term = level_weight * flux
        gu = total_of(jnp.where(sub < levels, term, 0.0))
        gv = total_of(jnp.where(sub < levels, 0.0, term))
        low_u, high_u = (-COURANT * wet_low) * gu, (COURANT * wet_high) * gu
        low_v, high_v = (-COURANT * wet_low) * gv, (COURANT * wet_high) * gv
        north, south = sides(jnp.where(sub < 4, high_v, low_v))
        across = north - south
        f_low = f_low + (0.5 * wet_low) * jnp.where(
            sub == 7, (tu_high + high_u) + across, jnp.where(sub == 6, low_u, 0.0)
        )
        f_high = f_high + (0.5 * wet_high) * jnp.where(
            sub == 0, across - (tu_low + low_u), jnp.where(sub == 1, -high_u, 0.0)
        )
        return speed, flux, f_low, f_high

    def row_of(ref, row):
        return jnp.broadcast_to(ref[pl.ds(row, 1)], (8, lanes))

    for k in (0, 1, 2):
        sent[k].wait_recv()
    west = row_of(a4, 0)
    speed_w, flux_w, f_low, f_high = seam(
        uv_rx[0], uv_tx[0], west, own, row_of(fw_rx, 0), row_of(tu, 0),
        fw_rx[pl.ds(WEST - 8, 8)], basis[0, pl.ds(WEST, 8)],
    )
    for r in range(0, WEST - 8, 8):
        basis[0, pl.ds(r, 8)] = fw_rx[pl.ds(r, 8)]
    basis[0, pl.ds(WEST - 8, 8)] = f_low
    basis[0, pl.ds(WEST, 8)] = f_high

    moments = [None] * MOMENTS
    base = [None, None]
    for p in range(SWEEPS):
        j = p + 1
        sums = sweep(
            p, floor8(j - 2 * SWEEPS - 2), ceil8(2 + j) if j < SWEEPS else inner_from, -WEST, rows,
            lambda r: west if r < 0 else own, (floor8(-SHIFT), 8),
        )
        for i, x in enumerate(sums):
            moments[2 * p + i] = x
        tail = []
        for r in range(8, inner_from, 8):
            k0, k1 = basis[p, pl.ds(WEST + r, 8)], basis[p + 1, pl.ds(WEST + r, 8)]
            tail.append((k0 * k0, k0 * k1) + ((k1 * k1,) if j == SWEEPS else ()))
        for i in range(len(sums)):
            moments[2 * p + i] = tree(
                [moments[2 * p + i], acc[2 * p + i]] + [fold(t[i]) for t in tail]
            )
    base = moments[:2]
    moments = base + [2.0 * x - base[i % 2] for i, x in enumerate(moments[2:])]
    spread = jnp.zeros((8, 128), F32)
    for i, x in enumerate(moments):
        spread = jnp.where(lane[:, :128] == i, jnp.sum(x, axis=1, keepdims=True), spread)
    slots[me] = jnp.sum(spread, axis=0, keepdims=True)
    copies = []
    for k in range(1, n):
        copy = pltpu.make_async_remote_copy(
            src_ref=slots.at[me], dst_ref=slots.at[me],
            send_sem=gs_sem.at[k], recv_sem=gr_sem.at[k],
            device_id={"blk": lax.rem(me + k, n)}, device_id_type=pl.DeviceIdType.MESH,
        )
        copy.start()
        copies.append(copy)

    for k in (3, 4, 5):
        sent[k].wait_recv()
    east = row_of(a4, WEST + rows + EAST - 1)
    speed_e, flux_e, f_low, f_high = seam(
        uv_tx[1], uv_rx[1], own, east, row_of(tu, rows - 1), row_of(fe_rx, EAST - 1),
        basis[0, pl.ds(WEST + rows - 8, 8)], fe_rx[pl.ds(0, 8)],
    )
    basis[0, pl.ds(WEST + rows - 8, 8)] = f_low
    basis[0, pl.ds(WEST + rows, 8)] = f_high
    for r in range(8, EAST, 8):
        basis[0, pl.ds(WEST + rows + r, 8)] = fe_rx[pl.ds(r, 8)]
    for p in range(SWEEPS):
        j = p + 1
        sweep(
            p, floor8(rows - 2 - j), ceil8(rows + SWEEPS - j), 0, rows + EAST,
            lambda r: own if r < rows else east, (0, 0),
        )

    for k in (6, 7):
        sent[k].wait_recv()

    def mend(outs, fixed, row):
        block, place = row // 8 * 8, row % 8
        for i, out in enumerate(outs):
            for level in range(levels):
                spot = i * levels + level
                old = out[level, pl.ds(block, 8)].astype(F32)
                x = pltpu.roll(fixed, (place - spot) % 8, 0) if (place - spot) % 8 else fixed
                out[level, pl.ds(block, 8)] = jnp.where(sub == place, x, old).astype(BF16)

    def carried(speed, low, high):
        return speed * jnp.where(speed > 0.0, low, high)

    mend((bu, bv), edges[0] + (COURANT * own) * flux_w, 0)
    mend((bu, bv), edges[1] - (COURANT * own) * flux_e, rows - 1)
    mend((bh, bs), edges[2] + (COURANT * own) * carried(speed_w, hs_rx[0], hs_tx[0]), 0)
    mend((bh, bs), edges[3] - (COURANT * own) * carried(speed_e, hs_tx[1], hs_rx[1]), rows - 1)

    for k in range(1, n):
        src = lax.rem(me + n - k, n)
        pltpu.make_async_remote_copy(
            src_ref=slots.at[src], dst_ref=slots.at[src],
            send_sem=gs_sem.at[k], recv_sem=gr_sem.at[k],
            device_id={"blk": src}, device_id_type=pl.DeviceIdType.MESH,
        ).wait_recv()
    mom[...] = jnp.broadcast_to(tree([slots[i] for i in range(n)]), (8, 128))
    for copy in copies:
        copy.wait_send()
    for copy in sent.values():
        copy.wait_send()


def finish(bh, bs, bu, bv, basis, mom, o_heat, o_salt, o_u, o_v, o_height, o_resid, hgt, res, sems):
    rows, lanes = hgt.shape
    stores = [
        pltpu.make_async_copy(src, dst, sems.at[i])
        for i, (src, dst) in enumerate(((bh, o_heat), (bs, o_salt), (bu, o_u), (bv, o_v)))
    ]
    for store in stores:
        store.start()
    row = mom[...]
    m = [jnp.broadcast_to(row[:, i : i + 1], (8, 128)) for i in range(MOMENTS)]
    gram = [[m[a + b] + m[abs(a - b)] for b in range(FIELDS)] for a in range(FIELDS)]
    offset, resid = inner_steps(gram, SWEEPS)

    def combine(vals, coef):
        return tree([c * v for v, c in zip(vals, coef) if c is not None])

    parts = 2
    step = rows // 8 // parts
    for part in range(parts):
        for s in range(part * step, (part + 1) * step):
            r = 8 * s
            for c in range(0, lanes, 128):
                vals = [basis[i, pl.ds(WEST + r, 8), c : c + 128] for i in range(FIELDS)]
                hgt[pl.ds(r, 8), c : c + 128] = combine(vals, offset)
                res[pl.ds(r, 8), c : c + 128] = combine(vals, resid)
        span = pl.ds(part * step * 8, step * 8)
        for i, (src, dst) in enumerate(((hgt, o_height), (res, o_resid))):
            store = pltpu.make_async_copy(src.at[span], dst.at[span], sems.at[4 + 2 * part + i])
            store.start()
            stores.append(store)
    for store in stores:
        store.wait()


def on_device(heat, salt, uvel, vvel, spacing, damp, flags):
    n = lax.axis_size("blk")
    levels, rows, lanes = uvel.shape
    total = WEST + rows + EAST
    hbm = pl.BlockSpec(memory_space=pltpu.HBM)
    vmem = pl.BlockSpec(memory_space=pltpu.VMEM)
    args = [
        pltpu.with_memory_space_constraint(x, pltpu.HBM)
        for x in (heat, salt, uvel, vvel, spacing, damp, flags)
    ]
    vm = pltpu.VMEM
    half = jax.ShapeDtypeStruct((levels, rows, lanes), BF16)
    flat = jax.ShapeDtypeStruct((rows, lanes), F32)
    full = vm((levels, rows, lanes), F32)
    dma = pltpu.SemaphoreType.DMA
    mids = (
        half, half, half, half,
        jax.ShapeDtypeStruct((FIELDS, total, lanes), F32),
        jax.ShapeDtypeStruct((8, 128), F32),
    )
    results = pl.pallas_call(
        functools.partial(kernel, n),
        out_shape=mids,
        in_specs=[hbm] * 7,
        out_specs=(vmem,) * 6,
        scratch_shapes=[
            full, full, full, full, full, full,
            vm((2, levels, rows, lanes), F32),
            vm((rows, lanes), F32),
            vm((rows, lanes), F32),
            vm((rows, lanes), F32),
            vm((MOMENTS, 8, 128), F32),
            vm((4, 8, lanes), F32),
            vm((2, 8, lanes), F32),
            vm((2, 8, lanes), F32),
            vm((2, 8, lanes), F32),
            vm((2, 8, lanes), F32),
            vm((WEST, lanes), F32),
            vm((EAST, lanes), F32),
            vm((total, lanes), F32),
            vm((WEST, lanes), F32),
            vm((EAST, lanes), F32),
            vm((WEST, lanes), F32),
            vm((EAST, lanes), F32),
            vm((n, 1, 128), F32),
            pltpu.SMEM(spacing.shape, F32),
            pltpu.SMEM(flags.shape, flags.dtype),
            dma((9,)),
            dma((8,)),
            dma((8,)),
            dma((n,)),
            dma((n,)),
        ],
        compiler_params=pltpu.CompilerParams(
            collective_id=0, has_side_effects=True, vmem_limit_bytes=40 * 1024 * 1024
        ),
    )(*args)
    results = [pltpu.with_memory_space_constraint(x, pltpu.VMEM) for x in results]
    shapes = (half, half, half, half, flat, flat)
    return pl.pallas_call(
        finish,
        out_shape=tuple(pltpu.HBM(x.shape, x.dtype) for x in shapes),
        in_specs=[vmem] * 6,
        out_specs=(hbm,) * 6,
        scratch_shapes=[vm((rows, lanes), F32), vm((rows, lanes), F32), dma((8,))],
        compiler_params=pltpu.CompilerParams(vmem_limit_bytes=8 * 1024 * 1024),
    )(*results)


def solution(mesh):
    return jax.shard_map(
        on_device,
        mesh=mesh,
        in_specs=(
            P("member", "blk", None),
            P("member", "blk", None),
            P("member", "blk", None),
            P("member", "blk", None),
            P(),
            P("blk", None),
            P("blk", None),
        ),
        out_specs=(
            P("member", "blk", None),
            P("member", "blk", None),
            P("member", "blk", None),
            P("member", "blk", None),
            P(("member", "blk"), None),
            P(("member", "blk"), None),
        ),
        check_vma=False,
    )
```

```python
import functools

import jax
import jax.numpy as jnp
import numpy as np
from jax import lax
from jax.experimental import pallas as pl
from jax.experimental.pallas import tpu as pltpu
from jax.sharding import PartitionSpec as P

SSTEP = 4
CG_BLOCKS = 3
SWEEPS = SSTEP * CG_BLOCKS
FIELDS = SWEEPS + 1
MOMENTS = 2 * SWEEPS + 1
COURANT = 0.2
SHIFT = SWEEPS + 2
WEST = -(-(2 * SWEEPS + 2) // 8) * 8
EAST = -(-(SWEEPS + 2) // 8) * 8
F32 = jnp.float32
BF16 = jnp.bfloat16


def shift_table(extent):
    table = np.zeros((extent, extent), np.float32)
    for source in range(extent - 1):
        if source == 0:
            table[1, 0] = table[0, 0] = 0.5
        else:
            table[source + 1, source] = 0.25
            table[source, source] = 0.5
            table[source - 1, source] = 0.25
    return table


def tree(terms):
    while len(terms) > 1:
        terms = [
            terms[i] + terms[i + 1] if i + 1 < len(terms) else terms[i]
            for i in range(0, len(terms), 2)
        ]
    return terms[0]


def quadratic(gram, left, right):
    rows = []
    for i, li in enumerate(left):
        if li is not None:
            rows.append(li * tree([gram[i][j] * rj for j, rj in enumerate(right) if rj is not None]))
    return tree(rows)


def plus(a, b):
    if a is None:
        return b
    if b is None:
        return a
    return a + b


def scaled(scale, a):
    return None if a is None else scale * a


def inner_steps(gram, sweeps):
    extent = sweeps + 1
    table = shift_table(extent)
    one = jnp.ones_like(gram[0][0])
    along = [one] + [None] * sweeps
    resid = [one] + [None] * sweeps
    offset = [None] * extent
    norm_now = gram[0][0]
    for sweep in range(sweeps):
        image = []
        for i in range(extent):
            total = None
            for j in range(extent):
                if table[i, j] != 0.0:
                    total = plus(total, scaled(float(table[i, j]), along[j]))
            image.append(total)
        scale = 1.0 / norm_now
        alpha = norm_now / quadratic(gram, along, image)
        offset = [plus(o, scaled(alpha, a)) for o, a in zip(offset, along)]
        resid = [plus(r, scaled(-alpha, a)) for r, a in zip(resid, image)]
        if sweep + 1 < sweeps:
            norm_next = quadratic(gram, resid, resid)
            beta = norm_next * scale
            along = [plus(r, scaled(beta, a)) for r, a in zip(resid, along)]
            norm_now = norm_next
    return offset, resid


def kernel(
    n,
    heat, salt, uvel, vvel, spacing, damp, flags,
    bh, bs, bu, bv, basis, mom,
    ue, ve, he, se, ef, nf, ff, de, tu, tv, acc, edges,
    uv_tx, hs_tx, uv_rx, hs_rx, aw_tx, ae_tx, a4, fw_tx, fe_tx, fw_rx, fe_rx, slots,
    space, marks,
    flux_e, lsem, ssem, rsem, gsem, late_sem,
):
    levels, rows, lanes = ue.shape
    me = lax.axis_index("blk")
    right, left = lax.rem(me + 1, n), lax.rem(me + n - 1, n)
    late = rows - WEST
    split = late - 8

    def part(ref, buf, lo, hi, sem):
        return pltpu.make_async_copy(
            ref.at[:, pl.ds(lo, hi - lo)], buf.at[:, pl.ds(lo, hi - lo)], lsem.at[sem]
        )

    def pair(lo, hi, sem):
        both = ff.at[:, :, pl.ds(lo, hi - lo)]
        return pltpu.make_async_copy(both, both, lsem.at[sem])

    loads = [
        pltpu.make_async_copy(flags, marks, lsem.at[0]),
        pltpu.make_async_copy(spacing, space, lsem.at[1]),
        part(uvel, ue, split, rows, 2),
        part(vvel, ve, split, rows, 2),
        pltpu.make_async_copy(damp, de, lsem.at[3]),
        part(uvel, ue, 0, split, 4),
        part(vvel, ve, 0, split, 4),
    ]
    more = [
        pltpu.make_async_copy(heat, he, lsem.at[5]),
        pltpu.make_async_copy(salt, se, lsem.at[5]),
    ]
    for load in loads[:4]:
        load.start()

    barrier = pltpu.get_barrier_semaphore()

    def tell(sem, to):
        pl.semaphore_signal(
            sem, inc=1, device_id={"blk": to}, device_id_type=pl.DeviceIdType.MESH
        )

    at_start, at_end = me == 0, me == n - 1
    pl.when(me > 0)(lambda: tell(barrier, left))
    for k in range(1, n):
        pl.when(me + k < n)(functools.partial(tell, barrier, lax.rem(me + k, n)))
    for load in loads[4:]:
        load.start()

    def pass_barrier():
        pl.semaphore_wait(barrier, jnp.where(at_end, n - 1, me + 1))
        for k in range(2, n):
            pl.when(me - k >= 0)(functools.partial(tell, late_sem.at[0], lax.rem(me + n - k, n)))

    def hear_late():
        later = n - 2 - me
        pl.when(later > 0)(lambda: pl.semaphore_wait(late_sem.at[0], later))

    lane = lax.broadcasted_iota(jnp.int32, (8, lanes), 1)
    sub = lax.broadcasted_iota(jnp.int32, (8, lanes), 0)
    top, bottom = sub == 0, sub == 7
    zero = jnp.zeros((8, lanes), F32)

    def north_of(x):
        return pltpu.roll(x, lanes - 1, 1)

    def south_of(x):
        return pltpu.roll(x, 1, 1)

    def sides(x):
        return jnp.where(lane == lanes - 1, 0.0, north_of(x)), jnp.where(lane == 0, 0.0, south_of(x))

    def up_one(x):
        return pltpu.roll(x, 7, 0)

    def down_one(x):
        return pltpu.roll(x, 1, 0)

    loads[0].wait()
    loads[1].wait()
    tiles = marks.shape[1]
    lane_tile = lane // (lanes // tiles)
    own = zero
    for k in range(tiles):
        own = jnp.where(lane_tile == k, marks[0, k].astype(F32), own)
    ahead = jnp.where(lane == lanes - 1, 0.0, own * north_of(own))
    whole_w = jnp.zeros((8, 128), F32)
    for j in range(levels):
        whole_w = whole_w + space[j]
    portions = [jnp.full((8, 128), space[j], F32) / whole_w for j in range(levels)]

    def wide(x):
        return jnp.concatenate([x] * (lanes // 128), axis=1)

    weight = [wide(x) for x in portions]
    level_weight = zero
    for j in range(levels):
        level_weight = jnp.where(sub % levels == j, weight[j], level_weight)

    def gather_row(refs, row):
        block, place = row // 8 * 8, row % 8
        packed = None
        for i, ref in enumerate(refs):
            for level in range(levels):
                x = ref[level, pl.ds(block, 8)]
                spot = i * levels + level
                if (spot - place) % 8:
                    x = pltpu.roll(x, (spot - place) % 8, 0)
                packed = x if packed is None else jnp.where(sub == spot, x, packed)
        return packed

    def pick(packed, block, spot, place):
        return jnp.where(sub == spot, pltpu.roll(block, (spot - place) % 8, 0) if (spot - place) % 8 else block, packed)

    def north_flux(first, last, fields, keep):
        for level in range(levels):
            for r in range(first, last, 8):
                here = pl.ds(r, 8)
                q0 = [ref[level, here] for ref in fields]
                qn = [north_of(q) for q in q0]
                if keep:
                    north = (q0[1] + qn[1]) * ahead
                    nf[level, here] = north
                else:
                    north = nf[level, here]
                for i in range(2):
                    ff[i, level, here] = north * jnp.where(north > 0.0, q0[i], qn[i])

    def flows(first, last, fields, outs, slot, keep):
        ends = [zero, zero]
        for level in range(levels):
            def ahead_of(ref, r, q0):
                if r + 8 < rows:
                    return jnp.where(bottom, up_one(ref[level, pl.ds(r + 8, 8)]), up_one(q0))
                return up_one(q0)

            def east_fluxes(r):
                q0 = [ref[level, pl.ds(r, 8)] for ref in fields]
                qp = [ahead_of(ref, r, q) for ref, q in zip(fields, q0)]
                if keep:
                    east = q0[0] + qp[0]
                    if r + 8 == rows:
                        east = jnp.where(bottom, 0.0, east)
                    ef[level, pl.ds(r, 8)] = east
                else:
                    east = ef[level, pl.ds(r, 8)]
                return q0, [east * jnp.where(east > 0.0, a, b) for a, b in zip(q0, qp)]

            before = [zero, zero] if first == 0 else [down_one(f) for f in east_fluxes(first - 8)[1]]
            pending = None
            for r in range(first, last, 8):
                here = pl.ds(r, 8)
                q0, fe = east_fluxes(r)
                news = []
                for i in range(2):
                    shifted = down_one(fe[i])
                    fw = jnp.where(top, before[i], shifted)
                    before[i] = shifted
                    fn = ff[i, level, here]
                    spread = (fe[i] - fw) + (fn - south_of(fn))
                    new = own * (q0[i] - (0.5 * COURANT) * spread)
                    news.append(new)
                    if keep:
                        total = (tu, tv)[i]
                        term = weight[level] * new
                        total[here] = term if level == 0 else total[here] + term
                    spot = i * levels + level
                    if r == 0:
                        ends[0] = pick(ends[0], new, spot, 0)
                    if r + 8 == rows:
                        ends[1] = pick(ends[1], new, spot, 7)
                if pending is None:
                    pending = news
                else:
                    for i, out in enumerate(outs):
                        out[level, pl.ds(r - 8, 16)] = jnp.concatenate([pending[i], news[i]], axis=0).astype(BF16)
                    pending = None
        if first == 0:
            edges[slot] = ends[0]
        if last == rows:
            edges[slot + 1] = ends[1]

    def forcing(r, low, high):
        t0, x0 = tv[pl.ds(r, 8)], tu[pl.ds(r, 8)]
        north, south = sides(t0)
        after = jnp.where(bottom, up_one(tu[pl.ds(r + 8, 8)]) if r + 8 < high else 0.0, up_one(x0))
        prior = jnp.where(top, down_one(tu[pl.ds(r - 8, 8)]) if r > low else 0.0, down_one(x0))
        return (0.5 * own) * ((after - prior) + (north - south))

    def send(src, dst, sem, to):
        pltpu.make_async_remote_copy(
            src_ref=src, dst_ref=dst, send_sem=ssem.at[0], recv_sem=rsem.at[sem],
            device_id={"blk": to}, device_id_type=pl.DeviceIdType.MESH,
        ).start()

    def arrive(sem, height):
        lot = a4.at[pl.ds(0, height)]
        pltpu.make_async_remote_copy(
            src_ref=lot, dst_ref=lot, send_sem=ssem.at[0], recv_sem=rsem.at[sem],
            device_id={"blk": right}, device_id_type=pl.DeviceIdType.MESH,
        ).wait_recv()

    def send_left():
        send(uv_tx.at[0], uv_rx.at[1], 1, left)
        send(ae_tx, a4.at[pl.ds(WEST + rows, EAST)], 1, left)
        send(fe_tx, fe_rx, 1, left)

    pair(split, rows, 2).wait()
    for load in more:
        load.start()
    uv_tx[1] = gather_row((ue, ve), rows - 1)
    loads[4].wait()
    for r in range(0, rows, 8):
        a = 0.5 * (own * (6.0 + de[pl.ds(r, 8)]) + (1.0 - own)) - 2.0
        a4[pl.ds(WEST + r, 8)] = a
        if r >= late:
            aw_tx[pl.ds(r - late, 8)] = jnp.where(top, own, a) if r == late else a
        if r < EAST:
            ae_tx[pl.ds(r, 8)] = jnp.where(bottom, own, a) if r + 8 == EAST else a
    pass_barrier()
    send(uv_tx.at[1], uv_rx.at[0], 0, right)
    send(aw_tx, a4.at[pl.ds(0, WEST)], 0, right)
    north_flux(late, rows, (ue, ve), True)
    flows(late, rows, (ue, ve), (bu, bv), 0, True)
    for r in range(late, rows, 8):
        f = forcing(r, late, rows)
        if r > late:
            basis[0, pl.ds(WEST + r, 8)] = f
        else:
            f = jnp.where(top, jnp.broadcast_to(tu[pl.ds(rows - 1, 1)], (8, lanes)), f)
        fw_tx[pl.ds(r - late, 8)] = f
    send(fw_tx, fw_rx, 0, right)

    pair(0, split, 4).wait()
    uv_tx[0] = gather_row((ue, ve), 0)
    north_flux(0, late, (ue, ve), True)
    flows(0, late, (ue, ve), (bu, bv), 0, True)
    for r in range(0, late + 8, 8):
        f = forcing(r, 0, rows)
        basis[0, pl.ds(WEST + r, 8)] = f
        if r < EAST:
            if r + 8 == EAST:
                f = jnp.where(bottom, jnp.broadcast_to(tu[pl.ds(0, 1)], (8, lanes)), f)
            fe_tx[pl.ds(r, 8)] = f
    pl.when(me > 0)(send_left)

    window = (-SHIFT, rows - SHIFT)

    def in_window(r, x):
        if r < window[0]:
            return jnp.where(sub >= window[0] - r, x, 0.0)
        if r + 8 > window[1]:
            return jnp.where(sub < window[1] - r, x, 0.0)
        return x

    def fold(x):
        return tree([x[:, c : c + 128] for c in range(0, lanes, 128)])

    def sweep(p, first, last, low, high, wet, summed):
        known = {}

        def block(r):
            if r not in known:
                k0 = basis[p, pl.ds(WEST + r, 8)]
                m = wet(r) * k0
                known[r] = (k0, m, down_one(m), up_one(m))
            return known[r]

        squares, crosses, lasts = [], [], []
        for r in range(first, last, 8):
            k0, m, down, up = block(r)
            prior = block(r - 8)[2] if r > low else down
            after = block(r + 8)[3] if r + 8 < high else up
            vert = jnp.where(top, prior, down) + jnp.where(bottom, after, up)
            north, south = sides(m + 0.5 * vert)
            here = pl.ds(WEST + r, 8)
            half = a4[here] * k0 - (0.5 * wet(r)) * (vert + (north + south))
            new = 0.5 * half if p == 0 else half - basis[p - 1, here]
            basis[p + 1, here] = new
            if summed[0] <= r < summed[1]:
                kept = in_window(r, k0)
                squares.append(kept * kept)
                crosses.append(kept * in_window(r, new))
                if p + 1 == SWEEPS:
                    lasts.append(in_window(r, new) * in_window(r, new))
        return [tree([fold(t) for t in x]) for x in (squares, crosses, lasts) if x]

    def floor8(x):
        return x // 8 * 8

    def ceil8(x):
        return -(-x // 8) * 8

    inner_from, inner_to = ceil8(SWEEPS + 2), rows - SHIFT
    for p in range(SWEEPS):
        j = p + 1
        sums = sweep(
            p, floor8(2 + j), ceil8(rows - 2 - j), 0, rows, lambda r: own, (inner_from, inner_to)
        )
        for i, x in enumerate(sums):
            acc[2 * p + i] = x

    pltpu.make_async_copy(ff, ff, lsem.at[5]).wait()
    hs_tx[0] = gather_row((he, se), 0)
    hs_tx[1] = gather_row((he, se), rows - 1)
    send(hs_tx.at[1], hs_rx.at[0], 2, right)
    pl.when(me > 0)(lambda: send(hs_tx.at[0], hs_rx.at[1], 2, left))

    def tracers():
        north_flux(0, rows, (he, se), False)
        flows(0, rows, (he, se), (bh, bs), 2, False)

    def total_of(x):
        for step in (4, 2, 1):
            x = x + pltpu.roll(x, step, 0)
        return x

    def face(low, high, both):
        twice = [jnp.where(sub < levels, x, pltpu.roll(x, levels, 0)) for x in (low, high)]
        return 0.5 * (twice[0] + twice[1]) * both

    def seam(uv_low, uv_high, wet_low, wet_high, tu_low, tu_high, f_low, f_high):
        speed = face(uv_low, uv_high, wet_low * wet_high)
        flux = speed * jnp.where(speed > 0.0, uv_low, uv_high)
        term = level_weight * flux
        gu = total_of(jnp.where(sub < levels, term, 0.0))
        gv = total_of(jnp.where(sub < levels, 0.0, term))
        low_u, high_u = (-COURANT * wet_low) * gu, (COURANT * wet_high) * gu
        low_v, high_v = (-COURANT * wet_low) * gv, (COURANT * wet_high) * gv
        north, south = sides(jnp.where(sub < 4, high_v, low_v))
        across = north - south
        f_low = f_low + (0.5 * wet_low) * jnp.where(
            sub == 7, (tu_high + high_u) + across, jnp.where(sub == 6, low_u, 0.0)
        )
        f_high = f_high + (0.5 * wet_high) * jnp.where(
            sub == 0, across - (tu_low + low_u), jnp.where(sub == 1, -high_u, 0.0)
        )
        return speed, flux, f_low, f_high

    def row_of(ref, row):
        return jnp.broadcast_to(ref[pl.ds(row, 1)], (8, lanes))

    def tracers_and_east(both=True):
        if both:
            tracers()
        arrive(1, 2 * EAST + 8)
        east = row_of(a4, WEST + rows + EAST - 1)
        _, flux, f_low, f_high = seam(
            uv_tx[1], uv_rx[1], own, east, row_of(tu, rows - 1), row_of(fe_rx, EAST - 1),
            basis[0, pl.ds(WEST + rows - 8, 8)], fe_rx[pl.ds(0, 8)],
        )
        flux_e[...] = flux
        basis[0, pl.ds(WEST + rows - 8, 8)] = f_low
        basis[0, pl.ds(WEST + rows, 8)] = f_high
        for r in range(8, EAST, 8):
            basis[0, pl.ds(WEST + rows + r, 8)] = fe_rx[pl.ds(r, 8)]
        for p in range(SWEEPS):
            j = p + 1
            sweep(
                p, floor8(rows - 2 - j), ceil8(rows + SWEEPS - j), 0, rows + EAST,
                lambda r: own if r < rows else east, (0, 0),
            )

    def before_west():
        tracers()
        hear_late()
        send_left()
        send(hs_tx.at[0], hs_rx.at[1], 2, left)
        tracers_and_east(False)

    pl.when(at_start)(before_west)

    arrive(0, 2 * WEST + 8)
    west = row_of(a4, 0)
    speed_w, flux_w, f_low, f_high = seam(
        uv_rx[0], uv_tx[0], west, own, row_of(fw_rx, 0), row_of(tu, 0),
        fw_rx[pl.ds(WEST - 8, 8)], basis[0, pl.ds(WEST, 8)],
    )
    for r in range(0, WEST - 8, 8):
        basis[0, pl.ds(r, 8)] = fw_rx[pl.ds(r, 8)]
    basis[0, pl.ds(WEST - 8, 8)] = f_low
    basis[0, pl.ds(WEST, 8)] = f_high

    moments = [None] * MOMENTS
    base = [None, None]
    for p in range(SWEEPS):
        j = p + 1
        sums = sweep(
            p, floor8(j - 2 * SWEEPS - 2), ceil8(2 + j) if j < SWEEPS else inner_from, -WEST, rows,
            lambda r: west if r < 0 else own, (floor8(-SHIFT), 8),
        )
        for i, x in enumerate(sums):
            moments[2 * p + i] = x
        tail = []
        for r in range(8, inner_from, 8):
            k0, k1 = basis[p, pl.ds(WEST + r, 8)], basis[p + 1, pl.ds(WEST + r, 8)]
            tail.append((k0 * k0, k0 * k1) + ((k1 * k1,) if j == SWEEPS else ()))
        for i in range(len(sums)):
            moments[2 * p + i] = tree(
                [moments[2 * p + i], acc[2 * p + i]] + [fold(t[i]) for t in tail]
            )
    base = moments[:2]
    moments = base + [2.0 * x - base[i % 2] for i, x in enumerate(moments[2:])]
    spread = jnp.zeros((8, 128), F32)
    for i, x in enumerate(moments):
        spread = jnp.where(lane[:, :128] == i, jnp.sum(x, axis=1, keepdims=True), spread)
    slots[me] = jnp.sum(spread, axis=0, keepdims=True)
    pl.when(me > 0)(hear_late)
    for k in range(n - 1):
        pltpu.make_async_remote_copy(
            src_ref=slots.at[me], dst_ref=slots.at[me],
            send_sem=gsem.at[0], recv_sem=gsem.at[1],
            device_id={"blk": k + jnp.where(k >= me, 1, 0)}, device_id_type=pl.DeviceIdType.MESH,
        ).start()

    pl.when(me > 0)(tracers_and_east)
    arrive(2, 16)

    def mend(outs, fixed, row):
        block, place = row // 8 * 8, row % 8
        for i, out in enumerate(outs):
            for level in range(levels):
                spot = i * levels + level
                old = out[level, pl.ds(block, 8)].astype(F32)
                x = pltpu.roll(fixed, (place - spot) % 8, 0) if (place - spot) % 8 else fixed
                out[level, pl.ds(block, 8)] = jnp.where(sub == place, x, old).astype(BF16)

    def carried(speed, low, high):
        return speed * jnp.where(speed > 0.0, low, high)

    mend((bu, bv), edges[0] + (COURANT * own) * flux_w, 0)
    mend((bu, bv), edges[1] - (COURANT * own) * flux_e[...], rows - 1)
    east = row_of(a4, WEST + rows + EAST - 1)
    speed_e = face(uv_tx[1], uv_rx[1], own * east)
    mend((bh, bs), edges[2] + (COURANT * own) * carried(speed_w, hs_rx[0], hs_tx[0]), 0)
    mend((bh, bs), edges[3] - (COURANT * own) * carried(speed_e, hs_tx[1], hs_rx[1]), rows - 1)

    others = slots.at[pl.ds(0, n - 1)]
    rest = pltpu.make_async_remote_copy(
        src_ref=others, dst_ref=others, send_sem=gsem.at[0], recv_sem=gsem.at[1],
        device_id={"blk": right}, device_id_type=pl.DeviceIdType.MESH,
    )
    rest.wait_recv()
    mom[...] = jnp.broadcast_to(tree([slots[i] for i in range(n)]), (8, 128))
    rest.wait_send()
    lot = a4.at[pl.ds(0, 2 * WEST + 2 * EAST + 32)]
    pltpu.make_async_remote_copy(
        src_ref=lot, dst_ref=lot, send_sem=ssem.at[0], recv_sem=rsem.at[0],
        device_id={"blk": right}, device_id_type=pl.DeviceIdType.MESH,
    ).wait_send()


def finish(bh, bs, bu, bv, basis, mom, o_heat, o_salt, o_u, o_v, o_height, o_resid, hgt, res, sems):
    rows, lanes = hgt.shape
    stores = [
        pltpu.make_async_copy(src, dst, sems.at[0])
        for src, dst in ((bh, o_heat), (bs, o_salt), (bu, o_u), (bv, o_v))
    ]
    for store in stores:
        store.start()
    row = mom[...]
    m = [jnp.broadcast_to(row[:, i : i + 1], (8, 128)) for i in range(MOMENTS)]
    gram = [[m[a + b] + m[abs(a - b)] for b in range(FIELDS)] for a in range(FIELDS)]
    offset, resid = inner_steps(gram, SWEEPS)

    def combine(vals, coef):
        return tree([c * v for v, c in zip(vals, coef) if c is not None])

    parts = 2
    step = rows // 8 // parts
    for part in range(parts):
        for s in range(part * step, (part + 1) * step):
            r = 8 * s
            for c in range(0, lanes, 128):
                vals = [basis[i, pl.ds(WEST + r, 8), c : c + 128] for i in range(FIELDS)]
                hgt[pl.ds(r, 8), c : c + 128] = combine(vals, offset)
                res[pl.ds(r, 8), c : c + 128] = combine(vals, resid)
        span = pl.ds(part * step * 8, step * 8)
        for src, dst in ((hgt, o_height), (res, o_resid)):
            pltpu.make_async_copy(src.at[span], dst.at[span], sems.at[1]).start()
    levels = bh.shape[0]
    for sem, count in ((0, 2 * levels), (1, 2)):
        lot = basis.at[pl.ds(0, count), pl.ds(0, rows)]
        pltpu.make_async_copy(lot, lot, sems.at[sem]).wait()


def on_device(heat, salt, uvel, vvel, spacing, damp, flags):
    n = lax.axis_size("blk")
    levels, rows, lanes = uvel.shape
    total = WEST + rows + EAST
    hbm = pl.BlockSpec(memory_space=pltpu.HBM)
    vmem = pl.BlockSpec(memory_space=pltpu.VMEM)
    args = [
        pltpu.with_memory_space_constraint(x, pltpu.HBM)
        for x in (heat, salt, uvel, vvel, spacing, damp, flags)
    ]
    vm = pltpu.VMEM
    half = jax.ShapeDtypeStruct((levels, rows, lanes), BF16)
    flat = jax.ShapeDtypeStruct((rows, lanes), F32)
    full = vm((levels, rows, lanes), F32)
    dma = pltpu.SemaphoreType.DMA
    mids = (
        half, half, half, half,
        jax.ShapeDtypeStruct((FIELDS, total, lanes), F32),
        jax.ShapeDtypeStruct((8, 128), F32),
    )
    results = pl.pallas_call(
        functools.partial(kernel, n),
        out_shape=mids,
        in_specs=[hbm] * 7,
        out_specs=(vmem,) * 6,
        scratch_shapes=[
            full, full, full, full, full, full,
            vm((2, levels, rows, lanes), F32),
            vm((rows, lanes), F32),
            vm((rows, lanes), F32),
            vm((rows, lanes), F32),
            vm((MOMENTS, 8, 128), F32),
            vm((4, 8, lanes), F32),
            vm((2, 8, lanes), F32),
            vm((2, 8, lanes), F32),
            vm((2, 8, lanes), F32),
            vm((2, 8, lanes), F32),
            vm((WEST, lanes), F32),
            vm((EAST, lanes), F32),
            vm((total, lanes), F32),
            vm((WEST, lanes), F32),
            vm((EAST, lanes), F32),
            vm((WEST, lanes), F32),
            vm((EAST, lanes), F32),
            vm((n, 1, 128), F32),
            pltpu.SMEM(spacing.shape, F32),
            pltpu.SMEM(flags.shape, flags.dtype),
            vm((8, lanes), F32),
            dma((6,)),
            dma((1,)),
            dma((3,)),
            dma((2,)),
            pltpu.SemaphoreType.REGULAR((1,)),
        ],
        compiler_params=pltpu.CompilerParams(
            collective_id=0, has_side_effects=True, vmem_limit_bytes=40 * 1024 * 1024
        ),
    )(*args)
    results = [pltpu.with_memory_space_constraint(x, pltpu.VMEM) for x in results]
    shapes = (half, half, half, half, flat, flat)
    return pl.pallas_call(
        finish,
        out_shape=tuple(pltpu.HBM(x.shape, x.dtype) for x in shapes),
        in_specs=[vmem] * 6,
        out_specs=(hbm,) * 6,
        scratch_shapes=[vm((rows, lanes), F32), vm((rows, lanes), F32), dma((2,))],
        compiler_params=pltpu.CompilerParams(vmem_limit_bytes=8 * 1024 * 1024),
    )(*results)


def solution(mesh):
    return jax.shard_map(
        on_device,
        mesh=mesh,
        in_specs=(
            P("member", "blk", None),
            P("member", "blk", None),
            P("member", "blk", None),
            P("member", "blk", None),
            P(),
            P("blk", None),
            P("blk", None),
        ),
        out_specs=(
            P("member", "blk", None),
            P("member", "blk", None),
            P("member", "blk", None),
            P("member", "blk", None),
            P(("member", "blk"), None),
            P(("member", "blk"), None),
        ),
        check_vma=False,
    )
```

```python
import functools

import jax
import jax.numpy as jnp
import numpy as np
from jax import lax
from jax.experimental import pallas as pl
from jax.experimental.pallas import tpu as pltpu
from jax.sharding import PartitionSpec as P

SSTEP = 4
CG_BLOCKS = 3
SWEEPS = SSTEP * CG_BLOCKS
FIELDS = SWEEPS + 1
MOMENTS = 2 * SWEEPS
COURANT = 0.2
SHIFT = SWEEPS + 2
WEST = -(-(2 * SWEEPS + 2) // 8) * 8
EAST = -(-(SWEEPS + 2) // 8) * 8
F32 = jnp.float32
BF16 = jnp.bfloat16


def shift_table(extent):
    table = np.zeros((extent, extent), np.float32)
    for source in range(extent - 1):
        if source == 0:
            table[1, 0] = table[0, 0] = 0.5
        else:
            table[source + 1, source] = 0.25
            table[source, source] = 0.5
            table[source - 1, source] = 0.25
    return table


def tree(terms):
    while len(terms) > 1:
        terms = [
            terms[i] + terms[i + 1] if i + 1 < len(terms) else terms[i]
            for i in range(0, len(terms), 2)
        ]
    return terms[0]


def square(even, coef):
    rows = []
    for i, ci in enumerate(coef):
        if ci is not None:
            row = [(even[2 * i] + even[0]) * ci]
            row += [2.0 * (even[i + j] + even[i - j]) * coef[j] for j in range(i)]
            rows.append(ci * tree(row))
    return tree(rows)


def plus(a, b):
    if a is None:
        return b
    if b is None:
        return a
    return a + b


def scaled(scale, a):
    return None if a is None else scale * a


def inner_steps(moments, sweeps):
    extent = sweeps + 1
    table = shift_table(extent)
    one = jnp.ones_like(moments[0])
    along = [one] + [None] * sweeps
    resid = [one] + [None] * sweeps
    offset = [None] * extent
    norm_now = moments[0] + moments[0]
    for sweep in range(sweeps):
        image = []
        for i in range(extent):
            total = None
            for j in range(extent):
                if table[i, j] != 0.0:
                    total = plus(total, scaled(float(table[i, j]), along[j]))
            image.append(total)
        scale = 1.0 / norm_now
        rows = []
        for i, ai in enumerate(along):
            if ai is not None:
                row = [
                    (moments[i + j] + moments[abs(i - j)]) * image[j]
                    for j in range(extent) if image[j] is not None
                ]
                rows.append(ai * tree(row))
        alpha = norm_now / tree(rows)
        offset = [plus(o, scaled(alpha, a)) for o, a in zip(offset, along)]
        resid = [plus(r, scaled(-alpha, a)) for r, a in zip(resid, image)]
        if sweep + 1 < sweeps:
            norm_next = square(moments, resid)
            beta = norm_next * scale
            along = [plus(r, scaled(beta, a)) for r, a in zip(resid, along)]
            norm_now = norm_next
    return offset, resid


def kernel(
    n,
    heat, salt, uvel, vvel, spacing, damp, flags,
    bh, bs, bu, bv, basis, mom,
    ue, ve, he, se, ef, nf, ff, de, tu, tv, acc, edges,
    uv_tx, hs_tx, uv_rx, hs_rx, aw_tx, ae_tx, a4, fw_tx, fe_tx, fw_rx, fe_rx, slots,
    space, marks,
    flux_e, lsem, ssem, rsem, gsem, late_sem,
):
    levels, rows, lanes = ue.shape
    me = lax.axis_index("blk")
    right, left = lax.rem(me + 1, n), lax.rem(me + n - 1, n)
    late = rows - WEST
    split = late - 8

    def part(ref, buf, lo, hi, sem):
        return pltpu.make_async_copy(
            ref.at[:, pl.ds(lo, hi - lo)], buf.at[:, pl.ds(lo, hi - lo)], lsem.at[sem]
        )

    def pair(lo, hi, sem):
        both = ff.at[:, :, pl.ds(lo, hi - lo)]
        return pltpu.make_async_copy(both, both, lsem.at[sem])

    loads = [
        pltpu.make_async_copy(flags, marks, lsem.at[0]),
        pltpu.make_async_copy(spacing, space, lsem.at[1]),
        pltpu.make_async_copy(damp, de, lsem.at[3]),
        part(uvel, ue, split, rows, 2),
        part(vvel, ve, split, rows, 2),
        part(uvel, ue, 0, split, 4),
        part(vvel, ve, 0, split, 4),
    ]
    more = [
        pltpu.make_async_copy(heat, he, lsem.at[5]),
        pltpu.make_async_copy(salt, se, lsem.at[5]),
    ]
    for load in loads[:5]:
        load.start()

    barrier = pltpu.get_barrier_semaphore()

    def tell(sem, to):
        pl.semaphore_signal(
            sem, inc=1, device_id={"blk": to}, device_id_type=pl.DeviceIdType.MESH
        )

    at_start, at_end = me == 0, me == n - 1
    pl.when(me > 0)(lambda: tell(barrier, left))
    for k in range(1, n):
        pl.when(me + k < n)(functools.partial(tell, barrier, lax.rem(me + k, n)))
    for load in loads[5:]:
        load.start()

    def pass_barrier():
        pl.semaphore_wait(barrier, jnp.where(at_end, n - 1, me + 1))

    def tell_earlier():
        for k in range(2, n):
            pl.when(me - k >= 0)(functools.partial(tell, late_sem.at[0], lax.rem(me + n - k, n)))

    def hear_late():
        later = n - 2 - me
        pl.when(later > 0)(lambda: pl.semaphore_wait(late_sem.at[0], later))

    lane = lax.broadcasted_iota(jnp.int32, (8, lanes), 1)
    sub = lax.broadcasted_iota(jnp.int32, (8, lanes), 0)
    top, bottom = sub == 0, sub == 7
    zero = jnp.zeros((8, lanes), F32)

    def north_of(x):
        return pltpu.roll(x, lanes - 1, 1)

    def south_of(x):
        return pltpu.roll(x, 1, 1)

    def sides(x):
        return jnp.where(lane == lanes - 1, 0.0, north_of(x)), jnp.where(lane == 0, 0.0, south_of(x))

    slim = lane[:, :128]

    def beside(x):
        tiles = [x[:, c : c + 128] for c in range(0, lanes, 128)]
        north = [pltpu.roll(t, 127, 1) for t in tiles] + [0.0]
        south = [pltpu.roll(t, 1, 1) for t in tiles]
        south = [0.0] + south
        return jnp.concatenate(
            [
                jnp.where(slim == 127, north[i + 1], north[i]) + jnp.where(slim == 0, south[i], south[i + 1])
                for i in range(len(tiles))
            ],
            axis=1,
        )

    def up_one(x):
        return pltpu.roll(x, 7, 0)

    def down_one(x):
        return pltpu.roll(x, 1, 0)

    loads[0].wait()
    loads[1].wait()
    tiles = marks.shape[1]
    lane_tile = lane // (lanes // tiles)
    own = zero
    for k in range(tiles):
        own = jnp.where(lane_tile == k, marks[0, k].astype(F32), own)
    ahead = jnp.where(lane == lanes - 1, 0.0, own * north_of(own))
    half_own = 0.5 * own
    whole_w = jnp.zeros((8, 128), F32)
    for j in range(levels):
        whole_w = whole_w + space[j]
    portions = [jnp.full((8, 128), space[j], F32) / whole_w for j in range(levels)]

    def wide(x):
        return jnp.concatenate([x] * (lanes // 128), axis=1)

    weight = [wide(x) for x in portions]
    level_weight = zero
    for j in range(levels):
        level_weight = jnp.where(sub % levels == j, weight[j], level_weight)

    def gather_row(refs, row):
        block, place = row // 8 * 8, row % 8
        packed = None
        for i, ref in enumerate(refs):
            for level in range(levels):
                x = ref[level, pl.ds(block, 8)]
                spot = i * levels + level
                if (spot - place) % 8:
                    x = pltpu.roll(x, (spot - place) % 8, 0)
                packed = x if packed is None else jnp.where(sub == spot, x, packed)
        return packed

    def pick(packed, block, spot, place):
        return jnp.where(sub == spot, pltpu.roll(block, (spot - place) % 8, 0) if (spot - place) % 8 else block, packed)

    def north_flux(first, last, fields, keep):
        for level in range(levels):
            for r in range(first, last, 8):
                here = pl.ds(r, 8)
                q0 = [ref[level, here] for ref in fields]
                qn = [north_of(q) for q in q0]
                if keep:
                    north = (q0[1] + qn[1]) * ahead
                    nf[level, here] = north
                else:
                    north = nf[level, here]
                for i in range(2):
                    ff[i, level, here] = north * jnp.where(north > 0.0, q0[i], qn[i])

    def flows(first, last, fields, outs, slot, keep):
        ends = [zero, zero]
        for level in range(levels):
            def ahead_of(ref, r, q0):
                if r + 8 < rows:
                    return jnp.where(bottom, up_one(ref[level, pl.ds(r + 8, 8)]), up_one(q0))
                return up_one(q0)

            def east_fluxes(r):
                q0 = [ref[level, pl.ds(r, 8)] for ref in fields]
                qp = [ahead_of(ref, r, q) for ref, q in zip(fields, q0)]
                if keep:
                    east = q0[0] + qp[0]
                    if r + 8 == rows:
                        east = jnp.where(bottom, 0.0, east)
                    ef[level, pl.ds(r, 8)] = east
                else:
                    east = ef[level, pl.ds(r, 8)]
                return q0, [east * jnp.where(east > 0.0, a, b) for a, b in zip(q0, qp)]

            before = [zero, zero] if first == 0 else [down_one(f) for f in east_fluxes(first - 8)[1]]
            pending = None
            for r in range(first, last, 8):
                here = pl.ds(r, 8)
                q0, fe = east_fluxes(r)
                news = []
                for i in range(2):
                    shifted = down_one(fe[i])
                    fw = jnp.where(top, before[i], shifted)
                    before[i] = shifted
                    fn = ff[i, level, here]
                    spread = (fe[i] - fw) + (fn - south_of(fn))
                    new = own * (q0[i] - (0.5 * COURANT) * spread)
                    news.append(new)
                    if keep:
                        total = (tu, tv)[i]
                        term = weight[level] * new
                        total[here] = term if level == 0 else total[here] + term
                    spot = i * levels + level
                    if r == 0:
                        ends[0] = pick(ends[0], new, spot, 0)
                    if r + 8 == rows:
                        ends[1] = pick(ends[1], new, spot, 7)
                if pending is None:
                    pending = news
                else:
                    for i, out in enumerate(outs):
                        out[level, pl.ds(r - 8, 16)] = jnp.concatenate([pending[i], news[i]], axis=0).astype(BF16)
                    pending = None
        if first == 0:
            edges[slot] = ends[0]
        if last == rows:
            edges[slot + 1] = ends[1]

    def forcing(r, low, high):
        t0, x0 = tv[pl.ds(r, 8)], tu[pl.ds(r, 8)]
        north, south = sides(t0)
        after = jnp.where(bottom, up_one(tu[pl.ds(r + 8, 8)]) if r + 8 < high else 0.0, up_one(x0))
        prior = jnp.where(top, down_one(tu[pl.ds(r - 8, 8)]) if r > low else 0.0, down_one(x0))
        return (0.5 * own) * ((after - prior) + (north - south))

    def send(src, dst, sem, to):
        pltpu.make_async_remote_copy(
            src_ref=src, dst_ref=dst, send_sem=ssem.at[0], recv_sem=rsem.at[sem],
            device_id={"blk": to}, device_id_type=pl.DeviceIdType.MESH,
        ).start()

    def arrive(sem, height):
        lot = a4.at[pl.ds(0, height)]
        pltpu.make_async_remote_copy(
            src_ref=lot, dst_ref=lot, send_sem=ssem.at[0], recv_sem=rsem.at[sem],
            device_id={"blk": right}, device_id_type=pl.DeviceIdType.MESH,
        ).wait_recv()

    def send_left():
        send(uv_tx.at[0], uv_rx.at[1], 1, left)
        send(ae_tx, a4.at[pl.ds(WEST + rows, EAST)], 1, left)
        send(fe_tx, fe_rx, 1, left)

    loads[2].wait()
    for r in range(0, rows, 8):
        a = 0.5 * (own * (6.0 + de[pl.ds(r, 8)]) + (1.0 - own)) - 2.0
        a4[pl.ds(WEST + r, 8)] = a
        if r >= late:
            aw_tx[pl.ds(r - late, 8)] = jnp.where(top, own, a) if r == late else a
        if r < EAST:
            ae_tx[pl.ds(r, 8)] = jnp.where(bottom, own, a) if r + 8 == EAST else a
    pair(split, rows, 2).wait()
    uv_tx[1] = gather_row((ue, ve), rows - 1)
    pass_barrier()
    send(uv_tx.at[1], uv_rx.at[0], 0, right)
    send(aw_tx, a4.at[pl.ds(0, WEST)], 0, right)
    tell_earlier()
    for load in more:
        load.start()
    north_flux(late, rows, (ue, ve), True)
    flows(late, rows, (ue, ve), (bu, bv), 0, True)
    for r in range(late, rows, 8):
        f = forcing(r, late, rows)
        if r > late:
            basis[0, pl.ds(WEST + r, 8)] = f
        else:
            f = jnp.where(top, jnp.broadcast_to(tu[pl.ds(rows - 1, 1)], (8, lanes)), f)
        fw_tx[pl.ds(r - late, 8)] = f
    send(fw_tx, fw_rx, 0, right)

    pair(0, split, 4).wait()
    uv_tx[0] = gather_row((ue, ve), 0)
    north_flux(0, late, (ue, ve), True)
    flows(0, late, (ue, ve), (bu, bv), 0, True)
    for r in range(0, late + 8, 8):
        f = forcing(r, 0, rows)
        basis[0, pl.ds(WEST + r, 8)] = f
        if r < EAST:
            if r + 8 == EAST:
                f = jnp.where(bottom, jnp.broadcast_to(tu[pl.ds(0, 1)], (8, lanes)), f)
            fe_tx[pl.ds(r, 8)] = f
    pl.when(me > 0)(send_left)

    window = (-SHIFT, rows - SHIFT)

    def in_window(r, x):
        if r < window[0]:
            return jnp.where(sub >= window[0] - r, x, 0.0)
        if r + 8 > window[1]:
            return jnp.where(sub < window[1] - r, x, 0.0)
        return x

    def fold(x):
        return tree([x[:, c : c + 128] for c in range(0, lanes, 128)])

    def sweep(p, first, last, low, high, half_wet, summed, held=None):
        held = {} if held is None else held
        known = {}

        def field(q, r):
            return held[q, r] if (q, r) in held else basis[q, pl.ds(WEST + r, 8)]

        def block(r):
            if r not in known:
                k0 = field(p, r)
                known[r] = (k0, down_one(k0), up_one(k0))
            return known[r]

        squares, crosses = [], []
        turned = {}
        for r in range(first, last, 8):
            k0, down, up = block(r)
            prior = block(r - 8)[1] if r > low else down
            after = block(r + 8)[2] if r + 8 < high else up
            vert = jnp.where(top, prior, down) + jnp.where(bottom, after, up)
            turned[r] = vert, beside(k0 + 0.5 * vert)
        for r in range(first, last, 8):
            k0 = block(r)[0]
            vert, side = turned[r]
            here = pl.ds(WEST + r, 8)
            half = a4[here] * k0 - half_wet(r) * (vert + side)
            new = 0.5 * half if p == 0 else half - field(p - 1, r)
            basis[p + 1, here] = new
            held[p + 1, r] = new
            if summed[0] <= r < summed[1]:
                kept = in_window(r, k0)
                squares.append(kept * kept)
                crosses.append(kept * in_window(r, new))
        for key in [key for key in held if key[0] < p]:
            del held[key]
        return [tree([fold(t) for t in x]) for x in (squares, crosses) if x]

    def floor8(x):
        return x // 8 * 8

    def ceil8(x):
        return -(-x // 8) * 8

    inner_from, inner_to = ceil8(SWEEPS + 2), rows - SHIFT
    for p in range(SWEEPS):
        j = p + 1
        sums = sweep(
            p, floor8(2 + j), ceil8(rows - 2 - j), 0, rows, lambda r: half_own, (inner_from, inner_to)
        )
        for i, x in enumerate(sums):
            acc[2 * p + i] = x

    pltpu.make_async_copy(ff, ff, lsem.at[5]).wait()
    hs_tx[0] = gather_row((he, se), 0)
    hs_tx[1] = gather_row((he, se), rows - 1)
    send(hs_tx.at[1], hs_rx.at[0], 2, right)
    pl.when(me > 0)(lambda: send(hs_tx.at[0], hs_rx.at[1], 2, left))

    def tracers():
        north_flux(0, rows, (he, se), False)
        flows(0, rows, (he, se), (bh, bs), 2, False)

    def total_of(x):
        for step in (4, 2, 1):
            x = x + pltpu.roll(x, step, 0)
        return x

    def face(low, high, both):
        twice = [jnp.where(sub < levels, x, pltpu.roll(x, levels, 0)) for x in (low, high)]
        return 0.5 * (twice[0] + twice[1]) * both

    def seam(uv_low, uv_high, wet_low, wet_high, tu_low, tu_high, f_low, f_high):
        speed = face(uv_low, uv_high, wet_low * wet_high)
        flux = speed * jnp.where(speed > 0.0, uv_low, uv_high)
        term = level_weight * flux
        gu = total_of(jnp.where(sub < levels, term, 0.0))
        gv = total_of(jnp.where(sub < levels, 0.0, term))
        low_u, high_u = (-COURANT * wet_low) * gu, (COURANT * wet_high) * gu
        low_v, high_v = (-COURANT * wet_low) * gv, (COURANT * wet_high) * gv
        north, south = sides(jnp.where(sub < 4, high_v, low_v))
        across = north - south
        f_low = f_low + (0.5 * wet_low) * jnp.where(
            sub == 7, (tu_high + high_u) + across, jnp.where(sub == 6, low_u, 0.0)
        )
        f_high = f_high + (0.5 * wet_high) * jnp.where(
            sub == 0, across - (tu_low + low_u), jnp.where(sub == 1, -high_u, 0.0)
        )
        return speed, flux, f_low, f_high

    def row_of(ref, row):
        return jnp.broadcast_to(ref[pl.ds(row, 1)], (8, lanes))

    def tracers_and_east(both=True):
        if both:
            tracers()
        arrive(1, 2 * EAST + 8)
        east = row_of(a4, WEST + rows + EAST - 1)
        _, flux, f_low, f_high = seam(
            uv_tx[1], uv_rx[1], own, east, row_of(tu, rows - 1), row_of(fe_rx, EAST - 1),
            basis[0, pl.ds(WEST + rows - 8, 8)], fe_rx[pl.ds(0, 8)],
        )
        flux_e[...] = flux
        basis[0, pl.ds(WEST + rows - 8, 8)] = f_low
        basis[0, pl.ds(WEST + rows, 8)] = f_high
        for r in range(8, EAST, 8):
            basis[0, pl.ds(WEST + rows + r, 8)] = fe_rx[pl.ds(r, 8)]
        held = {}
        half_east = 0.5 * east
        for p in range(SWEEPS):
            j = p + 1
            sweep(
                p, floor8(rows - 2 - j), ceil8(rows + SWEEPS - j), 0, rows + EAST,
                lambda r: half_own if r < rows else half_east, (0, 0), held,
            )

    def before_west():
        tracers()
        hear_late()
        send_left()
        send(hs_tx.at[0], hs_rx.at[1], 2, left)
        tracers_and_east(False)

    pl.when(at_start)(before_west)

    arrive(0, 2 * WEST + 8)
    west = row_of(a4, 0)
    speed_w, flux_w, f_low, f_high = seam(
        uv_rx[0], uv_tx[0], west, own, row_of(fw_rx, 0), row_of(tu, 0),
        fw_rx[pl.ds(WEST - 8, 8)], basis[0, pl.ds(WEST, 8)],
    )
    for r in range(0, WEST - 8, 8):
        basis[0, pl.ds(r, 8)] = fw_rx[pl.ds(r, 8)]
    basis[0, pl.ds(WEST - 8, 8)] = f_low
    basis[0, pl.ds(WEST, 8)] = f_high

    moments = [None] * MOMENTS
    west_held = {}
    half_west = 0.5 * west
    for p in range(SWEEPS):
        j = p + 1
        sums = sweep(
            p, floor8(j - 2 * SWEEPS - 2), ceil8(2 + j) if j < SWEEPS else inner_from, -WEST, rows,
            lambda r: half_west if r < 0 else half_own, (floor8(-SHIFT), 8), west_held,
        )
        for i, x in enumerate(sums):
            moments[2 * p + i] = x
        tail = []
        for r in range(8, inner_from, 8):
            k0, k1 = basis[p, pl.ds(WEST + r, 8)], basis[p + 1, pl.ds(WEST + r, 8)]
            tail.append((k0 * k0, k0 * k1))
        for i in range(len(sums)):
            moments[2 * p + i] = tree(
                [moments[2 * p + i], acc[2 * p + i]] + [fold(t[i]) for t in tail]
            )
    base = moments[:2]
    moments = base + [2.0 * x - base[i % 2] for i, x in enumerate(moments[2:])]
    spread = jnp.zeros((8, 128), F32)
    for i, x in enumerate(moments):
        spread = jnp.where(lane[:, :128] == i, jnp.sum(x, axis=1, keepdims=True), spread)
    slots[me] = jnp.sum(spread, axis=0, keepdims=True)
    pl.when(me > 0)(hear_late)
    for k in range(n - 1):
        pltpu.make_async_remote_copy(
            src_ref=slots.at[me], dst_ref=slots.at[me],
            send_sem=gsem.at[0], recv_sem=gsem.at[1],
            device_id={"blk": k + jnp.where(k >= me, 1, 0)}, device_id_type=pl.DeviceIdType.MESH,
        ).start()

    pl.when(me > 0)(tracers_and_east)
    arrive(2, 16)

    def mend(outs, fixed, row):
        block, place = row // 8 * 8, row % 8
        for i, out in enumerate(outs):
            for level in range(levels):
                spot = i * levels + level
                old = out[level, pl.ds(block, 8)].astype(F32)
                x = pltpu.roll(fixed, (place - spot) % 8, 0) if (place - spot) % 8 else fixed
                out[level, pl.ds(block, 8)] = jnp.where(sub == place, x, old).astype(BF16)

    def carried(speed, low, high):
        return speed * jnp.where(speed > 0.0, low, high)

    mend((bu, bv), edges[0] + (COURANT * own) * flux_w, 0)
    mend((bu, bv), edges[1] - (COURANT * own) * flux_e[...], rows - 1)
    east = row_of(a4, WEST + rows + EAST - 1)
    speed_e = face(uv_tx[1], uv_rx[1], own * east)
    mend((bh, bs), edges[2] + (COURANT * own) * carried(speed_w, hs_rx[0], hs_tx[0]), 0)
    mend((bh, bs), edges[3] - (COURANT * own) * carried(speed_e, hs_tx[1], hs_rx[1]), rows - 1)

    others = slots.at[pl.ds(0, n - 1)]
    rest = pltpu.make_async_remote_copy(
        src_ref=others, dst_ref=others, send_sem=gsem.at[0], recv_sem=gsem.at[1],
        device_id={"blk": right}, device_id_type=pl.DeviceIdType.MESH,
    )
    rest.wait_recv()
    mom[...] = jnp.broadcast_to(tree([slots[i] for i in range(n)]), (8, 128))
    rest.wait_send()
    lot = a4.at[pl.ds(0, 2 * WEST + 2 * EAST + 32)]
    pltpu.make_async_remote_copy(
        src_ref=lot, dst_ref=lot, send_sem=ssem.at[0], recv_sem=rsem.at[0],
        device_id={"blk": right}, device_id_type=pl.DeviceIdType.MESH,
    ).wait_send()


def finish(bh, bs, bu, bv, basis, mom, o_heat, o_salt, o_u, o_v, o_height, o_resid, hgt, res, sems):
    rows, lanes = hgt.shape
    stores = [
        pltpu.make_async_copy(src, dst, sems.at[0])
        for src, dst in ((bh, o_heat), (bs, o_salt), (bu, o_u), (bv, o_v))
    ]
    for store in stores:
        store.start()
    row = mom[...]
    m = [jnp.broadcast_to(row[:, i : i + 1], (8, 128)) for i in range(MOMENTS)]
    offset, resid = inner_steps(m, SWEEPS)

    def combine(vals, coef):
        return tree([c * v for v, c in zip(vals, coef) if c is not None])

    parts = 4
    step = rows // 8 // parts
    for part in range(parts):
        for s in range(part * step, (part + 1) * step):
            r = 8 * s
            for c in range(0, lanes, 128):
                vals = [basis[i, pl.ds(WEST + r, 8), c : c + 128] for i in range(FIELDS)]
                hgt[pl.ds(r, 8), c : c + 128] = combine(vals, offset)
                res[pl.ds(r, 8), c : c + 128] = combine(vals, resid)
        span = pl.ds(part * step * 8, step * 8)
        for src, dst in ((hgt, o_height), (res, o_resid)):
            pltpu.make_async_copy(src.at[span], dst.at[span], sems.at[1]).start()
    levels = bh.shape[0]
    for sem, count in ((0, 2 * levels), (1, 2)):
        lot = basis.at[pl.ds(0, count), pl.ds(0, rows)]
        pltpu.make_async_copy(lot, lot, sems.at[sem]).wait()


def on_device(heat, salt, uvel, vvel, spacing, damp, flags):
    n = lax.axis_size("blk")
    levels, rows, lanes = uvel.shape
    total = WEST + rows + EAST
    hbm = pl.BlockSpec(memory_space=pltpu.HBM)
    vmem = pl.BlockSpec(memory_space=pltpu.VMEM)
    args = [
        pltpu.with_memory_space_constraint(x, pltpu.HBM)
        for x in (heat, salt, uvel, vvel, spacing, damp, flags)
    ]
    vm = pltpu.VMEM
    half = jax.ShapeDtypeStruct((levels, rows, lanes), BF16)
    flat = jax.ShapeDtypeStruct((rows, lanes), F32)
    full = vm((levels, rows, lanes), F32)
    dma = pltpu.SemaphoreType.DMA
    mids = (
        half, half, half, half,
        jax.ShapeDtypeStruct((FIELDS, total, lanes), F32),
        jax.ShapeDtypeStruct((8, 128), F32),
    )
    results = pl.pallas_call(
        functools.partial(kernel, n),
        out_shape=mids,
        in_specs=[hbm] * 7,
        out_specs=(vmem,) * 6,
        scratch_shapes=[
            full, full, full, full, full, full,
            vm((2, levels, rows, lanes), F32),
            vm((rows, lanes), F32),
            vm((rows, lanes), F32),
            vm((rows, lanes), F32),
            vm((MOMENTS, 8, 128), F32),
            vm((4, 8, lanes), F32),
            vm((2, 8, lanes), F32),
            vm((2, 8, lanes), F32),
            vm((2, 8, lanes), F32),
            vm((2, 8, lanes), F32),
            vm((WEST, lanes), F32),
            vm((EAST, lanes), F32),
            vm((total, lanes), F32),
            vm((WEST, lanes), F32),
            vm((EAST, lanes), F32),
            vm((WEST, lanes), F32),
            vm((EAST, lanes), F32),
            vm((n, 1, 128), F32),
            pltpu.SMEM(spacing.shape, F32),
            pltpu.SMEM(flags.shape, flags.dtype),
            vm((8, lanes), F32),
            dma((6,)),
            dma((1,)),
            dma((3,)),
            dma((2,)),
            pltpu.SemaphoreType.REGULAR((1,)),
        ],
        compiler_params=pltpu.CompilerParams(
            collective_id=0, has_side_effects=True, vmem_limit_bytes=40 * 1024 * 1024
        ),
    )(*args)
    results = [pltpu.with_memory_space_constraint(x, pltpu.VMEM) for x in results]
    shapes = (half, half, half, half, flat, flat)
    return pl.pallas_call(
        finish,
        out_shape=tuple(pltpu.HBM(x.shape, x.dtype) for x in shapes),
        in_specs=[vmem] * 6,
        out_specs=(hbm,) * 6,
        scratch_shapes=[vm((rows, lanes), F32), vm((rows, lanes), F32), dma((2,))],
        compiler_params=pltpu.CompilerParams(vmem_limit_bytes=8 * 1024 * 1024),
    )(*results)


def solution(mesh):
    return jax.shard_map(
        on_device,
        mesh=mesh,
        in_specs=(
            P("member", "blk", None),
            P("member", "blk", None),
            P("member", "blk", None),
            P("member", "blk", None),
            P(),
            P("blk", None),
            P("blk", None),
        ),
        out_specs=(
            P("member", "blk", None),
            P("member", "blk", None),
            P("member", "blk", None),
            P("member", "blk", None),
            P(("member", "blk"), None),
            P(("member", "blk"), None),
        ),
        check_vma=False,
    )
```

```python
import functools

import jax
import jax.numpy as jnp
import numpy as np
from jax import lax
from jax.experimental import pallas as pl
from jax.experimental.pallas import tpu as pltpu
from jax.sharding import PartitionSpec as P

SSTEP = 4
CG_BLOCKS = 3
SWEEPS = SSTEP * CG_BLOCKS
FIELDS = SWEEPS + 1
MOMENTS = 2 * SWEEPS
COURANT = 0.2
SHIFT = SWEEPS + 2
WEST = -(-(2 * SWEEPS + 2) // 8) * 8
EAST = -(-(SWEEPS + 2) // 8) * 8
F32 = jnp.float32
BF16 = jnp.bfloat16


def shift_table(extent):
    table = np.zeros((extent, extent), np.float32)
    for source in range(extent - 1):
        if source == 0:
            table[1, 0] = table[0, 0] = 0.5
        else:
            table[source + 1, source] = 0.25
            table[source, source] = 0.5
            table[source - 1, source] = 0.25
    return table


def tree(terms):
    while len(terms) > 1:
        terms = [
            terms[i] + terms[i + 1] if i + 1 < len(terms) else terms[i]
            for i in range(0, len(terms), 2)
        ]
    return terms[0]


def plus(a, b):
    if a is None:
        return b
    if b is None:
        return a
    return a + b


def scaled(scale, a):
    return None if a is None else scale * a


def inner_steps(m, sweeps):
    extent = sweeps + 1
    table = shift_table(extent)
    ones = jnp.ones_like(m[0])
    pushed = [0.25 * (m[k + 1] + m[abs(k - 1)]) + 0.5 * m[k] for k in range(2 * sweeps - 1)]
    a = [[pushed[i + j] + pushed[i - j] for j in range(i + 1)] for i in range(sweeps)]
    lower = [[None] * sweeps for _ in range(sweeps)]
    inverse = []
    y = [m[i] + m[i] for i in range(sweeps)]
    for k in range(sweeps):
        inverse.append(ones / a[k][k])
        for i in range(k + 1, sweeps):
            lower[i][k] = a[i][k] * inverse[k]
        for i in range(k + 1, sweeps):
            for j in range(k + 1, i + 1):
                a[i][j] = a[i][j] - lower[i][k] * a[j][k]
            y[i] = y[i] - lower[i][k] * y[k]

    def backward(y):
        z = [v * d for v, d in zip(y, inverse)]
        for i in range(sweeps - 1, 0, -1):
            for j in range(i):
                z[j] = z[j] - lower[i][j] * z[i]
        return z

    def image(c):
        out = []
        for i in range(extent):
            total = None
            for j in range(sweeps):
                if table[i, j] != 0.0:
                    total = plus(total, scaled(float(table[i, j]), c[j]))
            out.append(total)
        return out

    offset = backward(y)
    resid = [-x for x in image(offset)]
    resid[0] = resid[0] + ones
    y = [
        tree([(m[i + j] + m[abs(i - j)]) * resid[j] for j in range(extent)]) for i in range(sweeps)
    ]
    for i in range(sweeps):
        for j in range(i + 1, sweeps):
            y[j] = y[j] - lower[j][i] * y[i]
    more = backward(y)
    offset = [c + d for c, d in zip(offset, more)]
    resid = [r - x for r, x in zip(resid, image(more))]
    return offset, resid


def kernel(
    n,
    heat, salt, uvel, vvel, spacing, damp, flags,
    bh, bs, bu, bv, basis, mom,
    ue, ve, he, se, ef, nf, ff, de, tu, tv, acc, edges,
    uv_tx, hs_tx, uv_rx, hs_rx, mix_tx, mix_rx, fx_tx, fx_rx, ae_tx, a4, fw_tx, fe_tx, fw_rx, fe_rx, slots,
    space, marks,
    flux_e, lsem, ssem, rsem, gsem, late_sem,
):
    levels, rows, lanes = ue.shape
    me = lax.axis_index("blk")
    right, left = lax.rem(me + 1, n), lax.rem(me + n - 1, n)
    late = rows - WEST
    west_rows = 2 * (WEST - 8) + (mix_tx.shape[0] + fx_tx.shape[0]) * 128 // lanes
    split = late - 8

    def part(ref, buf, lo, hi, sem):
        return pltpu.make_async_copy(
            ref.at[:, pl.ds(lo, hi - lo)], buf.at[:, pl.ds(lo, hi - lo)], lsem.at[sem]
        )

    def pair(lo, hi, sem):
        both = ff.at[:, :, pl.ds(lo, hi - lo)]
        return pltpu.make_async_copy(both, both, lsem.at[sem])

    loads = [
        pltpu.make_async_copy(flags, marks, lsem.at[0]),
        pltpu.make_async_copy(spacing, space, lsem.at[1]),
        pltpu.make_async_copy(damp.at[pl.ds(late, WEST)], de.at[pl.ds(late, WEST)], lsem.at[3]),
        part(uvel, ue, split, rows, 2),
        part(vvel, ve, split, rows, 2),
        part(uvel, ue, 0, split, 4),
        part(vvel, ve, 0, split, 4),
        pltpu.make_async_copy(damp.at[pl.ds(0, late)], de.at[pl.ds(0, late)], lsem.at[6]),
    ]
    more = [
        pltpu.make_async_copy(heat, he, lsem.at[5]),
        pltpu.make_async_copy(salt, se, lsem.at[5]),
    ]
    for load in loads[:5]:
        load.start()

    barrier = pltpu.get_barrier_semaphore()

    def tell(sem, to):
        pl.semaphore_signal(
            sem, inc=1, device_id={"blk": to}, device_id_type=pl.DeviceIdType.MESH
        )

    at_start, at_end = me == 0, me == n - 1
    pl.when(me > 0)(lambda: tell(barrier, left))
    for k in range(1, n):
        pl.when(me + k < n)(functools.partial(tell, barrier, lax.rem(me + k, n)))
    for load in loads[5:]:
        load.start()

    def pass_barrier():
        pl.semaphore_wait(barrier, jnp.where(at_end, n - 1, me + 1))

    def tell_earlier():
        for k in range(2, n):
            pl.when(me - k >= 0)(functools.partial(tell, late_sem.at[0], lax.rem(me + n - k, n)))

    def hear_late():
        later = n - 2 - me
        pl.when(later > 0)(lambda: pl.semaphore_wait(late_sem.at[0], later))

    lane = lax.broadcasted_iota(jnp.int32, (8, lanes), 1)
    sub = lax.broadcasted_iota(jnp.int32, (8, lanes), 0)
    top, bottom = sub == 0, sub == 7
    zero = jnp.zeros((8, lanes), F32)

    def north_of(x):
        return pltpu.roll(x, lanes - 1, 1)

    def south_of(x):
        return pltpu.roll(x, 1, 1)

    def sides(x):
        return jnp.where(lane == lanes - 1, 0.0, north_of(x)), jnp.where(lane == 0, 0.0, south_of(x))

    slim = lane[:, :128]

    def beside(x):
        tiles = [x[:, c : c + 128] for c in range(0, lanes, 128)]
        north = [pltpu.roll(t, 127, 1) for t in tiles] + [0.0]
        south = [pltpu.roll(t, 1, 1) for t in tiles]
        south = [0.0] + south
        return jnp.concatenate(
            [
                jnp.where(slim == 127, north[i + 1], north[i]) + jnp.where(slim == 0, south[i], south[i + 1])
                for i in range(len(tiles))
            ],
            axis=1,
        )

    def up_one(x):
        return pltpu.roll(x, 7, 0)

    def down_one(x):
        return pltpu.roll(x, 1, 0)

    loads[0].wait()
    loads[1].wait()
    tiles = marks.shape[1]
    lane_tile = lane // (lanes // tiles)
    own = zero
    for k in range(tiles):
        own = jnp.where(lane_tile == k, marks[0, k].astype(F32), own)
    ahead = jnp.where(lane == lanes - 1, 0.0, own * north_of(own))
    half_own = 0.5 * own
    whole_w = jnp.zeros((8, 128), F32)
    for j in range(levels):
        whole_w = whole_w + space[j]
    portions = [jnp.full((8, 128), space[j], F32) / whole_w for j in range(levels)]

    def wide(x):
        return jnp.concatenate([x] * (lanes // 128), axis=1)

    weight = [wide(x) for x in portions]
    level_weight = zero
    for j in range(levels):
        level_weight = jnp.where(sub % levels == j, weight[j], level_weight)

    def gather_row(refs, row):
        block, place = row // 8 * 8, row % 8
        packed = None
        for i, ref in enumerate(refs):
            for level in range(levels):
                x = ref[level, pl.ds(block, 8)]
                spot = i * levels + level
                if (spot - place) % 8:
                    x = pltpu.roll(x, (spot - place) % 8, 0)
                packed = x if packed is None else jnp.where(sub == spot, x, packed)
        return packed

    def pick(packed, block, spot, place):
        return jnp.where(sub == spot, pltpu.roll(block, (spot - place) % 8, 0) if (spot - place) % 8 else block, packed)

    def north_flux(first, last, fields, keep):
        for level in range(levels):
            for r in range(first, last, 8):
                here = pl.ds(r, 8)
                q0 = [ref[level, here] for ref in fields]
                qn = [north_of(q) for q in q0]
                if keep:
                    north = (q0[1] + qn[1]) * ahead
                    nf[level, here] = north
                else:
                    north = nf[level, here]
                for i in range(2):
                    ff[i, level, here] = north * jnp.where(north > 0.0, q0[i], qn[i])

    def flows(first, last, fields, outs, slot, keep):
        ends = [zero, zero]
        for level in range(levels):
            def ahead_of(ref, r, q0):
                if r + 8 < rows:
                    return jnp.where(bottom, up_one(ref[level, pl.ds(r + 8, 8)]), up_one(q0))
                return up_one(q0)

            def east_fluxes(r):
                q0 = [ref[level, pl.ds(r, 8)] for ref in fields]
                qp = [ahead_of(ref, r, q) for ref, q in zip(fields, q0)]
                if keep:
                    east = q0[0] + qp[0]
                    if r + 8 == rows:
                        east = jnp.where(bottom, 0.0, east)
                    ef[level, pl.ds(r, 8)] = east
                else:
                    east = ef[level, pl.ds(r, 8)]
                return q0, [east * jnp.where(east > 0.0, a, b) for a, b in zip(q0, qp)]

            before = [zero, zero] if first == 0 else [down_one(f) for f in east_fluxes(first - 8)[1]]
            pending = None
            for r in range(first, last, 8):
                here = pl.ds(r, 8)
                q0, fe = east_fluxes(r)
                news = []
                for i in range(2):
                    shifted = down_one(fe[i])
                    fw = jnp.where(top, before[i], shifted)
                    before[i] = shifted
                    fn = ff[i, level, here]
                    spread = (fe[i] - fw) + (fn - south_of(fn))
                    new = own * (q0[i] - (0.5 * COURANT) * spread)
                    news.append(new)
                    if keep:
                        total = (tu, tv)[i]
                        term = weight[level] * new
                        total[here] = term if level == 0 else total[here] + term
                    spot = i * levels + level
                    if r == 0:
                        ends[0] = pick(ends[0], new, spot, 0)
                    if r + 8 == rows:
                        ends[1] = pick(ends[1], new, spot, 7)
                if pending is None:
                    pending = news
                else:
                    for i, out in enumerate(outs):
                        out[level, pl.ds(r - 8, 16)] = jnp.concatenate([pending[i], news[i]], axis=0).astype(BF16)
                    pending = None
        if first == 0:
            edges[slot] = ends[0]
        if last == rows:
            edges[slot + 1] = ends[1]

    def forcing(r, low, high):
        t0, x0 = tv[pl.ds(r, 8)], tu[pl.ds(r, 8)]
        north, south = sides(t0)
        after = jnp.where(bottom, up_one(tu[pl.ds(r + 8, 8)]) if r + 8 < high else 0.0, up_one(x0))
        prior = jnp.where(top, down_one(tu[pl.ds(r - 8, 8)]) if r > low else 0.0, down_one(x0))
        return (0.5 * own) * ((after - prior) + (north - south))

    def send(src, dst, sem, to):
        pltpu.make_async_remote_copy(
            src_ref=src, dst_ref=dst, send_sem=ssem.at[0], recv_sem=rsem.at[sem],
            device_id={"blk": to}, device_id_type=pl.DeviceIdType.MESH,
        ).start()

    def arrive(sem, height):
        lot = a4.at[pl.ds(0, height)]
        pltpu.make_async_remote_copy(
            src_ref=lot, dst_ref=lot, send_sem=ssem.at[0], recv_sem=rsem.at[sem],
            device_id={"blk": right}, device_id_type=pl.DeviceIdType.MESH,
        ).wait_recv()

    def send_left():
        send(uv_tx.at[0], uv_rx, 1, left)
        send(ae_tx, a4.at[pl.ds(WEST + rows, EAST)], 1, left)
        send(fe_tx, fe_rx, 1, left)

    chunks = lanes // 128

    def pack(ref, base, items):
        packed = {}
        for i, (x, place) in enumerate(items):
            for c in range(chunks):
                group, spot = divmod(i * chunks + c, 8)
                t = x[:, 128 * c : 128 * c + 128]
                if (spot - place) % 8:
                    t = pltpu.roll(t, (spot - place) % 8, 0)
                packed[group] = jnp.where(sub[:, :128] == spot, t, packed[group]) if group in packed else t
        for group, x in packed.items():
            ref[pl.ds(base + 8 * group, 8)] = x

    def unpack(ref, base, i):
        return jnp.concatenate(
            [jnp.broadcast_to(ref[pl.ds(base + i * chunks + c, 1)], (8, 128)) for c in range(chunks)], axis=1
        )

    def damping(first, last):
        for r in range(first, last, 8):
            a4[pl.ds(WEST + r, 8)] = 0.5 * (own * (6.0 + de[pl.ds(r, 8)]) + (1.0 - own)) - 2.0

    loads[2].wait()
    damping(late, rows)
    pack(mix_tx, 8 * chunks, [(a4[pl.ds(WEST + late, 8)], 7), (own, 7)])
    pair(split, rows, 2).wait()
    uv_tx[1] = gather_row((ue, ve), rows - 1)
    for c in range(chunks):
        mix_tx[pl.ds(8 * c, 8)] = uv_tx[1, :, 128 * c : 128 * c + 128]
    pass_barrier()
    send(mix_tx, mix_rx, 0, right)
    send(a4.at[pl.ds(WEST + late + 8, WEST - 8)], a4.at[pl.ds(8, WEST - 8)], 0, right)
    tell_earlier()
    for load in more:
        load.start()
    north_flux(late, rows, (ue, ve), True)
    flows(late, rows, (ue, ve), (bu, bv), 0, True)
    for r in range(late, rows, 8):
        f = forcing(r, late, rows)
        if r > late:
            basis[0, pl.ds(WEST + r, 8)] = f
            fw_tx[pl.ds(r - late - 8, 8)] = f
        else:
            pack(fx_tx, 0, [(f, 6), (f, 7), (tu[pl.ds(rows - 8, 8)], 7)])
    send(fw_tx, fw_rx, 0, right)
    send(fx_tx, fx_rx, 0, right)

    pair(0, split, 4).wait()
    uv_tx[0] = gather_row((ue, ve), 0)
    loads[7].wait()
    damping(0, late)
    for r in range(0, EAST, 8):
        a = a4[pl.ds(WEST + r, 8)]
        ae_tx[pl.ds(r, 8)] = jnp.where(bottom, own, a) if r + 8 == EAST else a
    north_flux(0, late, (ue, ve), True)
    flows(0, late, (ue, ve), (bu, bv), 0, True)
    for r in range(0, late + 8, 8):
        f = forcing(r, 0, rows)
        basis[0, pl.ds(WEST + r, 8)] = f
        if r < EAST:
            if r + 8 == EAST:
                f = jnp.where(bottom, jnp.broadcast_to(tu[pl.ds(0, 1)], (8, lanes)), f)
            fe_tx[pl.ds(r, 8)] = f
    pl.when(me > 0)(send_left)

    window = (-SHIFT, rows - SHIFT)

    def in_window(r, x):
        if r < window[0]:
            return jnp.where(sub >= window[0] - r, x, 0.0)
        if r + 8 > window[1]:
            return jnp.where(sub < window[1] - r, x, 0.0)
        return x

    def fold(x):
        return tree([x[:, c : c + 128] for c in range(0, lanes, 128)])

    def sweep(p, first, last, low, high, half_wet, summed, held=None):
        held = {} if held is None else held
        known = {}

        def field(q, r):
            return held[q, r] if (q, r) in held else basis[q, pl.ds(WEST + r, 8)]

        def block(r):
            if r not in known:
                k0 = field(p, r)
                known[r] = (k0, down_one(k0), up_one(k0))
            return known[r]

        squares, crosses = [], []
        turned = {}
        for r in range(first, last, 8):
            k0, down, up = block(r)
            prior = block(r - 8)[1] if r > low else down
            after = block(r + 8)[2] if r + 8 < high else up
            vert = jnp.where(top, prior, down) + jnp.where(bottom, after, up)
            turned[r] = vert, beside(k0 + 0.5 * vert)
        for r in range(first, last, 8):
            k0 = block(r)[0]
            vert, side = turned[r]
            here = pl.ds(WEST + r, 8)
            half = a4[here] * k0 - half_wet(r) * (vert + side)
            new = 0.5 * half if p == 0 else half - field(p - 1, r)
            basis[p + 1, here] = new
            held[p + 1, r] = new
            if summed[0] <= r < summed[1]:
                kept = in_window(r, k0)
                squares.append(kept * kept)
                crosses.append(kept * in_window(r, new))
        for key in [key for key in held if key[0] < p]:
            del held[key]
        return [tree([fold(t) for t in x]) for x in (squares, crosses) if x]

    def floor8(x):
        return x // 8 * 8

    def ceil8(x):
        return -(-x // 8) * 8

    inner_from, inner_to = ceil8(SWEEPS + 2), rows - SHIFT
    for p in range(SWEEPS):
        j = p + 1
        sums = sweep(
            p, floor8(2 + j), ceil8(rows - 2 - j), 0, rows, lambda r: half_own, (inner_from, inner_to)
        )
        for i, x in enumerate(sums):
            acc[2 * p + i] = x

    pltpu.make_async_copy(ff, ff, lsem.at[5]).wait()
    hs_tx[0] = gather_row((he, se), 0)
    hs_tx[1] = gather_row((he, se), rows - 1)
    send(hs_tx.at[1], hs_rx.at[0], 2, right)
    pl.when(me > 0)(lambda: send(hs_tx.at[0], hs_rx.at[1], 2, left))

    def tracers():
        north_flux(0, rows, (he, se), False)
        flows(0, rows, (he, se), (bh, bs), 2, False)

    def total_of(x):
        for step in (4, 2, 1):
            x = x + pltpu.roll(x, step, 0)
        return x

    def face(low, high, both):
        twice = [jnp.where(sub < levels, x, pltpu.roll(x, levels, 0)) for x in (low, high)]
        return 0.5 * (twice[0] + twice[1]) * both

    def seam(uv_low, uv_high, wet_low, wet_high, tu_low, tu_high, f_low, f_high):
        speed = face(uv_low, uv_high, wet_low * wet_high)
        flux = speed * jnp.where(speed > 0.0, uv_low, uv_high)
        term = level_weight * flux
        gu = total_of(jnp.where(sub < levels, term, 0.0))
        gv = total_of(jnp.where(sub < levels, 0.0, term))
        low_u, high_u = (-COURANT * wet_low) * gu, (COURANT * wet_high) * gu
        low_v, high_v = (-COURANT * wet_low) * gv, (COURANT * wet_high) * gv
        north, south = sides(jnp.where(sub < 4, high_v, low_v))
        across = north - south
        f_low = f_low + (0.5 * wet_low) * jnp.where(
            sub == 7, (tu_high + high_u) + across, jnp.where(sub == 6, low_u, 0.0)
        )
        f_high = f_high + (0.5 * wet_high) * jnp.where(
            sub == 0, across - (tu_low + low_u), jnp.where(sub == 1, -high_u, 0.0)
        )
        return speed, flux, f_low, f_high

    def row_of(ref, row):
        return jnp.broadcast_to(ref[pl.ds(row, 1)], (8, lanes))

    def tracers_and_east(both=True):
        if both:
            tracers()
        arrive(1, 2 * EAST + 8)
        east = row_of(a4, WEST + rows + EAST - 1)
        _, flux, f_low, f_high = seam(
            uv_tx[1], uv_rx[...], own, east, row_of(tu, rows - 1), row_of(fe_rx, EAST - 1),
            basis[0, pl.ds(WEST + rows - 8, 8)], fe_rx[pl.ds(0, 8)],
        )
        flux_e[...] = flux
        basis[0, pl.ds(WEST + rows - 8, 8)] = f_low
        basis[0, pl.ds(WEST + rows, 8)] = f_high
        for r in range(8, EAST, 8):
            basis[0, pl.ds(WEST + rows + r, 8)] = fe_rx[pl.ds(r, 8)]
        held = {}
        half_east = 0.5 * east
        for p in range(SWEEPS):
            j = p + 1
            sweep(
                p, floor8(rows - 2 - j), ceil8(rows + SWEEPS - j), 0, rows + EAST,
                lambda r: half_own if r < rows else half_east, (0, 0), held,
            )

    def before_west():
        tracers()
        hear_late()
        send_left()
        send(hs_tx.at[0], hs_rx.at[1], 2, left)
        tracers_and_east(False)

    pl.when(at_start)(before_west)

    arrive(0, west_rows)
    west = unpack(mix_rx, 8 * chunks, 1)
    a4[pl.ds(0, 8)] = unpack(mix_rx, 8 * chunks, 0)
    uv_west = jnp.concatenate([mix_rx[pl.ds(8 * c, 8)] for c in range(chunks)], axis=1)
    speed_w, flux_w, f_low, f_high = seam(
        uv_west, uv_tx[0], west, own, unpack(fx_rx, 0, 2), row_of(tu, 0),
        fw_rx[pl.ds(WEST - 16, 8)], basis[0, pl.ds(WEST, 8)],
    )
    basis[0, pl.ds(0, 8)] = jnp.where(bottom, unpack(fx_rx, 0, 1), unpack(fx_rx, 0, 0))
    for r in range(8, WEST - 8, 8):
        basis[0, pl.ds(r, 8)] = fw_rx[pl.ds(r - 8, 8)]
    basis[0, pl.ds(WEST - 8, 8)] = f_low
    basis[0, pl.ds(WEST, 8)] = f_high

    moments = [None] * MOMENTS
    west_held = {}
    half_west = 0.5 * west
    for p in range(SWEEPS):
        j = p + 1
        sums = sweep(
            p, floor8(j - 2 * SWEEPS - 2), ceil8(2 + j) if j < SWEEPS else inner_from, -WEST, rows,
            lambda r: half_west if r < 0 else half_own, (floor8(-SHIFT), 8), west_held,
        )
        for i, x in enumerate(sums):
            moments[2 * p + i] = x
        tail = []
        for r in range(8, inner_from, 8):
            k0, k1 = basis[p, pl.ds(WEST + r, 8)], basis[p + 1, pl.ds(WEST + r, 8)]
            tail.append((k0 * k0, k0 * k1))
        for i in range(len(sums)):
            moments[2 * p + i] = tree(
                [moments[2 * p + i], acc[2 * p + i]] + [fold(t[i]) for t in tail]
            )
    base = moments[:2]
    moments = base + [2.0 * x - base[i % 2] for i, x in enumerate(moments[2:])]
    spread = jnp.zeros((8, 128), F32)
    for i, x in enumerate(moments):
        spread = jnp.where(lane[:, :128] == i, jnp.sum(x, axis=1, keepdims=True), spread)
    slots[me] = jnp.sum(spread, axis=0, keepdims=True)
    pl.when(me > 0)(hear_late)
    for k in range(n - 1):
        pltpu.make_async_remote_copy(
            src_ref=slots.at[me], dst_ref=slots.at[me],
            send_sem=gsem.at[0], recv_sem=gsem.at[1],
            device_id={"blk": k + jnp.where(k >= me, 1, 0)}, device_id_type=pl.DeviceIdType.MESH,
        ).start()

    pl.when(me > 0)(tracers_and_east)
    arrive(2, 16)

    def mend(outs, fixed, row):
        block, place = row // 8 * 8, row % 8
        for i, out in enumerate(outs):
            for level in range(levels):
                spot = i * levels + level
                old = out[level, pl.ds(block, 8)].astype(F32)
                x = pltpu.roll(fixed, (place - spot) % 8, 0) if (place - spot) % 8 else fixed
                out[level, pl.ds(block, 8)] = jnp.where(sub == place, x, old).astype(BF16)

    def carried(speed, low, high):
        return speed * jnp.where(speed > 0.0, low, high)

    mend((bu, bv), edges[0] + (COURANT * own) * flux_w, 0)
    mend((bu, bv), edges[1] - (COURANT * own) * flux_e[...], rows - 1)
    east = row_of(a4, WEST + rows + EAST - 1)
    speed_e = face(uv_tx[1], uv_rx[...], own * east)
    mend((bh, bs), edges[2] + (COURANT * own) * carried(speed_w, hs_rx[0], hs_tx[0]), 0)
    mend((bh, bs), edges[3] - (COURANT * own) * carried(speed_e, hs_tx[1], hs_rx[1]), rows - 1)

    others = slots.at[pl.ds(0, n - 1)]
    rest = pltpu.make_async_remote_copy(
        src_ref=others, dst_ref=others, send_sem=gsem.at[0], recv_sem=gsem.at[1],
        device_id={"blk": right}, device_id_type=pl.DeviceIdType.MESH,
    )
    rest.wait_recv()
    mom[...] = jnp.broadcast_to(tree([slots[i] for i in range(n)]), (8, 128))
    rest.wait_send()
    lot = a4.at[pl.ds(0, west_rows + 2 * EAST + 24)]
    pltpu.make_async_remote_copy(
        src_ref=lot, dst_ref=lot, send_sem=ssem.at[0], recv_sem=rsem.at[0],
        device_id={"blk": right}, device_id_type=pl.DeviceIdType.MESH,
    ).wait_send()


def finish(bh, bs, bu, bv, basis, mom, o_heat, o_salt, o_u, o_v, o_height, o_resid, hgt, res, sems):
    rows, lanes = hgt.shape
    stores = [
        pltpu.make_async_copy(src, dst, sems.at[0])
        for src, dst in ((bh, o_heat), (bs, o_salt), (bu, o_u), (bv, o_v))
    ]
    for store in stores:
        store.start()
    row = mom[...]
    m = [jnp.broadcast_to(row[:, i : i + 1], (8, 128)) for i in range(MOMENTS)]
    offset, resid = inner_steps(m, SWEEPS)

    def combine(vals, coef):
        return tree([c * v for v, c in zip(vals, coef) if c is not None])

    parts = 2
    step = rows // 8 // parts
    for part in range(parts):
        for s in range(part * step, (part + 1) * step):
            r = 8 * s
            for c in range(0, lanes, 128):
                vals = [basis[i, pl.ds(WEST + r, 8), c : c + 128] for i in range(FIELDS)]
                hgt[pl.ds(r, 8), c : c + 128] = combine(vals, offset)
                res[pl.ds(r, 8), c : c + 128] = combine(vals, resid)
        span = pl.ds(part * step * 8, step * 8)
        for src, dst in ((hgt, o_height), (res, o_resid)):
            pltpu.make_async_copy(src.at[span], dst.at[span], sems.at[1]).start()
    levels = bh.shape[0]
    for sem, count in ((0, 2 * levels), (1, 2)):
        lot = basis.at[pl.ds(0, count), pl.ds(0, rows)]
        pltpu.make_async_copy(lot, lot, sems.at[sem]).wait()


def on_device(heat, salt, uvel, vvel, spacing, damp, flags):
    n = lax.axis_size("blk")
    levels, rows, lanes = uvel.shape
    total = WEST + rows + EAST
    chunks = lanes // 128
    mixed, extra = 8 * chunks + -(-2 * chunks // 8) * 8, -(-3 * chunks // 8) * 8
    extra += -(mixed + extra) % (8 * chunks)
    hbm = pl.BlockSpec(memory_space=pltpu.HBM)
    vmem = pl.BlockSpec(memory_space=pltpu.VMEM)
    args = [
        pltpu.with_memory_space_constraint(x, pltpu.HBM)
        for x in (heat, salt, uvel, vvel, spacing, damp, flags)
    ]
    vm = pltpu.VMEM
    half = jax.ShapeDtypeStruct((levels, rows, lanes), BF16)
    flat = jax.ShapeDtypeStruct((rows, lanes), F32)
    full = vm((levels, rows, lanes), F32)
    dma = pltpu.SemaphoreType.DMA
    mids = (
        half, half, half, half,
        jax.ShapeDtypeStruct((FIELDS, total, lanes), F32),
        jax.ShapeDtypeStruct((8, 128), F32),
    )
    results = pl.pallas_call(
        functools.partial(kernel, n),
        out_shape=mids,
        in_specs=[hbm] * 7,
        out_specs=(vmem,) * 6,
        scratch_shapes=[
            full, full, full, full, full, full,
            vm((2, levels, rows, lanes), F32),
            vm((rows, lanes), F32),
            vm((rows, lanes), F32),
            vm((rows, lanes), F32),
            vm((MOMENTS, 8, 128), F32),
            vm((4, 8, lanes), F32),
            vm((2, 8, lanes), F32),
            vm((2, 8, lanes), F32),
            vm((8, lanes), F32),
            vm((2, 8, lanes), F32),
            vm((mixed, 128), F32),
            vm((mixed, 128), F32),
            vm((extra, 128), F32),
            vm((extra, 128), F32),
            vm((EAST, lanes), F32),
            vm((total, lanes), F32),
            vm((WEST - 8, lanes), F32),
            vm((EAST, lanes), F32),
            vm((WEST - 8, lanes), F32),
            vm((EAST, lanes), F32),
            vm((n, 1, 128), F32),
            pltpu.SMEM(spacing.shape, F32),
            pltpu.SMEM(flags.shape, flags.dtype),
            vm((8, lanes), F32),
            dma((7,)),
            dma((1,)),
            dma((3,)),
            dma((2,)),
            pltpu.SemaphoreType.REGULAR((1,)),
        ],
        compiler_params=pltpu.CompilerParams(
            collective_id=0, has_side_effects=True, vmem_limit_bytes=40 * 1024 * 1024
        ),
    )(*args)
    results = [pltpu.with_memory_space_constraint(x, pltpu.VMEM) for x in results]
    shapes = (half, half, half, half, flat, flat)
    return pl.pallas_call(
        finish,
        out_shape=tuple(pltpu.HBM(x.shape, x.dtype) for x in shapes),
        in_specs=[vmem] * 6,
        out_specs=(hbm,) * 6,
        scratch_shapes=[vm((rows, lanes), F32), vm((rows, lanes), F32), dma((2,))],
        compiler_params=pltpu.CompilerParams(vmem_limit_bytes=8 * 1024 * 1024),
    )(*results)


def solution(mesh):
    return jax.shard_map(
        on_device,
        mesh=mesh,
        in_specs=(
            P("member", "blk", None),
            P("member", "blk", None),
            P("member", "blk", None),
            P("member", "blk", None),
            P(),
            P("blk", None),
            P("blk", None),
        ),
        out_specs=(
            P("member", "blk", None),
            P("member", "blk", None),
            P("member", "blk", None),
            P("member", "blk", None),
            P(("member", "blk"), None),
            P(("member", "blk"), None),
        ),
        check_vma=False,
    )
```

```python
import functools

import jax
import jax.numpy as jnp
import numpy as np
from jax import lax
from jax.experimental import pallas as pl
from jax.experimental.pallas import tpu as pltpu
from jax.sharding import PartitionSpec as P

SSTEP = 4
CG_BLOCKS = 3
SWEEPS = SSTEP * CG_BLOCKS
FIELDS = SWEEPS + 1
MOMENTS = 2 * SWEEPS
COURANT = 0.2
SHIFT = SWEEPS + 2
WEST = -(-(2 * SWEEPS + 2) // 8) * 8
EAST = -(-(SWEEPS + 2) // 8) * 8
F32 = jnp.float32
BF16 = jnp.bfloat16


def shift_table(extent):
    table = np.zeros((extent, extent), np.float32)
    for source in range(extent - 1):
        if source == 0:
            table[1, 0] = table[0, 0] = 0.5
        else:
            table[source + 1, source] = 0.25
            table[source, source] = 0.5
            table[source - 1, source] = 0.25
    return table


def tree(terms):
    while len(terms) > 1:
        terms = [
            terms[i] + terms[i + 1] if i + 1 < len(terms) else terms[i]
            for i in range(0, len(terms), 2)
        ]
    return terms[0]


def plus(a, b):
    if a is None:
        return b
    if b is None:
        return a
    return a + b


def scaled(scale, a):
    return None if a is None else scale * a


def inner_steps(m, sweeps):
    extent = sweeps + 1
    table = shift_table(extent)
    ones = jnp.ones_like(m[0])
    pushed = [0.25 * (m[k + 1] + m[abs(k - 1)]) + 0.5 * m[k] for k in range(2 * sweeps - 1)]
    a = [[pushed[i + j] + pushed[i - j] for j in range(i + 1)] for i in range(sweeps)]
    lower = [[None] * sweeps for _ in range(sweeps)]
    inverse = []
    y = [m[i] + m[i] for i in range(sweeps)]
    for k in range(sweeps):
        inverse.append(ones / a[k][k])
        for i in range(k + 1, sweeps):
            lower[i][k] = a[i][k] * inverse[k]
        for i in range(k + 1, sweeps):
            for j in range(k + 1, i + 1):
                a[i][j] = a[i][j] - lower[i][k] * a[j][k]
            y[i] = y[i] - lower[i][k] * y[k]

    def backward(y):
        z = [v * d for v, d in zip(y, inverse)]
        for i in range(sweeps - 1, 0, -1):
            for j in range(i):
                z[j] = z[j] - lower[i][j] * z[i]
        return z

    def image(c):
        out = []
        for i in range(extent):
            total = None
            for j in range(sweeps):
                if table[i, j] != 0.0:
                    total = plus(total, scaled(float(table[i, j]), c[j]))
            out.append(total)
        return out

    offset = backward(y)
    resid = [-x for x in image(offset)]
    resid[0] = resid[0] + ones
    y = [
        tree([(m[i + j] + m[abs(i - j)]) * resid[j] for j in range(extent)]) for i in range(sweeps)
    ]
    for i in range(sweeps):
        for j in range(i + 1, sweeps):
            y[j] = y[j] - lower[j][i] * y[i]
    more = backward(y)
    offset = [c + d for c, d in zip(offset, more)]
    resid = [r - x for r, x in zip(resid, image(more))]
    return offset, resid


def kernel(
    n,
    heat, salt, uvel, vvel, spacing, damp, flags,
    bh, bs, bu, bv, basis, mom,
    ue, ve, he, se, ef, nf, ff, de, tu, tv, acc, edges,
    uv_tx, hs_tx, uv_rx, hs_rx, mix_tx, mix_rx, fx_tx, fx_rx, ae_tx, a4, fw_tx, fe_tx, fw_rx, fe_rx, slots,
    space, marks,
    flux_e, lsem, ssem, rsem, gsem, late_sem,
):
    levels, rows, lanes = ue.shape
    me = lax.axis_index("blk")
    right, left = lax.rem(me + 1, n), lax.rem(me + n - 1, n)
    late = rows - WEST
    west_rows = 2 * (WEST - 8) + (mix_tx.shape[0] + fx_tx.shape[0]) * 128 // lanes
    split = late - 8

    def part(ref, buf, lo, hi, sem):
        return pltpu.make_async_copy(
            ref.at[:, pl.ds(lo, hi - lo)], buf.at[:, pl.ds(lo, hi - lo)], lsem.at[sem]
        )

    def pair(lo, hi, sem):
        both = ff.at[:, :, pl.ds(lo, hi - lo)]
        return pltpu.make_async_copy(both, both, lsem.at[sem])

    loads = [
        pltpu.make_async_copy(flags, marks, lsem.at[0]),
        pltpu.make_async_copy(spacing, space, lsem.at[1]),
        pltpu.make_async_copy(damp.at[pl.ds(late, WEST)], de.at[pl.ds(late, WEST)], lsem.at[3]),
        part(uvel, ue, split, rows, 2),
        part(vvel, ve, split, rows, 2),
        part(uvel, ue, 0, split, 4),
        part(vvel, ve, 0, split, 4),
        pltpu.make_async_copy(damp.at[pl.ds(0, late)], de.at[pl.ds(0, late)], lsem.at[5]),
    ]
    more = [
        pltpu.make_async_copy(heat, he, lsem.at[2]),
        pltpu.make_async_copy(salt, se, lsem.at[2]),
    ]
    barrier = pltpu.get_barrier_semaphore()

    def tell(sem, to):
        pl.semaphore_signal(
            sem, inc=1, device_id={"blk": to}, device_id_type=pl.DeviceIdType.MESH
        )

    at_start, at_end = me == 0, me == n - 1
    pl.when(me > 0)(lambda: tell(barrier, left))
    for load in loads[:5]:
        load.start()
    for k in range(1, n):
        pl.when(me + k < n)(functools.partial(tell, barrier, lax.rem(me + k, n)))
    for load in loads[5:]:
        load.start()

    def pass_barrier():
        pl.semaphore_wait(barrier, jnp.where(at_end, n - 1, me + 1))

    def tell_earlier():
        for k in range(2, n):
            pl.when(me - k >= 0)(functools.partial(tell, late_sem.at[0], lax.rem(me + n - k, n)))

    def hear_late():
        later = n - 2 - me
        pl.when(later > 0)(lambda: pl.semaphore_wait(late_sem.at[0], later))

    lane = lax.broadcasted_iota(jnp.int32, (8, lanes), 1)
    sub = lax.broadcasted_iota(jnp.int32, (8, lanes), 0)
    top, bottom = sub == 0, sub == 7
    zero = jnp.zeros((8, lanes), F32)

    def north_of(x):
        return pltpu.roll(x, lanes - 1, 1)

    def south_of(x):
        return pltpu.roll(x, 1, 1)

    def sides(x):
        return jnp.where(lane == lanes - 1, 0.0, north_of(x)), jnp.where(lane == 0, 0.0, south_of(x))

    slim = lane[:, :128]

    def beside(x):
        tiles = [x[:, c : c + 128] for c in range(0, lanes, 128)]
        north = [pltpu.roll(t, 127, 1) for t in tiles] + [0.0]
        south = [pltpu.roll(t, 1, 1) for t in tiles]
        south = [0.0] + south
        return jnp.concatenate(
            [
                jnp.where(slim == 127, north[i + 1], north[i]) + jnp.where(slim == 0, south[i], south[i + 1])
                for i in range(len(tiles))
            ],
            axis=1,
        )

    def up_one(x):
        return pltpu.roll(x, 7, 0)

    def down_one(x):
        return pltpu.roll(x, 1, 0)

    loads[0].wait()
    loads[1].wait()
    tiles = marks.shape[1]
    lane_tile = lane // (lanes // tiles)
    own = zero
    for k in range(tiles):
        own = jnp.where(lane_tile == k, marks[0, k].astype(F32), own)
    ahead = jnp.where(lane == lanes - 1, 0.0, own * north_of(own))
    half_own = 0.5 * own
    whole_w = jnp.zeros((8, 128), F32)
    for j in range(levels):
        whole_w = whole_w + space[j]
    portions = [jnp.full((8, 128), space[j], F32) / whole_w for j in range(levels)]

    def wide(x):
        return jnp.concatenate([x] * (lanes // 128), axis=1)

    weight = [wide(x) for x in portions]
    level_weight = zero
    for j in range(levels):
        level_weight = jnp.where(sub % levels == j, weight[j], level_weight)

    def gather_row(refs, row):
        block, place = row // 8 * 8, row % 8
        packed = None
        for i, ref in enumerate(refs):
            for level in range(levels):
                x = ref[level, pl.ds(block, 8)]
                spot = i * levels + level
                if (spot - place) % 8:
                    x = pltpu.roll(x, (spot - place) % 8, 0)
                packed = x if packed is None else jnp.where(sub == spot, x, packed)
        return packed

    def pick(packed, block, spot, place):
        return jnp.where(sub == spot, pltpu.roll(block, (spot - place) % 8, 0) if (spot - place) % 8 else block, packed)

    def north_flux(first, last, fields, keep):
        for level in range(levels):
            for r in range(first, last, 8):
                here = pl.ds(r, 8)
                q0 = [ref[level, here] for ref in fields]
                qn = [north_of(q) for q in q0]
                if keep:
                    north = (q0[1] + qn[1]) * ahead
                    nf[level, here] = north
                else:
                    north = nf[level, here]
                for i in range(2):
                    ff[i, level, here] = north * jnp.where(north > 0.0, q0[i], qn[i])

    def flows(first, last, fields, outs, slot, keep):
        ends = [zero, zero]
        for level in range(levels):
            def ahead_of(ref, r, q0):
                if r + 8 < rows:
                    return jnp.where(bottom, up_one(ref[level, pl.ds(r + 8, 8)]), up_one(q0))
                return up_one(q0)

            def east_fluxes(r):
                q0 = [ref[level, pl.ds(r, 8)] for ref in fields]
                qp = [ahead_of(ref, r, q) for ref, q in zip(fields, q0)]
                if keep:
                    east = q0[0] + qp[0]
                    if r + 8 == rows:
                        east = jnp.where(bottom, 0.0, east)
                    ef[level, pl.ds(r, 8)] = east
                else:
                    east = ef[level, pl.ds(r, 8)]
                return q0, [east * jnp.where(east > 0.0, a, b) for a, b in zip(q0, qp)]

            before = [zero, zero] if first == 0 else [down_one(f) for f in east_fluxes(first - 8)[1]]
            pending = None
            for r in range(first, last, 8):
                here = pl.ds(r, 8)
                q0, fe = east_fluxes(r)
                news = []
                for i in range(2):
                    shifted = down_one(fe[i])
                    fw = jnp.where(top, before[i], shifted)
                    before[i] = shifted
                    fn = ff[i, level, here]
                    spread = (fe[i] - fw) + (fn - south_of(fn))
                    new = own * (q0[i] - (0.5 * COURANT) * spread)
                    news.append(new)
                    if keep:
                        total = (tu, tv)[i]
                        term = weight[level] * new
                        total[here] = term if level == 0 else total[here] + term
                    spot = i * levels + level
                    if r == 0:
                        ends[0] = pick(ends[0], new, spot, 0)
                    if r + 8 == rows:
                        ends[1] = pick(ends[1], new, spot, 7)
                if pending is None:
                    pending = news
                else:
                    for i, out in enumerate(outs):
                        out[level, pl.ds(r - 8, 16)] = jnp.concatenate([pending[i], news[i]], axis=0).astype(BF16)
                    pending = None
        if first == 0:
            edges[slot] = ends[0]
        if last == rows:
            edges[slot + 1] = ends[1]

    def forcing(r, low, high):
        t0, x0 = tv[pl.ds(r, 8)], tu[pl.ds(r, 8)]
        north, south = sides(t0)
        after = jnp.where(bottom, up_one(tu[pl.ds(r + 8, 8)]) if r + 8 < high else 0.0, up_one(x0))
        prior = jnp.where(top, down_one(tu[pl.ds(r - 8, 8)]) if r > low else 0.0, down_one(x0))
        return (0.5 * own) * ((after - prior) + (north - south))

    def send(src, dst, sem, to):
        pltpu.make_async_remote_copy(
            src_ref=src, dst_ref=dst, send_sem=ssem.at[0], recv_sem=rsem.at[sem],
            device_id={"blk": to}, device_id_type=pl.DeviceIdType.MESH,
        ).start()

    def arrive(sem, height):
        lot = a4.at[pl.ds(0, height)]
        pltpu.make_async_remote_copy(
            src_ref=lot, dst_ref=lot, send_sem=ssem.at[0], recv_sem=rsem.at[sem],
            device_id={"blk": right}, device_id_type=pl.DeviceIdType.MESH,
        ).wait_recv()

    def send_left():
        send(uv_tx.at[0], uv_rx, 1, left)
        send(ae_tx, a4.at[pl.ds(WEST + rows, EAST)], 1, left)
        send(fe_tx, fe_rx, 1, left)

    chunks = lanes // 128

    def pack(ref, base, items):
        packed = {}
        for i, (x, place) in enumerate(items):
            for c in range(chunks):
                group, spot = divmod(i * chunks + c, 8)
                t = x[:, 128 * c : 128 * c + 128]
                if (spot - place) % 8:
                    t = pltpu.roll(t, (spot - place) % 8, 0)
                packed[group] = jnp.where(sub[:, :128] == spot, t, packed[group]) if group in packed else t
        for group, x in packed.items():
            ref[pl.ds(base + 8 * group, 8)] = x

    def unpack(ref, base, i):
        return jnp.concatenate(
            [jnp.broadcast_to(ref[pl.ds(base + i * chunks + c, 1)], (8, 128)) for c in range(chunks)], axis=1
        )

    def damping(first, last):
        for r in range(first, last, 8):
            a4[pl.ds(WEST + r, 8)] = 0.5 * (own * (6.0 + de[pl.ds(r, 8)]) + (1.0 - own)) - 2.0

    loads[2].wait()
    damping(late, rows)
    pack(mix_tx, 8 * chunks, [(a4[pl.ds(WEST + late, 8)], 7), (own, 7)])
    pair(split, rows, 2).wait()
    uv_tx[1] = gather_row((ue, ve), rows - 1)
    for c in range(chunks):
        mix_tx[pl.ds(8 * c, 8)] = uv_tx[1, :, 128 * c : 128 * c + 128]
    pass_barrier()
    send(mix_tx, mix_rx, 0, right)
    send(a4.at[pl.ds(WEST + late + 8, WEST - 8)], a4.at[pl.ds(8, WEST - 8)], 0, right)
    tell_earlier()
    for load in more:
        load.start()
    north_flux(late, rows, (ue, ve), True)
    flows(late, rows, (ue, ve), (bu, bv), 0, True)
    for r in range(late, rows, 8):
        f = forcing(r, late, rows)
        if r > late:
            basis[0, pl.ds(WEST + r, 8)] = f
            fw_tx[pl.ds(r - late - 8, 8)] = f
        else:
            pack(fx_tx, 0, [(f, 6), (f, 7), (tu[pl.ds(rows - 8, 8)], 7)])
    send(fw_tx, fw_rx, 0, right)
    send(fx_tx, fx_rx, 0, right)

    pair(0, split, 4).wait()
    uv_tx[0] = gather_row((ue, ve), 0)
    loads[7].wait()
    damping(0, late)
    for r in range(0, EAST, 8):
        a = a4[pl.ds(WEST + r, 8)]
        ae_tx[pl.ds(r, 8)] = jnp.where(bottom, own, a) if r + 8 == EAST else a
    north_flux(0, late, (ue, ve), True)
    flows(0, late, (ue, ve), (bu, bv), 0, True)
    for r in range(0, late + 8, 8):
        f = forcing(r, 0, rows)
        basis[0, pl.ds(WEST + r, 8)] = f
        if r < EAST:
            if r + 8 == EAST:
                f = jnp.where(bottom, jnp.broadcast_to(tu[pl.ds(0, 1)], (8, lanes)), f)
            fe_tx[pl.ds(r, 8)] = f
    pl.when(me > 0)(send_left)

    window = (-SHIFT, rows - SHIFT)

    def in_window(r, x):
        if r < window[0]:
            return jnp.where(sub >= window[0] - r, x, 0.0)
        if r + 8 > window[1]:
            return jnp.where(sub < window[1] - r, x, 0.0)
        return x

    def fold(x):
        return tree([x[:, c : c + 128] for c in range(0, lanes, 128)])

    def sweep(p, first, last, low, high, half_wet, summed, held=None):
        held = {} if held is None else held
        known = {}

        def field(q, r):
            return held[q, r] if (q, r) in held else basis[q, pl.ds(WEST + r, 8)]

        def block(r):
            if r not in known:
                k0 = field(p, r)
                known[r] = (k0, down_one(k0), up_one(k0))
            return known[r]

        squares, crosses = [], []
        turned = {}
        for r in range(first, last, 8):
            k0, down, up = block(r)
            prior = block(r - 8)[1] if r > low else down
            after = block(r + 8)[2] if r + 8 < high else up
            vert = jnp.where(top, prior, down) + jnp.where(bottom, after, up)
            turned[r] = vert, beside(k0 + 0.5 * vert)
        for r in range(first, last, 8):
            k0 = block(r)[0]
            vert, side = turned[r]
            here = pl.ds(WEST + r, 8)
            half = a4[here] * k0 - half_wet(r) * (vert + side)
            new = 0.5 * half if p == 0 else half - field(p - 1, r)
            basis[p + 1, here] = new
            held[p + 1, r] = new
            if summed[0] <= r < summed[1]:
                kept = in_window(r, k0)
                squares.append(kept * kept)
                crosses.append(kept * in_window(r, new))
        for key in [key for key in held if key[0] < p]:
            del held[key]
        return [tree([fold(t) for t in x]) for x in (squares, crosses) if x]

    def floor8(x):
        return x // 8 * 8

    def ceil8(x):
        return -(-x // 8) * 8

    inner_from, inner_to = ceil8(SWEEPS + 2), rows - SHIFT
    for p in range(SWEEPS):
        j = p + 1
        sums = sweep(
            p, floor8(2 + j), ceil8(rows - 2 - j), 0, rows, lambda r: half_own, (inner_from, inner_to)
        )
        for i, x in enumerate(sums):
            acc[2 * p + i] = x

    pltpu.make_async_copy(ff, ff, lsem.at[2]).wait()
    hs_tx[0] = gather_row((he, se), 0)
    hs_tx[1] = gather_row((he, se), rows - 1)
    send(hs_tx.at[1], hs_rx.at[0], 2, right)
    pl.when(me > 0)(lambda: send(hs_tx.at[0], hs_rx.at[1], 2, left))

    def tracers():
        north_flux(0, rows, (he, se), False)
        flows(0, rows, (he, se), (bh, bs), 2, False)

    def total_of(x):
        for step in (4, 2, 1):
            x = x + pltpu.roll(x, step, 0)
        return x

    def face(low, high, both):
        twice = [jnp.where(sub < levels, x, pltpu.roll(x, levels, 0)) for x in (low, high)]
        return 0.5 * (twice[0] + twice[1]) * both

    def seam(uv_low, uv_high, wet_low, wet_high, tu_low, tu_high, f_low, f_high):
        speed = face(uv_low, uv_high, wet_low * wet_high)
        flux = speed * jnp.where(speed > 0.0, uv_low, uv_high)
        term = level_weight * flux
        gu = total_of(jnp.where(sub < levels, term, 0.0))
        gv = total_of(jnp.where(sub < levels, 0.0, term))
        low_u, high_u = (-COURANT * wet_low) * gu, (COURANT * wet_high) * gu
        low_v, high_v = (-COURANT * wet_low) * gv, (COURANT * wet_high) * gv
        north, south = sides(jnp.where(sub < 4, high_v, low_v))
        across = north - south
        f_low = f_low + (0.5 * wet_low) * jnp.where(
            sub == 7, (tu_high + high_u) + across, jnp.where(sub == 6, low_u, 0.0)
        )
        f_high = f_high + (0.5 * wet_high) * jnp.where(
            sub == 0, across - (tu_low + low_u), jnp.where(sub == 1, -high_u, 0.0)
        )
        return speed, flux, f_low, f_high

    def row_of(ref, row):
        return jnp.broadcast_to(ref[pl.ds(row, 1)], (8, lanes))

    def tracers_and_east(both=True):
        if both:
            tracers()
        arrive(1, 2 * EAST + 8)
        east = row_of(a4, WEST + rows + EAST - 1)
        _, flux, f_low, f_high = seam(
            uv_tx[1], uv_rx[...], own, east, row_of(tu, rows - 1), row_of(fe_rx, EAST - 1),
            basis[0, pl.ds(WEST + rows - 8, 8)], fe_rx[pl.ds(0, 8)],
        )
        flux_e[...] = flux
        basis[0, pl.ds(WEST + rows - 8, 8)] = f_low
        basis[0, pl.ds(WEST + rows, 8)] = f_high
        for r in range(8, EAST, 8):
            basis[0, pl.ds(WEST + rows + r, 8)] = fe_rx[pl.ds(r, 8)]
        held = {}
        half_east = 0.5 * east
        for p in range(SWEEPS):
            j = p + 1
            sweep(
                p, floor8(rows - 2 - j), ceil8(rows + SWEEPS - j), 0, rows + EAST,
                lambda r: half_own if r < rows else half_east, (0, 0), held,
            )

    def before_west():
        tracers()
        hear_late()
        send_left()
        send(hs_tx.at[0], hs_rx.at[1], 2, left)
        tracers_and_east(False)

    pl.when(at_start)(before_west)

    arrive(0, west_rows)
    west = unpack(mix_rx, 8 * chunks, 1)
    a4[pl.ds(0, 8)] = unpack(mix_rx, 8 * chunks, 0)
    uv_west = jnp.concatenate([mix_rx[pl.ds(8 * c, 8)] for c in range(chunks)], axis=1)
    speed_w, flux_w, f_low, f_high = seam(
        uv_west, uv_tx[0], west, own, unpack(fx_rx, 0, 2), row_of(tu, 0),
        fw_rx[pl.ds(WEST - 16, 8)], basis[0, pl.ds(WEST, 8)],
    )
    basis[0, pl.ds(0, 8)] = jnp.where(bottom, unpack(fx_rx, 0, 1), unpack(fx_rx, 0, 0))
    for r in range(8, WEST - 8, 8):
        basis[0, pl.ds(r, 8)] = fw_rx[pl.ds(r - 8, 8)]
    basis[0, pl.ds(WEST - 8, 8)] = f_low
    basis[0, pl.ds(WEST, 8)] = f_high

    moments = [None] * MOMENTS
    west_held = {}
    half_west = 0.5 * west
    for p in range(SWEEPS):
        j = p + 1
        sums = sweep(
            p, floor8(j - 2 * SWEEPS - 2), ceil8(2 + j) if j < SWEEPS else inner_from, -WEST, rows,
            lambda r: half_west if r < 0 else half_own, (floor8(-SHIFT), 8), west_held,
        )
        for i, x in enumerate(sums):
            moments[2 * p + i] = x
        tail = []
        for r in range(8, inner_from, 8):
            k0, k1 = basis[p, pl.ds(WEST + r, 8)], basis[p + 1, pl.ds(WEST + r, 8)]
            tail.append((k0 * k0, k0 * k1))
        for i in range(len(sums)):
            moments[2 * p + i] = tree(
                [moments[2 * p + i], acc[2 * p + i]] + [fold(t[i]) for t in tail]
            )
    base = moments[:2]
    moments = base + [2.0 * x - base[i % 2] for i, x in enumerate(moments[2:])]
    spread = jnp.zeros((8, 128), F32)
    for i, x in enumerate(moments):
        spread = jnp.where(lane[:, :128] == i, jnp.sum(x, axis=1, keepdims=True), spread)
    slots[me] = jnp.sum(spread, axis=0, keepdims=True)
    pl.when(me > 0)(hear_late)
    for k in range(n - 1):
        pltpu.make_async_remote_copy(
            src_ref=slots.at[me], dst_ref=slots.at[me],
            send_sem=gsem.at[0], recv_sem=gsem.at[1],
            device_id={"blk": k + jnp.where(k >= me, 1, 0)}, device_id_type=pl.DeviceIdType.MESH,
        ).start()

    pl.when(me > 0)(tracers_and_east)
    arrive(2, 16)

    def mend(outs, fixed, row):
        block, place = row // 8 * 8, row % 8
        for i, out in enumerate(outs):
            for level in range(levels):
                spot = i * levels + level
                old = out[level, pl.ds(block, 8)].astype(F32)
                x = pltpu.roll(fixed, (place - spot) % 8, 0) if (place - spot) % 8 else fixed
                out[level, pl.ds(block, 8)] = jnp.where(sub == place, x, old).astype(BF16)

    def carried(speed, low, high):
        return speed * jnp.where(speed > 0.0, low, high)

    mend((bu, bv), edges[0] + (COURANT * own) * flux_w, 0)
    mend((bu, bv), edges[1] - (COURANT * own) * flux_e[...], rows - 1)
    east = row_of(a4, WEST + rows + EAST - 1)
    speed_e = face(uv_tx[1], uv_rx[...], own * east)
    mend((bh, bs), edges[2] + (COURANT * own) * carried(speed_w, hs_rx[0], hs_tx[0]), 0)
    mend((bh, bs), edges[3] - (COURANT * own) * carried(speed_e, hs_tx[1], hs_rx[1]), rows - 1)

    others = slots.at[pl.ds(0, n - 1)]
    rest = pltpu.make_async_remote_copy(
        src_ref=others, dst_ref=others, send_sem=gsem.at[0], recv_sem=gsem.at[1],
        device_id={"blk": right}, device_id_type=pl.DeviceIdType.MESH,
    )
    rest.wait_recv()
    mom[...] = jnp.broadcast_to(tree([slots[i] for i in range(n)]), (8, 128))
    rest.wait_send()
    lot = a4.at[pl.ds(0, west_rows + 2 * EAST + 24)]
    pltpu.make_async_remote_copy(
        src_ref=lot, dst_ref=lot, send_sem=ssem.at[0], recv_sem=rsem.at[0],
        device_id={"blk": right}, device_id_type=pl.DeviceIdType.MESH,
    ).wait_send()


def finish(bh, bs, bu, bv, basis, mom, o_heat, o_salt, o_u, o_v, o_height, o_resid, hgt, res, sems):
    rows, lanes = hgt.shape
    stores = [
        pltpu.make_async_copy(src, dst, sems.at[0])
        for src, dst in ((bh, o_heat), (bs, o_salt), (bu, o_u), (bv, o_v))
    ]
    for store in stores:
        store.start()
    row = mom[...]
    m = [jnp.broadcast_to(row[:, i : i + 1], (8, 128)) for i in range(MOMENTS)]
    offset, resid = inner_steps(m, SWEEPS)

    def combine(vals, coef):
        return tree([c * v for v, c in zip(vals, coef) if c is not None])

    parts = 2
    step = rows // 8 // parts
    for part in range(parts):
        for s in range(part * step, (part + 1) * step):
            r = 8 * s
            for c in range(0, lanes, 128):
                vals = [basis[i, pl.ds(WEST + r, 8), c : c + 128] for i in range(FIELDS)]
                hgt[pl.ds(r, 8), c : c + 128] = combine(vals, offset)
                res[pl.ds(r, 8), c : c + 128] = combine(vals, resid)
        span = pl.ds(part * step * 8, step * 8)
        for src, dst in ((hgt, o_height), (res, o_resid)):
            pltpu.make_async_copy(src.at[span], dst.at[span], sems.at[1]).start()
    levels = bh.shape[0]
    for sem, count in ((0, 2 * levels), (1, 2)):
        lot = basis.at[pl.ds(0, count), pl.ds(0, rows)]
        pltpu.make_async_copy(lot, lot, sems.at[sem]).wait()


def on_device(heat, salt, uvel, vvel, spacing, damp, flags):
    n = lax.axis_size("blk")
    levels, rows, lanes = uvel.shape
    total = WEST + rows + EAST
    chunks = lanes // 128
    mixed, extra = 8 * chunks + -(-2 * chunks // 8) * 8, -(-3 * chunks // 8) * 8
    extra += -(mixed + extra) % (8 * chunks)
    hbm = pl.BlockSpec(memory_space=pltpu.HBM)
    vmem = pl.BlockSpec(memory_space=pltpu.VMEM)
    args = [
        pltpu.with_memory_space_constraint(x, pltpu.HBM)
        for x in (heat, salt, uvel, vvel, spacing, damp, flags)
    ]
    vm = pltpu.VMEM
    half = jax.ShapeDtypeStruct((levels, rows, lanes), BF16)
    flat = jax.ShapeDtypeStruct((rows, lanes), F32)
    full = vm((levels, rows, lanes), F32)
    dma = pltpu.SemaphoreType.DMA
    mids = (
        half, half, half, half,
        jax.ShapeDtypeStruct((FIELDS, total, lanes), F32),
        jax.ShapeDtypeStruct((8, 128), F32),
    )
    results = pl.pallas_call(
        functools.partial(kernel, n),
        out_shape=mids,
        in_specs=[hbm] * 7,
        out_specs=(vmem,) * 6,
        scratch_shapes=[
            full, full, full, full, full, full,
            vm((2, levels, rows, lanes), F32),
            vm((rows, lanes), F32),
            vm((rows, lanes), F32),
            vm((rows, lanes), F32),
            vm((MOMENTS, 8, 128), F32),
            vm((4, 8, lanes), F32),
            vm((2, 8, lanes), F32),
            vm((2, 8, lanes), F32),
            vm((8, lanes), F32),
            vm((2, 8, lanes), F32),
            vm((mixed, 128), F32),
            vm((mixed, 128), F32),
            vm((extra, 128), F32),
            vm((extra, 128), F32),
            vm((EAST, lanes), F32),
            vm((total, lanes), F32),
            vm((WEST - 8, lanes), F32),
            vm((EAST, lanes), F32),
            vm((WEST - 8, lanes), F32),
            vm((EAST, lanes), F32),
            vm((n, 1, 128), F32),
            pltpu.SMEM(spacing.shape, F32),
            pltpu.SMEM(flags.shape, flags.dtype),
            vm((8, lanes), F32),
            dma((6,)),
            dma((1,)),
            dma((3,)),
            dma((2,)),
            pltpu.SemaphoreType.REGULAR((1,)),
        ],
        compiler_params=pltpu.CompilerParams(
            collective_id=0, has_side_effects=True, vmem_limit_bytes=40 * 1024 * 1024
        ),
    )(*args)
    results = [pltpu.with_memory_space_constraint(x, pltpu.VMEM) for x in results]
    shapes = (half, half, half, half, flat, flat)
    return pl.pallas_call(
        finish,
        out_shape=tuple(pltpu.HBM(x.shape, x.dtype) for x in shapes),
        in_specs=[vmem] * 6,
        out_specs=(hbm,) * 6,
        scratch_shapes=[vm((rows, lanes), F32), vm((rows, lanes), F32), dma((2,))],
        compiler_params=pltpu.CompilerParams(vmem_limit_bytes=8 * 1024 * 1024),
    )(*results)


def solution(mesh):
    return jax.shard_map(
        on_device,
        mesh=mesh,
        in_specs=(
            P("member", "blk", None),
            P("member", "blk", None),
            P("member", "blk", None),
            P("member", "blk", None),
            P(),
            P("blk", None),
            P("blk", None),
        ),
        out_specs=(
            P("member", "blk", None),
            P("member", "blk", None),
            P("member", "blk", None),
            P("member", "blk", None),
            P(("member", "blk"), None),
            P(("member", "blk"), None),
        ),
        check_vma=False,
    )
```

```python
import functools

import jax
import jax.numpy as jnp
import numpy as np
from jax import lax
from jax.experimental import pallas as pl
from jax.experimental.pallas import tpu as pltpu
from jax.sharding import PartitionSpec as P

SSTEP = 4
CG_BLOCKS = 3
SWEEPS = SSTEP * CG_BLOCKS
FIELDS = SWEEPS + 1
MOMENTS = 2 * SWEEPS
COURANT = 0.2
SHIFT = SWEEPS + 2
WEST = -(-(2 * SWEEPS + 2) // 8) * 8
EAST = -(-(SWEEPS + 2) // 8) * 8
F32 = jnp.float32
BF16 = jnp.bfloat16


def shift_table(extent):
    table = np.zeros((extent, extent), np.float32)
    for source in range(extent - 1):
        if source == 0:
            table[1, 0] = table[0, 0] = 0.5
        else:
            table[source + 1, source] = 0.25
            table[source, source] = 0.5
            table[source - 1, source] = 0.25
    return table


def tree(terms):
    while len(terms) > 1:
        terms = [
            terms[i] + terms[i + 1] if i + 1 < len(terms) else terms[i]
            for i in range(0, len(terms), 2)
        ]
    return terms[0]


def plus(a, b):
    if a is None:
        return b
    if b is None:
        return a
    return a + b


def scaled(scale, a):
    return None if a is None else scale * a


def inner_steps(m, sweeps):
    extent = sweeps + 1
    table = shift_table(extent)
    ones = jnp.ones_like(m[0])
    pushed = [0.25 * (m[k + 1] + m[abs(k - 1)]) + 0.5 * m[k] for k in range(2 * sweeps - 1)]
    a = [[pushed[i + j] + pushed[i - j] for j in range(i + 1)] for i in range(sweeps)]
    lower = [[None] * sweeps for _ in range(sweeps)]
    inverse = []
    y = [m[i] + m[i] for i in range(sweeps)]
    for k in range(sweeps):
        inverse.append(ones / a[k][k])
        for i in range(k + 1, sweeps):
            lower[i][k] = a[i][k] * inverse[k]
        for i in range(k + 1, sweeps):
            for j in range(k + 1, i + 1):
                a[i][j] = a[i][j] - lower[i][k] * a[j][k]
            y[i] = y[i] - lower[i][k] * y[k]

    def backward(y):
        z = [v * d for v, d in zip(y, inverse)]
        for i in range(sweeps - 1, 0, -1):
            for j in range(i):
                z[j] = z[j] - lower[i][j] * z[i]
        return z

    def image(c):
        out = []
        for i in range(extent):
            total = None
            for j in range(sweeps):
                if table[i, j] != 0.0:
                    total = plus(total, scaled(float(table[i, j]), c[j]))
            out.append(total)
        return out

    offset = backward(y)
    resid = [-x for x in image(offset)]
    resid[0] = resid[0] + ones
    y = [
        tree([(m[i + j] + m[abs(i - j)]) * resid[j] for j in range(extent)]) for i in range(sweeps)
    ]
    for i in range(sweeps):
        for j in range(i + 1, sweeps):
            y[j] = y[j] - lower[j][i] * y[i]
    more = backward(y)
    offset = [c + d for c, d in zip(offset, more)]
    resid = [r - x for r, x in zip(resid, image(more))]
    return offset, resid


def kernel(
    n,
    heat, salt, uvel, vvel, spacing, damp, flags,
    bh, bs, bu, bv, basis, mom,
    ue, ve, he, se, ef, nf, ff, de, tu, tv, acc, edges,
    uv_tx, hs_tx, uv_rx, hs_rx, mix_tx, mix_rx, fx_tx, fx_rx, ae_tx, a4, fw_tx, fe_tx, fw_rx, fe_rx, slots,
    space, marks,
    flux_e, lsem, ssem, rsem, gsem, late_sem,
):
    levels, rows, lanes = ue.shape
    me = lax.axis_index("blk")
    right, left = lax.rem(me + 1, n), lax.rem(me + n - 1, n)
    late = rows - WEST
    chunks = lanes // 128
    west_rows = 2 * (WEST - 8) * chunks + mix_tx.shape[0] + fx_tx.shape[0]
    split = late - 8

    def part(ref, buf, lo, hi, sem):
        return pltpu.make_async_copy(
            ref.at[:, pl.ds(lo, hi - lo)], buf.at[:, pl.ds(lo, hi - lo)], lsem.at[sem]
        )

    def pair(lo, hi, sem):
        both = ff.at[:, :, pl.ds(lo, hi - lo)]
        return pltpu.make_async_copy(both, both, lsem.at[sem])

    loads = [
        pltpu.make_async_copy(flags, marks, lsem.at[0]),
        pltpu.make_async_copy(spacing, space, lsem.at[1]),
        pltpu.make_async_copy(damp.at[pl.ds(late, WEST)], de.at[pl.ds(late, WEST)], lsem.at[3]),
        part(uvel, ue, split, rows, 2),
        part(vvel, ve, split, rows, 2),
        part(uvel, ue, 0, split, 4),
        part(vvel, ve, 0, split, 4),
        pltpu.make_async_copy(damp.at[pl.ds(0, late)], de.at[pl.ds(0, late)], lsem.at[5]),
    ]
    more = [
        pltpu.make_async_copy(heat, he, lsem.at[2]),
        pltpu.make_async_copy(salt, se, lsem.at[2]),
    ]
    barrier = pltpu.get_barrier_semaphore()

    def tell(sem, to):
        pl.semaphore_signal(
            sem, inc=1, device_id={"blk": to}, device_id_type=pl.DeviceIdType.MESH
        )

    at_start, at_end = me == 0, me == n - 1
    pl.when(me > 0)(lambda: tell(barrier, left))
    for load in loads[:5]:
        load.start()
    for k in range(1, n):
        pl.when(me + k < n)(functools.partial(tell, barrier, lax.rem(me + k, n)))
    for load in loads[5:]:
        load.start()

    def pass_barrier():
        pl.semaphore_wait(barrier, jnp.where(at_end, n - 1, me + 1))

    def tell_earlier():
        for k in range(2, n):
            pl.when(me - k >= 0)(functools.partial(tell, late_sem.at[0], lax.rem(me + n - k, n)))

    def hear_late():
        later = n - 2 - me
        pl.when(later > 0)(lambda: pl.semaphore_wait(late_sem.at[0], later))

    lane = lax.broadcasted_iota(jnp.int32, (8, lanes), 1)
    sub = lax.broadcasted_iota(jnp.int32, (8, lanes), 0)
    top, bottom = sub == 0, sub == 7
    zero = jnp.zeros((8, lanes), F32)

    def north_of(x):
        return pltpu.roll(x, lanes - 1, 1)

    def south_of(x):
        return pltpu.roll(x, 1, 1)

    def sides(x):
        return jnp.where(lane == lanes - 1, 0.0, north_of(x)), jnp.where(lane == 0, 0.0, south_of(x))

    slim = lane[:, :128]

    def beside(x):
        tiles = [x[:, c : c + 128] for c in range(0, lanes, 128)]
        north = [pltpu.roll(t, 127, 1) for t in tiles] + [0.0]
        south = [pltpu.roll(t, 1, 1) for t in tiles]
        south = [0.0] + south
        return jnp.concatenate(
            [
                jnp.where(slim == 127, north[i + 1], north[i]) + jnp.where(slim == 0, south[i], south[i + 1])
                for i in range(len(tiles))
            ],
            axis=1,
        )

    def up_one(x):
        return pltpu.roll(x, 7, 0)

    def down_one(x):
        return pltpu.roll(x, 1, 0)

    loads[0].wait()
    loads[1].wait()
    tiles = marks.shape[1]
    lane_tile = lane // (lanes // tiles)
    own = zero
    for k in range(tiles):
        own = jnp.where(lane_tile == k, marks[0, k].astype(F32), own)
    ahead = jnp.where(lane == lanes - 1, 0.0, own * north_of(own))
    half_own = 0.5 * own
    whole_w = jnp.zeros((8, 128), F32)
    for j in range(levels):
        whole_w = whole_w + space[j]
    portions = [jnp.full((8, 128), space[j], F32) / whole_w for j in range(levels)]

    def wide(x):
        return jnp.concatenate([x] * (lanes // 128), axis=1)

    weight = [wide(x) for x in portions]
    level_weight = zero
    for j in range(levels):
        level_weight = jnp.where(sub % levels == j, weight[j], level_weight)

    def gather_row(refs, row):
        block, place = row // 8 * 8, row % 8
        packed = None
        for i, ref in enumerate(refs):
            for level in range(levels):
                x = ref[level, pl.ds(block, 8)]
                spot = i * levels + level
                if (spot - place) % 8:
                    x = pltpu.roll(x, (spot - place) % 8, 0)
                packed = x if packed is None else jnp.where(sub == spot, x, packed)
        return packed

    def pick(packed, block, spot, place):
        return jnp.where(sub == spot, pltpu.roll(block, (spot - place) % 8, 0) if (spot - place) % 8 else block, packed)

    def north_flux(first, last, fields, keep):
        for level in range(levels):
            for r in range(first, last, 8):
                here = pl.ds(r, 8)
                q0 = [ref[level, here] for ref in fields]
                qn = [north_of(q) for q in q0]
                if keep:
                    north = (q0[1] + qn[1]) * ahead
                    nf[level, here] = north
                else:
                    north = nf[level, here]
                for i in range(2):
                    ff[i, level, here] = north * jnp.where(north > 0.0, q0[i], qn[i])

    def flows(first, last, fields, outs, slot, keep):
        ends = [zero, zero]
        for level in range(levels):
            def ahead_of(ref, r, q0):
                if r + 8 < rows:
                    return jnp.where(bottom, up_one(ref[level, pl.ds(r + 8, 8)]), up_one(q0))
                return up_one(q0)

            def east_fluxes(r):
                q0 = [ref[level, pl.ds(r, 8)] for ref in fields]
                qp = [ahead_of(ref, r, q) for ref, q in zip(fields, q0)]
                if keep:
                    east = q0[0] + qp[0]
                    if r + 8 == rows:
                        east = jnp.where(bottom, 0.0, east)
                    ef[level, pl.ds(r, 8)] = east
                else:
                    east = ef[level, pl.ds(r, 8)]
                return q0, [east * jnp.where(east > 0.0, a, b) for a, b in zip(q0, qp)]

            before = [zero, zero] if first == 0 else [down_one(f) for f in east_fluxes(first - 8)[1]]
            pending = None
            for r in range(first, last, 8):
                here = pl.ds(r, 8)
                q0, fe = east_fluxes(r)
                news = []
                for i in range(2):
                    shifted = down_one(fe[i])
                    fw = jnp.where(top, before[i], shifted)
                    before[i] = shifted
                    fn = ff[i, level, here]
                    spread = (fe[i] - fw) + (fn - south_of(fn))
                    new = own * (q0[i] - (0.5 * COURANT) * spread)
                    news.append(new)
                    if keep:
                        total = (tu, tv)[i]
                        term = weight[level] * new
                        total[here] = term if level == 0 else total[here] + term
                    spot = i * levels + level
                    if r == 0:
                        ends[0] = pick(ends[0], new, spot, 0)
                    if r + 8 == rows:
                        ends[1] = pick(ends[1], new, spot, 7)
                if pending is None:
                    pending = news
                else:
                    for i, out in enumerate(outs):
                        out[level, pl.ds(r - 8, 16)] = jnp.concatenate([pending[i], news[i]], axis=0).astype(BF16)
                    pending = None
        if first == 0:
            edges[slot] = ends[0]
        if last == rows:
            edges[slot + 1] = ends[1]

    def forcing(r, low, high):
        t0, x0 = tv[pl.ds(r, 8)], tu[pl.ds(r, 8)]
        north, south = sides(t0)
        after = jnp.where(bottom, up_one(tu[pl.ds(r + 8, 8)]) if r + 8 < high else 0.0, up_one(x0))
        prior = jnp.where(top, down_one(tu[pl.ds(r - 8, 8)]) if r > low else 0.0, down_one(x0))
        return (0.5 * own) * ((after - prior) + (north - south))

    def send(src, dst, sem, to):
        pltpu.make_async_remote_copy(
            src_ref=src, dst_ref=dst, send_sem=ssem.at[0], recv_sem=rsem.at[sem],
            device_id={"blk": to}, device_id_type=pl.DeviceIdType.MESH,
        ).start()

    def lot_of(count):
        return acc.at[pl.ds(0, count // 8)]

    def arrive(sem, count):
        lot = lot_of(count)
        pltpu.make_async_remote_copy(
            src_ref=lot, dst_ref=lot, send_sem=ssem.at[0], recv_sem=rsem.at[sem],
            device_id={"blk": right}, device_id_type=pl.DeviceIdType.MESH,
        ).wait_recv()

    def send_left():
        send(uv_tx.at[0], uv_rx, 1, left)
        send(ae_tx, a4.at[pl.ds(WEST + rows, EAST)], 1, left)
        send(fe_tx, fe_rx, 1, left)

    def pack(ref, base, items):
        packed = {}
        for i, (x, place) in enumerate(items):
            for c in range(chunks):
                group, spot = divmod(i * chunks + c, 8)
                t = x[:, 128 * c : 128 * c + 128]
                if (spot - place) % 8:
                    t = pltpu.roll(t, (spot - place) % 8, 0)
                packed[group] = jnp.where(sub[:, :128] == spot, t, packed[group]) if group in packed else t
        for group, x in packed.items():
            ref[pl.ds(base + 8 * group, 8)] = x

    def unpack(ref, base, i):
        return jnp.concatenate(
            [jnp.broadcast_to(ref[pl.ds(base + i * chunks + c, 1)], (8, 128)) for c in range(chunks)], axis=1
        )

    def damping(first, last):
        for r in range(first, last, 8):
            a4[pl.ds(WEST + r, 8)] = 0.5 * (own * (6.0 + de[pl.ds(r, 8)]) + (1.0 - own)) - 2.0

    loads[2].wait()
    damping(late, rows)
    pack(mix_tx, 8 * chunks, [(a4[pl.ds(WEST + late, 8)], 7), (own, 7)])
    pair(split, rows, 2).wait()
    uv_tx[1] = gather_row((ue, ve), rows - 1)
    for c in range(chunks):
        mix_tx[pl.ds(8 * c, 8)] = uv_tx[1, :, 128 * c : 128 * c + 128]
    def open_right():
        pass_barrier()
        send(mix_tx, mix_rx, 0, right)
        send(a4.at[pl.ds(WEST + late + 8, WEST - 8)], a4.at[pl.ds(8, WEST - 8)], 0, right)
        tell_earlier()

    waits = (lax.rem(me, 2) == 1) & (me < n - 1)
    pl.when(jnp.logical_not(waits))(open_right)
    for load in more:
        load.start()
    north_flux(late, rows, (ue, ve), True)
    flows(late, rows, (ue, ve), (bu, bv), 0, True)
    for r in range(late, rows, 8):
        f = forcing(r, late, rows)
        if r > late:
            basis[0, pl.ds(WEST + r, 8)] = f
            fw_tx[pl.ds(r - late - 8, 8)] = f
        else:
            pack(fx_tx, 0, [(f, 6), (f, 7), (tu[pl.ds(rows - 8, 8)], 7)])
    pl.when(waits)(open_right)
    send(fw_tx, fw_rx, 0, right)
    send(fx_tx, fx_rx, 0, right)

    pair(0, split, 4).wait()
    uv_tx[0] = gather_row((ue, ve), 0)
    loads[7].wait()
    damping(0, late)
    for r in range(0, EAST, 8):
        a = a4[pl.ds(WEST + r, 8)]
        ae_tx[pl.ds(r, 8)] = jnp.where(bottom, own, a) if r + 8 == EAST else a
    north_flux(0, late, (ue, ve), True)
    flows(0, late, (ue, ve), (bu, bv), 0, True)
    for r in range(0, late + 8, 8):
        f = forcing(r, 0, rows)
        basis[0, pl.ds(WEST + r, 8)] = f
        if r < EAST:
            if r + 8 == EAST:
                f = jnp.where(bottom, jnp.broadcast_to(tu[pl.ds(0, 1)], (8, lanes)), f)
            fe_tx[pl.ds(r, 8)] = f
    pl.when(me > 0)(send_left)

    window = (-SHIFT, rows - SHIFT)

    def in_window(r, x):
        if r < window[0]:
            return jnp.where(sub >= window[0] - r, x, 0.0)
        if r + 8 > window[1]:
            return jnp.where(sub < window[1] - r, x, 0.0)
        return x

    def fold(x):
        return tree([x[:, c : c + 128] for c in range(0, lanes, 128)])

    def sweep(p, first, last, low, high, half_wet, summed, held=None):
        held = {} if held is None else held
        known = {}

        def field(q, r):
            return held[q, r] if (q, r) in held else basis[q, pl.ds(WEST + r, 8)]

        def block(r):
            if r not in known:
                k0 = field(p, r)
                known[r] = (k0, down_one(k0), up_one(k0))
            return known[r]

        squares, crosses = [], []
        turned = {}
        for r in range(first, last, 8):
            k0, down, up = block(r)
            prior = block(r - 8)[1] if r > low else down
            after = block(r + 8)[2] if r + 8 < high else up
            vert = jnp.where(top, prior, down) + jnp.where(bottom, after, up)
            turned[r] = vert, beside(k0 + 0.5 * vert)
        for r in range(first, last, 8):
            k0 = block(r)[0]
            vert, side = turned[r]
            here = pl.ds(WEST + r, 8)
            half = a4[here] * k0 - half_wet(r) * (vert + side)
            new = 0.5 * half if p == 0 else half - field(p - 1, r)
            basis[p + 1, here] = new
            held[p + 1, r] = new
            if summed[0] <= r < summed[1]:
                kept = in_window(r, k0)
                squares.append(kept * kept)
                crosses.append(kept * in_window(r, new))
        for key in [key for key in held if key[0] < p]:
            del held[key]
        return [tree([fold(t) for t in x]) for x in (squares, crosses) if x]

    def floor8(x):
        return x // 8 * 8

    def ceil8(x):
        return -(-x // 8) * 8

    inner_from, inner_to = ceil8(SWEEPS + 2), rows - SHIFT
    for p in range(SWEEPS):
        j = p + 1
        sums = sweep(
            p, floor8(2 + j), ceil8(rows - 2 - j), 0, rows, lambda r: half_own, (inner_from, inner_to)
        )
        for i, x in enumerate(sums):
            acc[2 * p + i] = x

    pltpu.make_async_copy(ff, ff, lsem.at[2]).wait()
    hs_tx[0] = gather_row((he, se), 0)
    hs_tx[1] = gather_row((he, se), rows - 1)
    send(hs_tx.at[1], hs_rx.at[0], 2, right)
    pl.when(me > 0)(lambda: send(hs_tx.at[0], hs_rx.at[1], 2, left))

    def tracers():
        north_flux(0, rows, (he, se), False)
        flows(0, rows, (he, se), (bh, bs), 2, False)

    def total_of(x):
        for step in (4, 2, 1):
            x = x + pltpu.roll(x, step, 0)
        return x

    def face(low, high, both):
        twice = [jnp.where(sub < levels, x, pltpu.roll(x, levels, 0)) for x in (low, high)]
        return 0.5 * (twice[0] + twice[1]) * both

    def seam(uv_low, uv_high, wet_low, wet_high, tu_low, tu_high, f_low, f_high):
        speed = face(uv_low, uv_high, wet_low * wet_high)
        flux = speed * jnp.where(speed > 0.0, uv_low, uv_high)
        term = level_weight * flux
        gu = total_of(jnp.where(sub < levels, term, 0.0))
        gv = total_of(jnp.where(sub < levels, 0.0, term))
        low_u, high_u = (-COURANT * wet_low) * gu, (COURANT * wet_high) * gu
        low_v, high_v = (-COURANT * wet_low) * gv, (COURANT * wet_high) * gv
        north, south = sides(jnp.where(sub < 4, high_v, low_v))
        across = north - south
        f_low = f_low + (0.5 * wet_low) * jnp.where(
            sub == 7, (tu_high + high_u) + across, jnp.where(sub == 6, low_u, 0.0)
        )
        f_high = f_high + (0.5 * wet_high) * jnp.where(
            sub == 0, across - (tu_low + low_u), jnp.where(sub == 1, -high_u, 0.0)
        )
        return speed, flux, f_low, f_high

    def row_of(ref, row):
        return jnp.broadcast_to(ref[pl.ds(row, 1)], (8, lanes))

    def tracers_and_east(both=True):
        if both:
            tracers()
        arrive(1, (2 * EAST + 8) * chunks)
        east = row_of(a4, WEST + rows + EAST - 1)
        _, flux, f_low, f_high = seam(
            uv_tx[1], uv_rx[...], own, east, row_of(tu, rows - 1), row_of(fe_rx, EAST - 1),
            basis[0, pl.ds(WEST + rows - 8, 8)], fe_rx[pl.ds(0, 8)],
        )
        flux_e[...] = flux
        basis[0, pl.ds(WEST + rows - 8, 8)] = f_low
        basis[0, pl.ds(WEST + rows, 8)] = f_high
        for r in range(8, EAST, 8):
            basis[0, pl.ds(WEST + rows + r, 8)] = fe_rx[pl.ds(r, 8)]
        held = {}
        half_east = 0.5 * east
        for p in range(SWEEPS):
            j = p + 1
            sweep(
                p, floor8(rows - 2 - j), ceil8(rows + SWEEPS - j), 0, rows + EAST,
                lambda r: half_own if r < rows else half_east, (0, 0), held,
            )

    def before_west():
        tracers()
        hear_late()
        send_left()
        send(hs_tx.at[0], hs_rx.at[1], 2, left)
        tracers_and_east(False)

    pl.when(at_start)(before_west)

    arrive(0, west_rows)
    west = unpack(mix_rx, 8 * chunks, 1)
    a4[pl.ds(0, 8)] = unpack(mix_rx, 8 * chunks, 0)
    uv_west = jnp.concatenate([mix_rx[pl.ds(8 * c, 8)] for c in range(chunks)], axis=1)
    speed_w, flux_w, f_low, f_high = seam(
        uv_west, uv_tx[0], west, own, unpack(fx_rx, 0, 2), row_of(tu, 0),
        fw_rx[pl.ds(WEST - 16, 8)], basis[0, pl.ds(WEST, 8)],
    )
    basis[0, pl.ds(0, 8)] = jnp.where(bottom, unpack(fx_rx, 0, 1), unpack(fx_rx, 0, 0))
    for r in range(8, WEST - 8, 8):
        basis[0, pl.ds(r, 8)] = fw_rx[pl.ds(r - 8, 8)]
    basis[0, pl.ds(WEST - 8, 8)] = f_low
    basis[0, pl.ds(WEST, 8)] = f_high

    moments = [None] * MOMENTS
    west_held = {}
    half_west = 0.5 * west
    for p in range(SWEEPS):
        j = p + 1
        sums = sweep(
            p, floor8(j - 2 * SWEEPS - 2), ceil8(2 + j) if j < SWEEPS else inner_from, -WEST, rows,
            lambda r: half_west if r < 0 else half_own, (floor8(-SHIFT), 8), west_held,
        )
        for i, x in enumerate(sums):
            moments[2 * p + i] = x
        tail = []
        for r in range(8, inner_from, 8):
            k0, k1 = basis[p, pl.ds(WEST + r, 8)], basis[p + 1, pl.ds(WEST + r, 8)]
            tail.append((k0 * k0, k0 * k1))
        for i in range(len(sums)):
            moments[2 * p + i] = tree(
                [moments[2 * p + i], acc[2 * p + i]] + [fold(t[i]) for t in tail]
            )
    base = moments[:2]
    moments = base + [2.0 * x - base[i % 2] for i, x in enumerate(moments[2:])]
    spread = jnp.zeros((8, 128), F32)
    for i, x in enumerate(moments):
        spread = jnp.where(lane[:, :128] == i, jnp.sum(x, axis=1, keepdims=True), spread)
    slots[me] = jnp.sum(spread, axis=0, keepdims=True)
    pl.when(me > 0)(hear_late)
    for k in range(n - 1):
        pltpu.make_async_remote_copy(
            src_ref=slots.at[me], dst_ref=slots.at[me],
            send_sem=gsem.at[0], recv_sem=gsem.at[1],
            device_id={"blk": k + jnp.where(k >= me, 1, 0)}, device_id_type=pl.DeviceIdType.MESH,
        ).start()

    pl.when(me > 0)(tracers_and_east)
    arrive(2, 16 * chunks)

    def mend(outs, fixed, row):
        block, place = row // 8 * 8, row % 8
        for i, out in enumerate(outs):
            for level in range(levels):
                spot = i * levels + level
                old = out[level, pl.ds(block, 8)].astype(F32)
                x = pltpu.roll(fixed, (place - spot) % 8, 0) if (place - spot) % 8 else fixed
                out[level, pl.ds(block, 8)] = jnp.where(sub == place, x, old).astype(BF16)

    def carried(speed, low, high):
        return speed * jnp.where(speed > 0.0, low, high)

    mend((bu, bv), edges[0] + (COURANT * own) * flux_w, 0)
    mend((bu, bv), edges[1] - (COURANT * own) * flux_e[...], rows - 1)
    east = row_of(a4, WEST + rows + EAST - 1)
    speed_e = face(uv_tx[1], uv_rx[...], own * east)
    mend((bh, bs), edges[2] + (COURANT * own) * carried(speed_w, hs_rx[0], hs_tx[0]), 0)
    mend((bh, bs), edges[3] - (COURANT * own) * carried(speed_e, hs_tx[1], hs_rx[1]), rows - 1)

    others = slots.at[pl.ds(0, n - 1)]
    rest = pltpu.make_async_remote_copy(
        src_ref=others, dst_ref=others, send_sem=gsem.at[0], recv_sem=gsem.at[1],
        device_id={"blk": right}, device_id_type=pl.DeviceIdType.MESH,
    )
    rest.wait_recv()
    mom[...] = jnp.broadcast_to(tree([slots[i] for i in range(n)]), (8, 128))
    rest.wait_send()
    lot = lot_of(west_rows + (2 * EAST + 24) * chunks)
    pltpu.make_async_remote_copy(
        src_ref=lot, dst_ref=lot, send_sem=ssem.at[0], recv_sem=rsem.at[0],
        device_id={"blk": right}, device_id_type=pl.DeviceIdType.MESH,
    ).wait_send()


def finish(bh, bs, bu, bv, basis, mom, o_heat, o_salt, o_u, o_v, o_height, o_resid, hgt, res, sems):
    rows, lanes = hgt.shape
    stores = [
        pltpu.make_async_copy(src, dst, sems.at[0])
        for src, dst in ((bh, o_heat), (bs, o_salt), (bu, o_u), (bv, o_v))
    ]
    for store in stores:
        store.start()
    row = mom[...]
    m = [jnp.broadcast_to(row[:, i : i + 1], (8, 128)) for i in range(MOMENTS)]
    offset, resid = inner_steps(m, SWEEPS)

    def combine(vals, coef):
        return tree([c * v for v, c in zip(vals, coef) if c is not None])

    parts = 2
    step = rows // 8 // parts
    for part in range(parts):
        for s in range(part * step, (part + 1) * step):
            r = 8 * s
            for c in range(0, lanes, 128):
                vals = [basis[i, pl.ds(WEST + r, 8), c : c + 128] for i in range(FIELDS)]
                hgt[pl.ds(r, 8), c : c + 128] = combine(vals, offset)
                res[pl.ds(r, 8), c : c + 128] = combine(vals, resid)
        span = pl.ds(part * step * 8, step * 8)
        for src, dst in ((hgt, o_height), (res, o_resid)):
            pltpu.make_async_copy(src.at[span], dst.at[span], sems.at[1]).start()
    levels = bh.shape[0]
    for sem, count in ((0, 2 * levels), (1, 2)):
        lot = basis.at[pl.ds(0, count), pl.ds(0, rows)]
        pltpu.make_async_copy(lot, lot, sems.at[sem]).wait()


def on_device(heat, salt, uvel, vvel, spacing, damp, flags):
    n = lax.axis_size("blk")
    levels, rows, lanes = uvel.shape
    total = WEST + rows + EAST
    chunks = lanes // 128
    mixed, extra = 8 * chunks + -(-2 * chunks // 8) * 8, -(-3 * chunks // 8) * 8
    hbm = pl.BlockSpec(memory_space=pltpu.HBM)
    vmem = pl.BlockSpec(memory_space=pltpu.VMEM)
    args = [
        pltpu.with_memory_space_constraint(x, pltpu.HBM)
        for x in (heat, salt, uvel, vvel, spacing, damp, flags)
    ]
    vm = pltpu.VMEM
    half = jax.ShapeDtypeStruct((levels, rows, lanes), BF16)
    flat = jax.ShapeDtypeStruct((rows, lanes), F32)
    full = vm((levels, rows, lanes), F32)
    dma = pltpu.SemaphoreType.DMA
    mids = (
        half, half, half, half,
        jax.ShapeDtypeStruct((FIELDS, total, lanes), F32),
        jax.ShapeDtypeStruct((8, 128), F32),
    )
    results = pl.pallas_call(
        functools.partial(kernel, n),
        out_shape=mids,
        in_specs=[hbm] * 7,
        out_specs=(vmem,) * 6,
        scratch_shapes=[
            full, full, full, full, full, full,
            vm((2, levels, rows, lanes), F32),
            vm((rows, lanes), F32),
            vm((rows, lanes), F32),
            vm((rows, lanes), F32),
            vm((max(MOMENTS, (total + WEST) * chunks // 8), 8, 128), F32),
            vm((4, 8, lanes), F32),
            vm((2, 8, lanes), F32),
            vm((2, 8, lanes), F32),
            vm((8, lanes), F32),
            vm((2, 8, lanes), F32),
            vm((mixed, 128), F32),
            vm((mixed, 128), F32),
            vm((extra, 128), F32),
            vm((extra, 128), F32),
            vm((EAST, lanes), F32),
            vm((total, lanes), F32),
            vm((WEST - 8, lanes), F32),
            vm((EAST, lanes), F32),
            vm((WEST - 8, lanes), F32),
            vm((EAST, lanes), F32),
            vm((n, 1, 128), F32),
            pltpu.SMEM(spacing.shape, F32),
            pltpu.SMEM(flags.shape, flags.dtype),
            vm((8, lanes), F32),
            dma((6,)),
            dma((1,)),
            dma((3,)),
            dma((2,)),
            pltpu.SemaphoreType.REGULAR((1,)),
        ],
        compiler_params=pltpu.CompilerParams(
            collective_id=0, has_side_effects=True, vmem_limit_bytes=40 * 1024 * 1024
        ),
    )(*args)
    results = [pltpu.with_memory_space_constraint(x, pltpu.VMEM) for x in results]
    shapes = (half, half, half, half, flat, flat)
    return pl.pallas_call(
        finish,
        out_shape=tuple(pltpu.HBM(x.shape, x.dtype) for x in shapes),
        in_specs=[vmem] * 6,
        out_specs=(hbm,) * 6,
        scratch_shapes=[vm((rows, lanes), F32), vm((rows, lanes), F32), dma((2,))],
        compiler_params=pltpu.CompilerParams(vmem_limit_bytes=8 * 1024 * 1024),
    )(*results)


def solution(mesh):
    return jax.shard_map(
        on_device,
        mesh=mesh,
        in_specs=(
            P("member", "blk", None),
            P("member", "blk", None),
            P("member", "blk", None),
            P("member", "blk", None),
            P(),
            P("blk", None),
            P("blk", None),
        ),
        out_specs=(
            P("member", "blk", None),
            P("member", "blk", None),
            P("member", "blk", None),
            P("member", "blk", None),
            P(("member", "blk"), None),
            P(("member", "blk"), None),
        ),
        check_vma=False,
    )
```
